256 devices in a mesh: seq: 64 (over x, z, core), var: 4 (over y).
Axes of the slice: x: 4, y: 4, z: 8, core: 2. Of those that a mesh axis runs over, the one named last changes fastest.
Arguments:
- clean_proj: bfloat16 [2048, 10240], P('seq'), may hold values from -8 to 8
- corrupt_proj: bfloat16 [2048, 10240], P('seq'), may hold values from -8 to 8
- patch_pos: int32 [4, 16], P('var'), may hold values from 0 to 2047
- patch_mode: int32 [4], P('var'), may hold values from 0 to 2
- a_log: float32 [16, 5120], replicated, may hold values from -6 to 1.5
- dt_bias: float32 [5120], replicated, may hold values from -6 to -2
- conv_weight: float32 [4, 5120], replicated, may hold values from -3 to 3
- conv_bias: float32 [5120], replicated, may hold values from -3 to 3
- x_weight: bfloat16 [5120, 192], replicated, may hold values from -0.078125 to 0.078125
- dt_weight: bfloat16 [160, 5120], replicated, may hold values from -0.5 to 0.5
- d_skip: float32 [5120], replicated, may hold values from 0.5 to 1.5
Outputs:
- patched_out: bfloat16 [4, 2048, 5120], P('var', 'seq')
- effect_peak: float32 [4, 5120], P('var')
The draws below stay inside these ranges and needn't reach their ends.
Inputs may be any that keep to these rules, and one draw needn't show every extreme that they name: `patch_pos`: positions of one variant may repeat.
All inputs are finite; a program needn't handle non-finite values.
Results may differ from the reference program's by a relative error of at most 0.0029.
The reference program's roundings to bfloat16 on the way (of `conv_act`, `low_rank` and `patched_in`) count: a program that leaves them out, or rounds other values in their place, can miss the bound.
Values may be sent and summed in bfloat16 or wider, within the bound.
A program may use at most 128 MiB of HBM per device.

```python
import jax
import jax.numpy as jnp
from jax import lax

INNER = 5120
STATE = 16
RANK = 160
CONV = 4
PATCHES = 16
SEQ = 2048
VARS = 4


def paired_inputs(key):
    base_key = jax.random.fold_in(key, 101)
    jitter_key = jax.random.fold_in(key, 202)
    shape_full = (SEQ, 2 * INNER)
    base_values = jax.random.normal(base_key, shape_full, jnp.float32)
    jitter = jax.random.normal(jitter_key, shape_full, jnp.float32)
    position = jnp.arange(SEQ, dtype=jnp.float32) / SEQ
    growth = 1.0 + 2.0 * position
    clean_values = jnp.clip(base_values, -8.0, 8.0)
    corrupt_values = jnp.clip(base_values + 0.6 * growth[:, None] * jitter, -8.0, 8.0)
    return (clean_values, corrupt_values)


def draw_clean_proj(key, part):
    return paired_inputs(key)[0].astype(jnp.bfloat16)


def draw_corrupt_proj(key, part):
    return paired_inputs(key)[1].astype(jnp.bfloat16)


def place_ends(drawn, own_key, smallest, top_value):
    longest = drawn.shape.index(max(drawn.shape))
    spots = []
    for shift in (0, 1):
        where = [jax.random.randint(jax.random.fold_in(own_key, axis), (), 0, length) for axis, length in enumerate(drawn.shape)]
        where[longest] = (where[longest] + shift) % drawn.shape[longest]
        spots.append(tuple(where))
    return drawn.at[spots[0]].set(smallest).at[spots[1]].set(top_value)


def bell_draw(key, dims, width, bound, kind=jnp.bfloat16):
    drawn = width * jax.random.normal(key, dims, jnp.float32)
    return jnp.clip(drawn, min=-bound, max=bound).astype(kind)


def setup_inputs(seed: int = 0) -> dict:
    arg_keys = jax.random.split(jax.random.key(seed), 12)
    return {
        "clean_proj": draw_clean_proj(jax.random.fold_in(arg_keys[11], 71), 0),
        "corrupt_proj": draw_corrupt_proj(jax.random.fold_in(arg_keys[11], 71), 0),
        "patch_pos": place_ends(jax.random.randint(arg_keys[2], (VARS, PATCHES), 0, SEQ), jax.random.fold_in(arg_keys[2], 1), 0, SEQ - 1).astype(jnp.int32),
        "patch_mode": place_ends(jax.random.randint(arg_keys[3], (VARS,), 0, 3), jax.random.fold_in(arg_keys[3], 1), 0, 2).astype(jnp.int32),
        "a_log": jnp.clip(jax.random.uniform(arg_keys[4], (STATE, INNER), jnp.float32, -6.0, 1.5), -6.0, 1.5),
        "dt_bias": jnp.clip(jax.random.uniform(arg_keys[5], (INNER,), jnp.float32, -6.0, -2.0), -6.0, -2.0),
        "conv_weight": bell_draw(arg_keys[6], (CONV, INNER), CONV ** -0.5, 3.0, jnp.float32),
        "conv_bias": bell_draw(arg_keys[7], (INNER,), 0.5, 3.0, jnp.float32),
        "x_weight": bell_draw(arg_keys[8], (INNER, RANK + 2 * STATE), INNER ** -0.5, 0.078125),
        "dt_weight": bell_draw(arg_keys[9], (RANK, INNER), RANK ** -0.5, 0.5),
        "d_skip": jnp.clip(1.0 + 0.1 * jax.random.normal(arg_keys[10], (INNER,), jnp.float32), 0.5, 1.5),
    }


def mixer_run(projection, a_log, dt_bias, conv_weight, conv_bias, x_weight, dt_weight, d_skip):
    length = projection.shape[0]
    signal = projection[:, :INNER].astype(jnp.float32)
    gate_rows = projection[:, INNER:].astype(jnp.float32)
    padded = jnp.concatenate([jnp.zeros((CONV - 1, INNER), jnp.float32), signal], axis=0)
    conv_sum = conv_bias[None, :] + conv_weight[0][None, :] * padded[0:length]
    for lag_index in range(1, CONV):
        conv_sum = conv_sum + conv_weight[lag_index][None, :] * padded[lag_index:lag_index + length]
    conv_act = lax.optimization_barrier(jax.nn.silu(conv_sum).astype(jnp.bfloat16))
    projected = jnp.dot(conv_act, x_weight, preferred_element_type=jnp.float32)
    low_rank = projected[:, :RANK].astype(jnp.bfloat16)
    input_map = projected[:, RANK:RANK + STATE]
    output_map = projected[:, RANK + STATE:]
    step_size = jax.nn.softplus(jnp.dot(low_rank, dt_weight, preferred_element_type=jnp.float32) + dt_bias[None, :])
    decay_rates = jnp.exp(a_log)
    signal_f = conv_act.astype(jnp.float32)

    def stepper(carried, inputs):
        step_row, signal_row, input_vec, output_vec = inputs
        carried = jnp.exp(-step_row[None, :] * decay_rates) * carried + (step_row * signal_row)[None, :] * input_vec[:, None]
        return (carried, lax.optimization_barrier(jnp.sum(output_vec[:, None] * carried, axis=0)))
    final_state, readout = lax.scan(stepper, jnp.zeros((STATE, INNER), jnp.float32), (step_size, signal_f, input_map, output_map))
    result_rows = (readout + d_skip[None, :] * signal_f) * jax.nn.silu(gate_rows)
    return result_rows.astype(jnp.bfloat16)

def reference(clean_proj, corrupt_proj, patch_pos, patch_mode, a_log, dt_bias, conv_weight, conv_bias, x_weight, dt_weight, d_skip):
    clean_out = mixer_run(clean_proj, a_log, dt_bias, conv_weight, conv_bias, x_weight, dt_weight, d_skip)
    corrupt_out = mixer_run(corrupt_proj, a_log, dt_bias, conv_weight, conv_bias, x_weight, dt_weight, d_skip)
    clean_out, corrupt_out = lax.optimization_barrier((clean_out, corrupt_out))
    clean_f = clean_out.astype(jnp.float32)
    corrupt_f = corrupt_out.astype(jnp.float32)
    normalizer = lax.optimization_barrier(jnp.sum((clean_f - corrupt_f) ** 2, axis=0))
    spread = jnp.sqrt(normalizer / SEQ + 1e-06)
    positions = jnp.arange(SEQ, dtype=jnp.int32)
    columns = jnp.arange(2 * INNER, dtype=jnp.int32)

    def variant(payload):
        targets, chosen_mode = payload
        hit_rows = jnp.any(positions[:, None] == targets[None, :], axis=1)
        take_signal = (hit_rows & (chosen_mode != 1))[:, None] & (columns < INNER)[None, :]
        take_gate = (hit_rows & (chosen_mode != 0))[:, None] & (columns >= INNER)[None, :]
        patched_in = jnp.where(take_signal | take_gate, clean_proj, corrupt_proj)
        patched = mixer_run(patched_in, a_log, dt_bias, conv_weight, conv_bias, x_weight, dt_weight, d_skip)
        patched = lax.optimization_barrier(patched)
        peak = lax.optimization_barrier(jnp.max(jnp.abs(patched.astype(jnp.float32) - corrupt_f), axis=0)) / spread
        return (patched, peak)
    patched_out, effect_peak = lax.map(variant, (patch_pos, patch_mode))
    return (patched_out, effect_peak)
```

```python
import functools

import jax
import jax.numpy as jnp
from jax import lax
from jax.experimental import pallas as pl
from jax.experimental.pallas import tpu as pltpu
from jax.sharding import PartitionSpec as P

STATE = 16
RANK = 160
ROWS = 32
INNER = 5120
SPAN = 1280
TAPS = 4
LANES = 128
CHUNKS = 64
SHARDS = 64
VARS = 4
TILES = INNER // LANES
CUT_TILES = SPAN // LANES
GROUPS = CHUNKS // 8
MESH = pl.DeviceIdType.MESH
LOG2E = 1.4426950408889634
TINY = 1e-06
F32 = jnp.float32
BF16 = jnp.bfloat16
LINK = jnp.float32
CLEAN, CORRUPT, PATCHED = 0, 1, 2


def cut_slot(run, tile):
    if tile < 8:
        return TILES + 8 * run + tile
    return 56 + 2 * run + (tile - 8)


def hit_rows(pos_ref, first, count):
    rows = first + lax.broadcasted_iota(jnp.int32, (count, LANES), 0)
    hits = rows == pos_ref[0, 0]
    for k in range(1, pos_ref.shape[1]):
        hits = hits | (rows == pos_ref[0, k])
    return hits


def silu(value):
    return value / (1.0 + jnp.exp(-value))


def softplus(value):
    return jnp.maximum(value, 0.0) + jnp.log1p(jnp.exp(-jnp.abs(value)))


def row_of(ref, row):
    return jnp.broadcast_to(ref[pl.ds(row, 1), :], (8, LANES))


def scan_group(dts, us, rate, group, state, drive, readout, out):
    def step(t, carry):
        row = pl.multiple_of(t * CHUNKS + group * 8, 8)
        steps = dts[pl.ds(row, 8), :]
        flow = us[pl.ds(row, 8), :]
        entries = []
        total = None
        for n in range(STATE):
            decay = jnp.exp2(steps * rate[n])
            entry = decay * carry[n] + flow * drive(t, n)
            entries.append(entry)
            if readout is not None:
                term = readout(t, n) * entry
                total = term if total is None else total + term
        if readout is not None:
            out[pl.ds(row, 8), :] = total
            return tuple(entries)
        return (*entries, carry[STATE] + steps)

    return lax.fori_loop(0, ROWS, step, state)


def splat_reader(ref, base):
    return lambda t, n: row_of(ref, base + t * STATE + n)


def mixed_reader(ref):
    first = lax.broadcasted_iota(jnp.int32, (8, LANES), 0) < 2

    def read(t, n):
        return jnp.where(
            first,
            row_of(ref, CLEAN * ROWS * STATE + t * STATE + n),
            row_of(ref, CORRUPT * ROWS * STATE + t * STATE + n),
        )

    return read


def front_kernel(
    pos, mode, clean, corrupt, rims, conv_w, conv_b, x_w, dt_w, dt_b, a_log,
    ends, totals, rates, dts, us, bs, cs, acts, pad, low,
):
    v = lax.axis_index("var")
    first = lax.axis_index("seq") * ROWS
    take = hit_rows(pos, first, ROWS)[:, :1] & (mode[0] != 1)
    take_rim = hit_rows(pos, first - 8, 8)[:, :1] & (mode[0] != 1)

    width = 512

    def conv(i, _):
        cols = pl.ds(pl.multiple_of(i * width, width), width)
        sig_clean = clean[:, cols].astype(F32)
        sig_corrupt = corrupt[:, cols].astype(F32)
        rim_clean = rims[0, :, cols].astype(F32)
        rim_corrupt = rims[1, :, cols].astype(F32)
        pieces = (
            (rim_clean, sig_clean),
            (rim_corrupt, sig_corrupt),
            (
                jnp.where(take_rim, rim_clean, rim_corrupt),
                jnp.where(take, sig_clean, sig_corrupt),
            ),
        )
        bias = conv_b[:, cols]
        for run, (rim, sig) in enumerate(pieces):
            pad[run, 0:8, :] = rim
            pad[run, 8:, :] = sig
            total = bias + conv_w[0:1, cols] * pad[run, 5 : 5 + ROWS, :]
            for k in range(1, TAPS):
                total = total + conv_w[k : k + 1, cols] * pad[run, 5 + k : 5 + k + ROWS, :]
            acts[run * ROWS : (run + 1) * ROWS, cols] = silu(total).astype(BF16)
        return 0

    lax.fori_loop(0, INNER // width, conv, 0)

    projected = jnp.dot(acts[...], x_w[...], preferred_element_type=F32)
    low[...] = projected[:, :RANK].astype(BF16)
    for run in range(3):
        mine = projected[run * ROWS : (run + 1) * ROWS]
        for n in range(STATE):
            at = run * ROWS * STATE + n
            bs[pl.ds(at, ROWS, stride=STATE), :] = jnp.broadcast_to(
                mine[:, RANK + n : RANK + n + 1], (ROWS, LANES)
            )
            cs[pl.ds(at, ROWS, stride=STATE), :] = jnp.broadcast_to(
                mine[:, RANK + STATE + n : RANK + STATE + n + 1], (ROWS, LANES)
            )

    def place(slot, steps, act, log_rate):
        dts[pl.ds(slot, ROWS, stride=CHUNKS), :] = steps
        us[pl.ds(slot, ROWS, stride=CHUNKS), :] = steps * act
        at = (slot // 8) * (STATE * 8) + slot % 8
        rates[pl.ds(at, STATE, stride=8), :] = jnp.exp(log_rate) * (-LOG2E)

    wide = 640

    def patched_steps(i, _):
        start = pl.multiple_of(i * wide, wide)
        cols = pl.ds(start, wide)
        raw = jnp.dot(low[2 * ROWS :, :], dt_w[:, cols], preferred_element_type=F32)
        steps = softplus(raw + dt_b[:, cols])
        act = acts[2 * ROWS :, cols].astype(F32)
        logs = a_log[:, cols]
        for k in range(wide // LANES):
            part = slice(k * LANES, (k + 1) * LANES)
            place(i * (wide // LANES) + k, steps[:, part], act[:, part], logs[:, part])
        return 0

    lax.fori_loop(0, INNER // wide, patched_steps, 0)

    cols = pl.ds(pl.multiple_of(v * SPAN, LANES), SPAN)
    raw = jnp.dot(low[: 2 * ROWS, :], dt_w[:, cols], preferred_element_type=F32)
    steps = softplus(raw + dt_b[:, cols])
    act = acts[: 2 * ROWS, cols].astype(F32)
    logs = a_log[:, cols]
    for run in (CLEAN, CORRUPT):
        rows = slice(run * ROWS, (run + 1) * ROWS)
        for tile in range(CUT_TILES):
            part = slice(tile * LANES, (tile + 1) * LANES)
            place(cut_slot(run, tile), steps[rows, part], act[rows, part], logs[:, part])
    blank = jnp.zeros((ROWS, LANES), F32)
    for slot in range(60, CHUNKS):
        place(slot, blank, blank, jnp.zeros((STATE, LANES), F32))

    zero = jnp.zeros((8, LANES), F32)

    def one_group(group, drive):
        base = group * (STATE * 8)
        rate = [rates[pl.ds(pl.multiple_of(base + n * 8, 8), 8), :] for n in range(STATE)]
        found = scan_group(dts, us, rate, group, (zero,) * (STATE + 1), drive, None, None)
        for n in range(STATE):
            ends[pl.ds(base + n, 8, stride=STATE), :] = found[n]
        totals[pl.ds(pl.multiple_of(group * 8, 8), 8), :] = found[STATE]

    def plain(group, _):
        run = jnp.where(group < 5, PATCHED, group - 5)
        one_group(group, splat_reader(bs, run * (ROWS * STATE)))
        return 0

    lax.fori_loop(0, GROUPS - 1, plain, 0)
    one_group(GROUPS - 1, mixed_reader(bs))


def wait_for(ref, sem):
    pltpu.make_async_copy(ref, ref, sem).wait()


def exchange_kernel(
    ends, totals, rate, incoming,
    got_ends, got_totals, leaving, landed, send_a, send_b, send_c, recv_a, recv_b, recv_c,
):
    me = lax.axis_index("seq")
    v = lax.axis_index("var")

    barrier = pltpu.get_barrier_semaphore()

    def greet(k, _):
        peer = lax.rem(me + k, SHARDS)
        pl.semaphore_signal(barrier, inc=1, device_id=(peer, v), device_id_type=MESH)
        return 0

    lax.fori_loop(1, SHARDS, greet, 0)
    own_a = pltpu.make_async_copy(ends.at[me], got_ends.at[me], recv_a)
    own_b = pltpu.make_async_copy(totals.at[me], got_totals.at[me], recv_b)
    own_a.start()
    own_b.start()
    pl.semaphore_wait(barrier, SHARDS - 1)

    def send(k, _):
        peer = lax.rem(me + k, SHARDS)
        pltpu.make_async_remote_copy(
            src_ref=ends.at[peer], dst_ref=got_ends.at[me], send_sem=send_a, recv_sem=recv_a,
            device_id=(peer, v), device_id_type=MESH,
        ).start()
        pltpu.make_async_remote_copy(
            src_ref=totals.at[peer], dst_ref=got_totals.at[me], send_sem=send_b, recv_sem=recv_b,
            device_id=(peer, v), device_id_type=MESH,
        ).start()
        return 0

    lax.fori_loop(1, SHARDS, send, 0)
    wait_for(got_totals, recv_b)
    wait_for(got_ends, recv_a)

    def chain(s, state):
        leaving[s] = state.astype(LINK)
        return jnp.exp2(rate[...] * got_totals[s]) * state + got_ends[s].astype(F32)

    lax.fori_loop(0, SHARDS, chain, jnp.zeros((STATE, LANES), F32), unroll=4)

    own_c = pltpu.make_async_copy(leaving.at[me], landed.at[me], recv_c)
    own_c.start()

    def give(k, _):
        peer = lax.rem(me + k, SHARDS)
        pltpu.make_async_remote_copy(
            src_ref=leaving.at[peer], dst_ref=landed.at[me], send_sem=send_c, recv_sem=recv_c,
            device_id=(peer, v), device_id_type=MESH,
        ).start()
        return 0

    lax.fori_loop(1, SHARDS, give, 0)
    others = pl.ds(0, SHARDS - 1)
    wait_for(ends.at[others], send_a)
    wait_for(totals.at[others], send_b)
    wait_for(leaving.at[others], send_c)
    wait_for(landed, recv_c)
    incoming[...] = landed[...]


def back_kernel(
    pos, mode, clean_gate, corrupt_gate, d_skip, incoming, rates, dts, us, bs, cs, acts,
    patched, cut, squares, start, ys,
):
    v = lax.axis_index("var")
    first = lax.axis_index("seq") * ROWS
    take = hit_rows(pos, first, ROWS)[:, :1] & (mode[0] != 0)

    def widen(c, _):
        start[pl.ds(pl.multiple_of(c * STATE, STATE), STATE), :] = incoming[c].astype(F32)
        return 0

    lax.fori_loop(0, CHUNKS, widen, 0, unroll=4)

    def one_group(group, drive, readout):
        base = group * (STATE * 8)
        rate = [rates[pl.ds(pl.multiple_of(base + n * 8, 8), 8), :] for n in range(STATE)]
        state = tuple(start[pl.ds(base + n, 8, stride=STATE), :] for n in range(STATE))
        scan_group(dts, us, rate, group, state, drive, readout, ys)

    def plain(group, _):
        run = jnp.where(group < 5, PATCHED, group - 5) * (ROWS * STATE)
        one_group(group, splat_reader(bs, run), splat_reader(cs, run))
        return 0

    lax.fori_loop(0, GROUPS - 1, plain, 0)
    one_group(GROUPS - 1, mixed_reader(bs), mixed_reader(cs))

    def result(slot, act, skip, gate):
        y = ys[pl.ds(slot, ROWS, stride=CHUNKS), :]
        return ((y + skip * act) * silu(gate)).astype(BF16)

    for tile in range(CUT_TILES):
        cols = pl.ds(pl.multiple_of(v * SPAN + tile * LANES, LANES), LANES)
        skip = d_skip[:, cols]
        clean_out = result(
            cut_slot(CLEAN, tile), acts[:ROWS, cols].astype(F32), skip,
            clean_gate[:, cols].astype(F32),
        )
        corrupt_out = result(
            cut_slot(CORRUPT, tile), acts[ROWS : 2 * ROWS, cols].astype(F32), skip,
            corrupt_gate[:, cols].astype(F32),
        )
        cut[:, tile * LANES : (tile + 1) * LANES] = corrupt_out
        gap = clean_out.astype(F32) - corrupt_out.astype(F32)
        squares[tile] = jnp.sum(gap * gap, axis=0, keepdims=True)

    def patched_tile(tile, _):
        cols = pl.ds(pl.multiple_of(tile * LANES, LANES), LANES)
        gate = jnp.where(take, clean_gate[:, cols].astype(F32), corrupt_gate[:, cols].astype(F32))
        patched[:, cols] = result(tile, acts[2 * ROWS :, cols].astype(F32), d_skip[:, cols], gate)
        return 0

    lax.fori_loop(0, TILES, patched_tile, 0, unroll=2)


def tail_kernel(
    cut, patched, squares, effect,
    whole, peaks, got_squares, spread, got_peaks, answer, answers,
    send_cut, send_sq, send_pk, send_sp, send_an, recv_cut, recv_sq, recv_pk, recv_sp, recv_an,
):
    me = lax.axis_index("seq")
    v = lax.axis_index("var")
    barrier = pltpu.get_barrier_semaphore()

    def greet(k, _):
        peer = lax.rem(me + k, SHARDS)
        pl.semaphore_signal(barrier, inc=1, device_id=(peer, v), device_id_type=MESH)
        return 0

    lax.fori_loop(1, SHARDS, greet, 0)
    for k in range(1, VARS):
        pl.semaphore_signal(
            barrier, inc=1, device_id=(me, lax.rem(v + k, VARS)), device_id_type=MESH
        )
    pl.semaphore_wait(barrier, SHARDS - 1 + VARS - 1)

    def to_variant(k, src, dst, send_sem, recv_sem):
        return pltpu.make_async_remote_copy(
            src_ref=src, dst_ref=dst, send_sem=send_sem, recv_sem=recv_sem,
            device_id=(me, lax.rem(v + k, VARS)), device_id_type=MESH,
        )

    def to_shard(peer, src, dst, send_sem, recv_sem):
        return pltpu.make_async_remote_copy(
            src_ref=src, dst_ref=dst, send_sem=send_sem, recv_sem=recv_sem,
            device_id=(peer, v), device_id_type=MESH,
        )

    for k in range(1, VARS):
        to_variant(k, cut, whole.at[v], send_cut.at[k], recv_cut.at[k]).start()

    def send_square(i, _):
        peer = v * CUT_TILES + i

        @pl.when(peer != me)
        def _():
            to_shard(
                peer, squares.at[i], got_squares.at[me], send_sq.at[i], recv_sq
            ).start()

        @pl.when(peer == me)
        def _():
            pltpu.make_async_copy(squares.at[i], got_squares.at[me], recv_sq).start()

        return 0

    lax.fori_loop(0, CUT_TILES, send_square, 0)
    whole[v] = cut[...]
    for k in range(1, VARS):
        to_variant(k, cut, whole.at[lax.rem(v + VARS - k, VARS)], send_cut.at[k], recv_cut.at[k]).wait()

    for w in range(VARS):
        def peak_tile(i, _):
            here = pl.ds(pl.multiple_of(i * LANES, LANES), LANES)
            there = pl.ds(pl.multiple_of(w * SPAN + i * LANES, LANES), LANES)
            gap = jnp.abs(patched[:, there].astype(F32) - whole[w, :, here].astype(F32))
            peaks[w * CUT_TILES + i] = jnp.max(gap, axis=0, keepdims=True)
            return 0

        lax.fori_loop(0, CUT_TILES, peak_tile, 0, unroll=2)

    def send_peak(c, _):
        @pl.when(c != me)
        def _():
            to_shard(c, peaks.at[c], got_peaks.at[me], send_pk.at[c], recv_pk).start()

        @pl.when(c == me)
        def _():
            pltpu.make_async_copy(peaks.at[c], got_peaks.at[me], recv_pk).start()

        return 0

    lax.fori_loop(0, TILES, send_peak, 0)

    owner = lax.div(me, CUT_TILES)

    @pl.when(owner == v)
    def _():
        wait_for(got_squares, recv_sq)
        total = jnp.sum(got_squares[...], axis=0)
        spread[...] = jnp.sqrt(total / (SHARDS * ROWS) + TINY)
        for k in range(1, VARS):
            to_variant(k, spread, spread, send_sp.at[k], recv_sp).start()

    @pl.when((owner != v) & (me < TILES))
    def _():
        wait_for(spread, recv_sp)

    @pl.when(me < TILES)
    def _():
        wait_for(got_peaks, recv_pk)
        answer[...] = jnp.max(got_peaks[...], axis=0) / spread[...]
        pltpu.make_async_copy(answer, answers.at[me], recv_an).start()

        def share(k, _):
            peer = lax.rem(me + k, SHARDS)
            to_shard(peer, answer, answers.at[me], send_an.at[k], recv_an).start()
            return 0

        lax.fori_loop(1, SHARDS, share, 0)

    wait_for(answers, recv_an)
    for c in range(TILES):
        effect[:, c * LANES : (c + 1) * LANES] = answers[c]

    @pl.when(me < TILES)
    def _():
        def done(k, _):
            peer = lax.rem(me + k, SHARDS)
            to_shard(peer, answer, answers.at[me], send_an.at[k], recv_an).wait_send()
            return 0

        lax.fori_loop(1, SHARDS, done, 0)

    @pl.when(owner == v)
    def _():
        for k in range(1, VARS):
            to_variant(k, spread, spread, send_sp.at[k], recv_sp).wait_send()

    def sent_peak(c, _):
        @pl.when(c != me)
        def _():
            to_shard(c, peaks.at[c], got_peaks.at[me], send_pk.at[c], recv_pk).wait_send()

        return 0

    lax.fori_loop(0, TILES, sent_peak, 0)

    def sent_square(i, _):
        peer = v * CUT_TILES + i

        @pl.when(peer != me)
        def _():
            to_shard(
                peer, squares.at[i], got_squares.at[me], send_sq.at[i], recv_sq
            ).wait_send()

        return 0

    lax.fori_loop(0, CUT_TILES, sent_square, 0)


VMEM = pl.BlockSpec(memory_space=pltpu.VMEM)
SMEM = pl.BlockSpec(memory_space=pltpu.SMEM)
DMA = pltpu.SemaphoreType.DMA
LIMIT = 40 * 1024 * 1024


def shape(dims, kind):
    return jax.ShapeDtypeStruct(dims, kind)


def half(which):
    return pl.BlockSpec((ROWS, INNER), lambda i: (0, which))


def shards(
    clean_proj, corrupt_proj, patch_pos, patch_mode, a_log, dt_bias,
    conv_weight, conv_bias, x_weight, dt_weight, d_skip,
):
    me = lax.axis_index("seq")
    v = lax.axis_index("var")
    tails = jnp.stack([clean_proj[ROWS - 8 :, :INNER], corrupt_proj[ROWS - 8 :, :INNER]])
    rims = lax.ppermute(tails, "seq", [(s, s + 1) for s in range(SHARDS - 1)])

    ends, totals, rates, dts, us, bs, cs, acts = pl.pallas_call(
        front_kernel,
        out_shape=(
            shape((CHUNKS * STATE, LANES), F32),
            shape((CHUNKS, LANES), F32),
            shape((GROUPS * STATE * 8, LANES), F32),
            shape((ROWS * CHUNKS, LANES), F32),
            shape((ROWS * CHUNKS, LANES), F32),
            shape((3 * ROWS * STATE, LANES), F32),
            shape((3 * ROWS * STATE, LANES), F32),
            shape((3 * ROWS, INNER), BF16),
        ),
        grid=(1,),
        in_specs=[SMEM, SMEM, half(0), half(0)] + [VMEM] * 7,
        out_specs=(VMEM,) * 8,
        scratch_shapes=[
            pltpu.VMEM((3, 8 + ROWS, 512), F32),
            pltpu.VMEM((3 * ROWS, RANK), BF16),
        ],
        compiler_params=pltpu.CompilerParams(vmem_limit_bytes=LIMIT),
        name="front",
    )(
        patch_pos, patch_mode, clean_proj, corrupt_proj, rims, conv_weight,
        conv_bias[None], x_weight, dt_weight, dt_bias[None], a_log,
    )

    ends = ends.reshape(CHUNKS, STATE, LANES).astype(LINK)
    totals = totals.reshape(CHUNKS, 1, LANES)
    place = jnp.where(me < 56, me - 8 * (me >= 48) - 40, jnp.where(me < 58, me - 48, me - 50))
    tile = jnp.where(me < TILES, me, jnp.where(me < 60, v * CUT_TILES + place, 0))
    rate = jnp.exp(lax.dynamic_slice_in_dim(a_log, tile * LANES, LANES, 1)) * (-LOG2E)
    incoming = pl.pallas_call(
        exchange_kernel,
        out_shape=shape((CHUNKS, STATE, LANES), LINK),
        in_specs=[VMEM] * 3,
        out_specs=VMEM,
        scratch_shapes=[
            pltpu.VMEM((SHARDS, STATE, LANES), LINK),
            pltpu.VMEM((SHARDS, 1, LANES), F32),
            pltpu.VMEM((SHARDS, STATE, LANES), LINK),
            pltpu.VMEM((CHUNKS, STATE, LANES), LINK),
        ]
        + [DMA] * 6,
        compiler_params=pltpu.CompilerParams(
            collective_id=0, has_side_effects=True, vmem_limit_bytes=16 * 1024 * 1024
        ),
        name="exchange",
    )(ends, totals, rate)

    patched, cut, squares = pl.pallas_call(
        back_kernel,
        out_shape=(
            shape((ROWS, INNER), BF16),
            shape((ROWS, SPAN), BF16),
            shape((CUT_TILES, 1, LANES), F32),
        ),
        grid=(1,),
        in_specs=[SMEM, SMEM, half(1), half(1)] + [VMEM] * 8,
        out_specs=(VMEM,) * 3,
        scratch_shapes=[
            pltpu.VMEM((CHUNKS * STATE, LANES), F32),
            pltpu.VMEM((ROWS * CHUNKS, LANES), F32),
        ],
        compiler_params=pltpu.CompilerParams(vmem_limit_bytes=LIMIT),
        name="back",
    )(
        patch_pos, patch_mode, clean_proj, corrupt_proj, d_skip[None], incoming, rates,
        dts, us, bs, cs, acts,
    )

    effect = pl.pallas_call(
        tail_kernel,
        out_shape=shape((1, INNER), F32),
        in_specs=[VMEM] * 3,
        out_specs=VMEM,
        scratch_shapes=[
            pltpu.VMEM((VARS, ROWS, SPAN), BF16),
            pltpu.VMEM((TILES, 1, LANES), F32),
            pltpu.VMEM((SHARDS, 1, LANES), F32),
            pltpu.VMEM((1, LANES), F32),
            pltpu.VMEM((SHARDS, 1, LANES), F32),
            pltpu.VMEM((1, LANES), F32),
            pltpu.VMEM((TILES, 1, LANES), F32),
            DMA((VARS,)),
            DMA((CUT_TILES,)),
            DMA((TILES,)),
            DMA((VARS,)),
            DMA((SHARDS,)),
            DMA((VARS,)),
            DMA,
            DMA,
            DMA,
            DMA,
        ],
        compiler_params=pltpu.CompilerParams(
            collective_id=1, has_side_effects=True, vmem_limit_bytes=16 * 1024 * 1024
        ),
        name="tail",
    )(cut, patched, squares)
    return (patched[None], effect)


def solution(mesh):
    return jax.shard_map(
        shards,
        mesh=mesh,
        in_specs=(
            P("seq", None), P("seq", None), P("var", None), P("var"),
            P(), P(), P(), P(), P(), P(), P(),
        ),
        out_specs=(P("var", "seq", None), P("var", None)),
        check_vma=False,
    )
```

```python
import functools

import jax
import jax.numpy as jnp
from jax import lax
from jax.experimental import pallas as pl
from jax.experimental.pallas import tpu as pltpu
from jax.sharding import PartitionSpec as P

STATE = 16
RANK = 160
ROWS = 32
INNER = 5120
SPAN = 1280
TAPS = 4
LANES = 128
CHUNKS = 64
SHARDS = 64
VARS = 4
TILES = INNER // LANES
CUT_TILES = SPAN // LANES
GROUPS = CHUNKS // 8
HALF = CHUNKS // 2
CHIPS = SHARDS // 2
PITCH = 72
SPLAT = 17
MESH = pl.DeviceIdType.MESH
LOG2E = 1.4426950408889634
TINY = 1e-06
F32 = jnp.float32
BF16 = jnp.bfloat16
UNROLL = 4
CLEAN, CORRUPT, PATCHED = 0, 1, 2


def cut_slot(run, tile):
    if tile < 8:
        return TILES + 8 * run + tile
    return 56 + 2 * run + (tile - 8)


def hit_rows(pos_ref, first, count):
    rows = first + lax.broadcasted_iota(jnp.int32, (count, LANES), 0)
    hits = rows == pos_ref[0, 0]
    for k in range(1, pos_ref.shape[1]):
        hits = hits | (rows == pos_ref[0, k])
    return hits


def silu(value):
    return value / (1.0 + jnp.exp(-value))


def softplus(value):
    return jnp.maximum(value, 0.0) + jnp.log1p(jnp.exp(-jnp.abs(value)))


def row_of(ref, row):
    return jnp.broadcast_to(ref[pl.ds(row, 1), :], (8, LANES))


def scan_group(dts, us, rate, group, state, drive, readout, out):
    def step(t, carry):
        row = pl.multiple_of(t * PITCH + group * 8, 8)
        steps = dts[pl.ds(row, 8), :]
        flow = us[pl.ds(row, 8), :]
        entries = []
        total = None
        for n in range(STATE):
            decay = jnp.exp2(steps * rate[n])
            entry = decay * carry[n] + flow * drive(t, n)
            entries.append(entry)
            if readout is not None:
                term = readout(t, n) * entry
                total = term if total is None else total + term
        if readout is not None:
            out[pl.ds(row, 8), :] = total
        return tuple(entries)

    return lax.fori_loop(0, ROWS, step, state, unroll=UNROLL)


def splat_reader(ref, base):
    return lambda t, n: row_of(ref, base + t * SPLAT + n)


def mixed_reader(ref):
    first = lax.broadcasted_iota(jnp.int32, (8, LANES), 0) < 2

    def read(t, n):
        return jnp.where(
            first,
            row_of(ref, CLEAN * ROWS * SPLAT + t * SPLAT + n),
            row_of(ref, CORRUPT * ROWS * SPLAT + t * SPLAT + n),
        )

    return read


def wait_for(ref, sem):
    pltpu.make_async_copy(ref, ref, sem).wait()


def kernel(
    pos, mode, clean_in, corrupt_in, rims_in, conv_w_in, conv_b_in, x_w_in, dt_w_in, dt_b_in,
    a_log_in, d_skip_in,
    patched, effect,
    clean, corrupt, rims, conv_w, conv_b, x_w, dt_w, dt_b, a_log, d_skip,
    pad, acts, low, dts, us, bs, cs, rates, ends, totals,
    pair_ends, pair_totals, chip_ends, chip_totals, got_ends, got_totals,
    leaving, landed, across, start, ys,
    cut, squares, whole, peaks, got_squares, spread, got_peaks, answer, answers,
    load_sem, send_pt, recv_pt, send_pe, recv_pe, send_ct, recv_ct, send_ce, recv_ce,
    send_in, recv_in, send_st, recv_st,
    send_cut, send_sq, send_pk, send_sp, send_an, recv_cut, recv_sq, recv_pk, recv_sp, recv_an,
):
    me = lax.axis_index("seq")
    v = lax.axis_index("var")
    chip = lax.div(me, 2)
    core = lax.rem(me, 2)
    mate = me + 1 - 2 * core
    mine = core * HALF
    theirs = HALF - mine
    barrier = pltpu.get_barrier_semaphore()

    loads = [
        pltpu.make_async_copy(src, dst, load_sem.at[i])
        for i, (src, dst) in enumerate(
            (
                (clean_in, clean), (corrupt_in, corrupt), (rims_in, rims), (conv_w_in, conv_w),
                (conv_b_in, conv_b), (x_w_in, x_w), (dt_w_in, dt_w), (dt_b_in, dt_b),
                (a_log_in, a_log), (d_skip_in, d_skip),
            )
        )
    ]
    for load in loads:
        load.start()

    def greet(k, _):
        peer = lax.rem(me + k, SHARDS)
        pl.semaphore_signal(barrier, inc=1, device_id=(peer, v), device_id_type=MESH)
        return 0

    lax.fori_loop(1, SHARDS, greet, 0)
    for k in range(1, VARS):
        pl.semaphore_signal(
            barrier, inc=1, device_id=(me, lax.rem(v + k, VARS)), device_id_type=MESH
        )

    def to_variant(k, src, dst, send_sem, recv_sem):
        return pltpu.make_async_remote_copy(
            src_ref=src, dst_ref=dst, send_sem=send_sem, recv_sem=recv_sem,
            device_id=(me, lax.rem(v + k, VARS)), device_id_type=MESH,
        )

    def to_shard(peer, src, dst, send_sem, recv_sem):
        return pltpu.make_async_remote_copy(
            src_ref=src, dst_ref=dst, send_sem=send_sem, recv_sem=recv_sem,
            device_id=(peer, v), device_id_type=MESH,
        )

    first = me * ROWS
    hits = hit_rows(pos, first, ROWS)[:, :1]
    take = hits & (mode[0] != 1)
    take_gate = hits & (mode[0] != 0)
    take_rim = hit_rows(pos, first - 8, 8)[:, :1] & (mode[0] != 1)

    for load in loads[:5]:
        load.wait()
    width = 512

    def conv(i, _):
        cols = pl.ds(pl.multiple_of(i * width, width), width)
        sig_clean = clean[:, cols].astype(F32)
        sig_corrupt = corrupt[:, cols].astype(F32)
        rim_clean = rims[0:8, cols].astype(F32)
        rim_corrupt = rims[8:16, cols].astype(F32)
        pieces = (
            (rim_clean, sig_clean),
            (rim_corrupt, sig_corrupt),
            (
                jnp.where(take_rim, rim_clean, rim_corrupt),
                jnp.where(take, sig_clean, sig_corrupt),
            ),
        )
        bias = conv_b[:, cols]
        for run, (rim, sig) in enumerate(pieces):
            pad[run, 0:8, :] = rim
            pad[run, 8:, :] = sig
            total = bias + conv_w[0:1, cols] * pad[run, 5 : 5 + ROWS, :]
            for k in range(1, TAPS):
                total = total + conv_w[k : k + 1, cols] * pad[run, 5 + k : 5 + k + ROWS, :]
            acts[run * ROWS : (run + 1) * ROWS, cols] = silu(total).astype(BF16)
        return 0

    lax.fori_loop(0, INNER // width, conv, 0)

    loads[5].wait()
    projected = lax.dot_general(
        acts[...], x_w[...], (((1,), (1,)), ((), ())), preferred_element_type=F32
    )
    low[...] = projected[:, :RANK].astype(BF16)
    for run in range(3):
        part = projected[run * ROWS : (run + 1) * ROWS]
        for n in range(STATE):
            at = run * ROWS * SPLAT + n
            bs[pl.ds(at, ROWS, stride=SPLAT), :] = jnp.broadcast_to(
                part[:, RANK + n : RANK + n + 1], (ROWS, LANES)
            )
            cs[pl.ds(at, ROWS, stride=SPLAT), :] = jnp.broadcast_to(
                part[:, RANK + STATE + n : RANK + STATE + n + 1], (ROWS, LANES)
            )

    for load in loads[6:9]:
        load.wait()

    def rate_at(slot):
        return pl.ds(lax.div(slot, 8) * (STATE * 8) + lax.rem(slot, 8), STATE, stride=8)

    def place(slot, steps, act, log_rate):
        dts[pl.ds(slot, ROWS, stride=PITCH), :] = steps
        us[pl.ds(slot, ROWS, stride=PITCH), :] = steps * act
        totals[slot] = jnp.sum(steps, axis=0, keepdims=True)
        rates[rate_at(slot), :] = jnp.exp(log_rate) * (-LOG2E)

    wide = 640

    def patched_steps(i, _):
        cols = pl.ds(pl.multiple_of(i * wide, wide), wide)
        raw = jnp.dot(low[2 * ROWS :, :], dt_w[:, cols], preferred_element_type=F32)
        steps = softplus(raw + dt_b[:, cols])
        act = acts[2 * ROWS :, cols].astype(F32)
        logs = a_log[:, cols]
        for k in range(wide // LANES):
            part = slice(k * LANES, (k + 1) * LANES)
            place(i * (wide // LANES) + k, steps[:, part], act[:, part], logs[:, part])
        return 0

    lax.fori_loop(0, INNER // wide, patched_steps, 0)

    cols = pl.ds(pl.multiple_of(v * SPAN, LANES), SPAN)
    raw = jnp.dot(low[: 2 * ROWS, :], dt_w[:, cols], preferred_element_type=F32)
    steps = softplus(raw + dt_b[:, cols])
    act = acts[: 2 * ROWS, cols].astype(F32)
    logs = a_log[:, cols]
    for run in (CLEAN, CORRUPT):
        rows = slice(run * ROWS, (run + 1) * ROWS)
        for tile in range(CUT_TILES):
            part = slice(tile * LANES, (tile + 1) * LANES)
            place(cut_slot(run, tile), steps[rows, part], act[rows, part], logs[:, part])
    blank = jnp.zeros((ROWS, LANES), F32)
    for slot in range(60, CHUNKS):
        place(slot, blank, blank, jnp.zeros((STATE, LANES), F32))

    pl.semaphore_wait(barrier, SHARDS - 1 + VARS - 1)
    theirs_3 = pl.ds(theirs, HALF)
    swap_totals = to_shard(mate, totals.at[theirs_3], pair_totals, send_pt, recv_pt)
    swap_totals.start()

    zero = jnp.zeros((8, LANES), F32)

    def rates_of(group):
        base = group * (STATE * 8)
        return [rates[pl.ds(pl.multiple_of(base + n * 8, 8), 8), :] for n in range(STATE)]

    def run_base(group):
        return jnp.where(group < 5, PATCHED, group - 5) * (ROWS * SPLAT)

    def local_group(group, drive):
        found = scan_group(
            dts, us, rates_of(group), group, (zero,) * STATE, drive, None, None
        )
        for n in range(STATE):
            ends[pl.ds(group * (STATE * 8) + n, 8, stride=STATE), :] = found[n]

    def local_pass(offset):
        def body(i, _):
            group = offset + i

            @pl.when(group < GROUPS - 1)
            def _():
                local_group(group, splat_reader(bs, run_base(group)))

            @pl.when(group == GROUPS - 1)
            def _():
                local_group(group, mixed_reader(bs))

            return 0

        lax.fori_loop(0, GROUPS // 2, body, 0)

    local_pass(lax.div(theirs, 8))
    theirs_2 = pl.ds(pl.multiple_of(theirs * STATE, 8), HALF * STATE)
    swap_ends = to_shard(mate, ends.at[theirs_2], pair_ends, send_pe, recv_pe)
    swap_ends.start()
    local_pass(lax.div(mine, 8))
    swap_totals.wait()
    leads = core == 0

    def my_summary(k):
        own = ends[pl.ds(pl.multiple_of((mine + k) * STATE, 8), STATE), :]
        return own, totals[mine + k]

    def pair_of(k):
        own_end, own_total = my_summary(k)
        other_end = pair_ends[pl.ds(pl.multiple_of(k * STATE, 8), STATE), :]
        other_total = pair_totals[k]
        return (
            jnp.where(leads, own_end, other_end), jnp.where(leads, own_total, other_total),
            jnp.where(leads, other_end, own_end), jnp.where(leads, other_total, own_total),
        )

    def chip_total(k, _):
        chip_totals[k] = totals[mine + k] + pair_totals[k]
        return 0

    lax.fori_loop(0, HALF, chip_total, 0, unroll=4)
    swap_ends.wait()

    def chip_end(k, _):
        end_a, total_a, end_b, total_b = pair_of(k)
        chip_ends[k] = jnp.exp2(rates[rate_at(mine + k), :] * total_b) * end_a + end_b
        return 0

    lax.fori_loop(0, HALF, chip_end, 0, unroll=4)
    pltpu.make_async_copy(chip_totals.at[chip], got_totals.at[chip], recv_ct).start()
    pltpu.make_async_copy(chip_ends.at[chip], got_ends.at[chip], recv_ce).start()

    def spread_out(k, _):
        peer = lax.rem(chip + k, CHIPS)
        target = 2 * peer + core
        to_shard(target, chip_ends.at[peer], got_ends.at[chip], send_ce, recv_ce).start()
        to_shard(target, chip_totals.at[peer], got_totals.at[chip], send_ct, recv_ct).start()
        return 0

    lax.fori_loop(1, CHIPS, spread_out, 0)
    my_rate = rates[rate_at(mine + chip), :]
    wait_for(got_totals, recv_ct)
    wait_for(got_ends, recv_ce)

    def chain(s, state):
        leaving[s] = state
        return jnp.exp2(my_rate * got_totals[s]) * state + got_ends[s]

    lax.fori_loop(0, CHIPS, chain, jnp.zeros((STATE, LANES), F32), unroll=4)
    pltpu.make_async_copy(leaving.at[chip], landed.at[chip], recv_in).start()

    def give(k, _):
        peer = lax.rem(chip + k, CHIPS)
        to_shard(2 * peer + core, leaving.at[peer], landed.at[chip], send_in, recv_in).start()
        return 0

    lax.fori_loop(1, CHIPS, give, 0)
    wait_for(landed, recv_in)

    def enter(k, _):
        end_a, total_a, _, _ = pair_of(k)
        before = landed[k]
        after = jnp.exp2(rates[rate_at(mine + k), :] * total_a) * before + end_a
        at = pl.ds(pl.multiple_of((mine + k) * STATE, 8), STATE)
        start[at, :] = jnp.where(leads, before, after)
        across[pl.ds(pl.multiple_of(k * STATE, 8), STATE), :] = jnp.where(leads, after, before)
        return 0

    lax.fori_loop(0, HALF, enter, 0, unroll=4)
    mine_2 = pl.ds(pl.multiple_of(mine * STATE, 8), HALF * STATE)
    swap_start = to_shard(mate, across, start.at[mine_2], send_st, recv_st)
    swap_start.start()
    loads[9].wait()
    swap_start.wait()

    def final_group(group, drive, readout):
        base = group * (STATE * 8)
        state = tuple(start[pl.ds(base + n, 8, stride=STATE), :] for n in range(STATE))
        scan_group(dts, us, rates_of(group), group, state, drive, readout, ys)

    def final_plain(group, _):
        base = run_base(group)
        final_group(group, splat_reader(bs, base), splat_reader(cs, base))
        return 0

    def result(slot, act, skip, gate):
        y = ys[pl.ds(slot, ROWS, stride=PITCH), :]
        return ((y + skip * act) * silu(gate)).astype(BF16)

    lax.fori_loop(5, GROUPS - 1, final_plain, 0)
    final_group(GROUPS - 1, mixed_reader(bs), mixed_reader(cs))
    for tile in range(CUT_TILES):
        at = v * SPAN + tile * LANES
        cols = pl.ds(pl.multiple_of(at, LANES), LANES)
        gate_cols = pl.ds(pl.multiple_of(INNER + at, LANES), LANES)
        skip = d_skip[:, cols]
        clean_out = result(
            cut_slot(CLEAN, tile), acts[:ROWS, cols].astype(F32), skip,
            clean[:, gate_cols].astype(F32),
        )
        corrupt_out = result(
            cut_slot(CORRUPT, tile), acts[ROWS : 2 * ROWS, cols].astype(F32), skip,
            corrupt[:, gate_cols].astype(F32),
        )
        cut[:, tile * LANES : (tile + 1) * LANES] = corrupt_out
        gap = clean_out.astype(F32) - corrupt_out.astype(F32)
        squares[tile] = jnp.sum(gap * gap, axis=0, keepdims=True)

    for k in range(1, VARS):
        to_variant(k, cut, whole.at[v], send_cut.at[k], recv_cut.at[k]).start()

    def send_square(i, _):
        peer = v * CUT_TILES + i

        @pl.when(peer != me)
        def _():
            to_shard(
                peer, squares.at[i], got_squares.at[me], send_sq.at[i], recv_sq
            ).start()

        @pl.when(peer == me)
        def _():
            pltpu.make_async_copy(squares.at[i], got_squares.at[me], recv_sq).start()

        return 0

    lax.fori_loop(0, CUT_TILES, send_square, 0)
    whole[v] = cut[...]

    lax.fori_loop(0, 5, final_plain, 0)

    def patched_tile(tile, _):
        cols = pl.ds(pl.multiple_of(tile * LANES, LANES), LANES)
        gate_cols = pl.ds(pl.multiple_of(INNER + tile * LANES, LANES), LANES)
        gate = jnp.where(
            take_gate, clean[:, gate_cols].astype(F32), corrupt[:, gate_cols].astype(F32)
        )
        patched[:, cols] = result(tile, acts[2 * ROWS :, cols].astype(F32), d_skip[:, cols], gate)
        return 0

    lax.fori_loop(0, TILES, patched_tile, 0, unroll=2)

    for k in range(1, VARS):
        to_variant(
            k, cut, whole.at[lax.rem(v + VARS - k, VARS)], send_cut.at[k], recv_cut.at[k]
        ).wait()

    for w in range(VARS):
        def peak_tile(i, _):
            here = pl.ds(pl.multiple_of(i * LANES, LANES), LANES)
            there = pl.ds(pl.multiple_of(w * SPAN + i * LANES, LANES), LANES)
            gap = jnp.abs(patched[:, there].astype(F32) - whole[w, :, here].astype(F32))
            peaks[w * CUT_TILES + i] = jnp.max(gap, axis=0, keepdims=True)
            return 0

        lax.fori_loop(0, CUT_TILES, peak_tile, 0, unroll=2)

    def send_peak(c, _):
        @pl.when(c != me)
        def _():
            to_shard(c, peaks.at[c], got_peaks.at[me], send_pk.at[c], recv_pk).start()

        @pl.when(c == me)
        def _():
            pltpu.make_async_copy(peaks.at[c], got_peaks.at[me], recv_pk).start()

        return 0

    lax.fori_loop(0, TILES, send_peak, 0)

    owner = lax.div(me, CUT_TILES)

    @pl.when(owner == v)
    def _():
        wait_for(got_squares, recv_sq)
        total = jnp.sum(got_squares[...], axis=0)
        spread[...] = jnp.sqrt(total / (SHARDS * ROWS) + TINY)
        for k in range(1, VARS):
            to_variant(k, spread, spread, send_sp.at[k], recv_sp).start()

    @pl.when((owner != v) & (me < TILES))
    def _():
        wait_for(spread, recv_sp)

    @pl.when(me < TILES)
    def _():
        wait_for(got_peaks, recv_pk)
        answer[...] = jnp.max(got_peaks[...], axis=0) / spread[...]
        pltpu.make_async_copy(answer, answers.at[me], recv_an).start()

        def share(k, _):
            peer = lax.rem(me + k, SHARDS)
            to_shard(peer, answer, answers.at[me], send_an.at[k], recv_an).start()
            return 0

        lax.fori_loop(1, SHARDS, share, 0)

    wait_for(answers, recv_an)
    for c in range(TILES):
        effect[:, c * LANES : (c + 1) * LANES] = answers[c]

    @pl.when(me < TILES)
    def _():
        def done(k, _):
            peer = lax.rem(me + k, SHARDS)
            to_shard(peer, answer, answers.at[me], send_an.at[k], recv_an).wait_send()
            return 0

        lax.fori_loop(1, SHARDS, done, 0)

    @pl.when(owner == v)
    def _():
        for k in range(1, VARS):
            to_variant(k, spread, spread, send_sp.at[k], recv_sp).wait_send()

    def sent_peak(c, _):
        @pl.when(c != me)
        def _():
            to_shard(c, peaks.at[c], got_peaks.at[me], send_pk.at[c], recv_pk).wait_send()

        return 0

    lax.fori_loop(0, TILES, sent_peak, 0)

    def sent_square(i, _):
        peer = v * CUT_TILES + i

        @pl.when(peer != me)
        def _():
            to_shard(
                peer, squares.at[i], got_squares.at[me], send_sq.at[i], recv_sq
            ).wait_send()

        return 0

    lax.fori_loop(0, CUT_TILES, sent_square, 0)
    others = pl.ds(0, CHIPS - 1)
    wait_for(chip_totals.at[others], send_ct)
    wait_for(chip_ends.at[others], send_ce)
    wait_for(leaving.at[others], send_in)


SMEM = pl.BlockSpec(memory_space=pltpu.SMEM)
HBM = pl.BlockSpec(memory_space=pltpu.HBM)
VMEM = pl.BlockSpec(memory_space=pltpu.VMEM)
DMA = pltpu.SemaphoreType.DMA


def shards(
    clean_proj, corrupt_proj, patch_pos, patch_mode, a_log, dt_bias,
    conv_weight, conv_bias, x_weight, dt_weight, d_skip,
):
    tails = jnp.concatenate([clean_proj[ROWS - 8 :, :INNER], corrupt_proj[ROWS - 8 :, :INNER]])
    rims = lax.ppermute(tails, "seq", [(s, s + 1) for s in range(SHARDS - 1)])
    row = (1, LANES)
    tile = (STATE, LANES)
    patched, effect = pl.pallas_call(
        kernel,
        out_shape=(
            jax.ShapeDtypeStruct((ROWS, INNER), BF16),
            jax.ShapeDtypeStruct((1, INNER), F32),
        ),
        in_specs=[SMEM, SMEM] + [HBM] * 10,
        out_specs=(VMEM, VMEM),
        scratch_shapes=[
            pltpu.VMEM((ROWS, 2 * INNER), BF16),
            pltpu.VMEM((ROWS, 2 * INNER), BF16),
            pltpu.VMEM((16, INNER), BF16),
            pltpu.VMEM((TAPS, INNER), F32),
            pltpu.VMEM((1, INNER), F32),
            pltpu.VMEM((RANK + 2 * STATE, INNER), BF16),
            pltpu.VMEM((RANK, INNER), BF16),
            pltpu.VMEM((1, INNER), F32),
            pltpu.VMEM((STATE, INNER), F32),
            pltpu.VMEM((1, INNER), F32),
            pltpu.VMEM((3, 8 + ROWS, 512), F32),
            pltpu.VMEM((3 * ROWS, INNER), BF16),
            pltpu.VMEM((3 * ROWS, RANK), BF16),
            pltpu.VMEM((ROWS * PITCH, LANES), F32),
            pltpu.VMEM((ROWS * PITCH, LANES), F32),
            pltpu.VMEM((3 * ROWS * SPLAT + 8, LANES), F32),
            pltpu.VMEM((3 * ROWS * SPLAT + 8, LANES), F32),
            pltpu.VMEM((CHUNKS * STATE, LANES), F32),
            pltpu.VMEM((CHUNKS * STATE, LANES), F32),
            pltpu.VMEM((CHUNKS, *row), F32),
            pltpu.VMEM((HALF * STATE, LANES), F32),
            pltpu.VMEM((HALF, *row), F32),
            pltpu.VMEM((HALF, *tile), F32),
            pltpu.VMEM((HALF, *row), F32),
            pltpu.VMEM((CHIPS, *tile), F32),
            pltpu.VMEM((CHIPS, *row), F32),
            pltpu.VMEM((CHIPS, *tile), F32),
            pltpu.VMEM((HALF, *tile), F32),
            pltpu.VMEM((HALF * STATE, LANES), F32),
            pltpu.VMEM((CHUNKS * STATE, LANES), F32),
            pltpu.VMEM((ROWS * PITCH, LANES), F32),
            pltpu.VMEM((ROWS, SPAN), BF16),
            pltpu.VMEM((CUT_TILES, *row), F32),
            pltpu.VMEM((VARS, ROWS, SPAN), BF16),
            pltpu.VMEM((TILES, *row), F32),
            pltpu.VMEM((SHARDS, *row), F32),
            pltpu.VMEM(row, F32),
            pltpu.VMEM((SHARDS, *row), F32),
            pltpu.VMEM(row, F32),
            pltpu.VMEM((TILES, *row), F32),
            DMA((10,)),
        ]
        + [DMA] * 12
        + [
            DMA((VARS,)), DMA((CUT_TILES,)), DMA((TILES,)), DMA((VARS,)), DMA((SHARDS,)),
            DMA((VARS,)), DMA, DMA, DMA, DMA,
        ],
        compiler_params=pltpu.CompilerParams(
            collective_id=0, has_side_effects=True, vmem_limit_bytes=48 * 1024 * 1024
        ),
        name="mixer",
    )(
        patch_pos, patch_mode, clean_proj, corrupt_proj, rims, conv_weight, conv_bias[None],
        x_weight.T, dt_weight, dt_bias[None], a_log, d_skip[None],
    )
    return (patched[None], effect)


def solution(mesh):
    return jax.shard_map(
        shards,
        mesh=mesh,
        in_specs=(
            P("seq", None), P("seq", None), P("var", None), P("var"),
            P(), P(), P(), P(), P(), P(), P(),
        ),
        out_specs=(P("var", "seq", None), P("var", None)),
        check_vma=False,
    )
```

```python
import functools

import jax
import jax.numpy as jnp
from jax import lax
from jax.experimental import pallas as pl
from jax.experimental.pallas import tpu as pltpu
from jax.sharding import PartitionSpec as P

STATE = 16
RANK = 160
ROWS = 32
INNER = 5120
SPAN = 1280
TAPS = 4
LANES = 128
CHUNKS = 64
SHARDS = 64
VARS = 4
TILES = INNER // LANES
CUT_TILES = SPAN // LANES
GROUPS = CHUNKS // 8
HALF = CHUNKS // 2
CHIPS = SHARDS // 2
PITCH = 72
SPLAT = 17
MESH = pl.DeviceIdType.MESH
LOG2E = 1.4426950408889634
TINY = 1e-06
F32 = jnp.float32
BF16 = jnp.bfloat16
UNROLL = 8
CLEAN, CORRUPT, PATCHED = 0, 1, 2
STEPS = sorted(
    ((dx, dz) for dx in range(4) for dz in range(8) if dx or dz),
    key=lambda step: -(min(step[0], 4 - step[0]) + min(step[1], 8 - step[1])),
)


def cut_slot(run, tile):
    if tile < 8:
        return TILES + 8 * run + tile
    return 56 + 2 * run + (tile - 8)


def hit_rows(pos_ref, first, count):
    rows = first + lax.broadcasted_iota(jnp.int32, (count, LANES), 0)
    hits = rows == pos_ref[0, 0]
    for k in range(1, pos_ref.shape[1]):
        hits = hits | (rows == pos_ref[0, k])
    return hits


def silu(value):
    return value / (1.0 + jnp.exp(-value))


def softplus(value):
    return jnp.maximum(value, 0.0) + jnp.log1p(jnp.exp(-jnp.abs(value)))


def row_of(ref, row):
    return jnp.broadcast_to(ref[pl.ds(row, 1), :], (8, LANES))


def scan_group(dts, us, rate, group, state, drive, readout, out):
    def step(t, carry):
        row = pl.multiple_of(t * PITCH + group * 8, 8)
        steps = dts[pl.ds(row, 8), :]
        flow = us[pl.ds(row, 8), :]
        entries = []
        total = None
        for n in range(STATE):
            decay = jnp.exp2(steps * rate[n])
            entry = decay * carry[n] + flow * drive(t, n)
            entries.append(entry)
            if readout is not None:
                term = readout(t, n) * entry
                total = term if total is None else total + term
        if readout is not None:
            out[pl.ds(row, 8), :] = total
        return tuple(entries)

    return lax.fori_loop(0, ROWS, step, state, unroll=UNROLL)


def splat_reader(ref, base):
    return lambda t, n: row_of(ref, base + t * SPLAT + n)


def mixed_reader(ref):
    first = lax.broadcasted_iota(jnp.int32, (8, LANES), 0) < 2

    def read(t, n):
        return jnp.where(
            first,
            row_of(ref, CLEAN * ROWS * SPLAT + t * SPLAT + n),
            row_of(ref, CORRUPT * ROWS * SPLAT + t * SPLAT + n),
        )

    return read


def wait_for(ref, sem):
    pltpu.make_async_copy(ref, ref, sem).wait()


def halo_kernel(clean, corrupt, rims, send_sem, recv_sem):
    me = lax.axis_index("seq")
    v = lax.axis_index("var")
    after = lax.rem(me + 1, SHARDS)
    barrier = pltpu.get_barrier_semaphore()
    for peer in (after, lax.rem(me + SHARDS - 1, SHARDS)):
        pl.semaphore_signal(barrier, inc=1, device_id=(peer, v), device_id_type=MESH)
    pl.semaphore_wait(barrier, 2)
    copies = [
        pltpu.make_async_remote_copy(
            src_ref=src.at[ROWS - 8 :, :INNER], dst_ref=rims.at[i], send_sem=send_sem.at[i],
            recv_sem=recv_sem.at[i], device_id=(after, v), device_id_type=MESH,
        )
        for i, src in enumerate((clean, corrupt))
    ]
    for copy in copies:
        copy.start()
    for copy in copies:
        copy.wait()


def emit_kernel(patched_in, effect_in, patched_out, effect_out, patched, effect, sems_in, sems_out):
    cut = ROWS // 2
    pieces = [
        (patched_in.at[i * cut : (i + 1) * cut], patched.at[i * cut : (i + 1) * cut],
         patched_out.at[i * cut : (i + 1) * cut])
        for i in range(2)
    ]
    pieces.append((effect_in, effect, effect_out))
    arrivals = [
        pltpu.make_async_copy(src, here, sems_in.at[i]) for i, (src, here, _) in enumerate(pieces)
    ]
    departures = [
        pltpu.make_async_copy(here, dst, sems_out.at[i]) for i, (_, here, dst) in enumerate(pieces)
    ]
    for arrival in arrivals:
        arrival.start()
    for arrival, departure in zip(arrivals, departures):
        arrival.wait()
        departure.start()
    for departure in departures:
        departure.wait()


def kernel(
    pos, mode, clean_in, corrupt_in, rims_in, conv_w_in, conv_b_in, x_w_in, dt_w_in, dt_b_in,
    a_log_in, d_skip_in,
    patched_out, effect,
    patched, clean, corrupt, rims, conv_w, conv_b, x_w, dt_w, dt_b, a_log, d_skip,
    pad, acts, low, dts, us, bs, cs, rates, ends, totals,
    pair_ends, pair_totals, chip_ends, chip_totals, got_ends, got_totals,
    leaving, landed, across, start, ys,
    cut, squares, whole, peaks, squares_z, line_squares, squares_x, spreads,
    peaks_z, line_peaks, peaks_x,
    load_sem, send_pt, recv_pt, send_pe, recv_pe, send_ct, recv_ct, send_ce, recv_ce,
    send_in, recv_in, send_st, recv_st,
    send_cut, recv_cut, send_sz, recv_sz, send_sx, recv_sx, send_sp, recv_sp,
    send_pz, recv_pz, send_px, recv_px,
):
    me = lax.axis_index("seq")
    v = lax.axis_index("var")
    chip = lax.div(me, 2)
    core = lax.rem(me, 2)
    mate = me + 1 - 2 * core
    mine = core * HALF
    theirs = HALF - mine
    barrier = pltpu.get_barrier_semaphore()

    loads = [
        pltpu.make_async_copy(src, dst, load_sem.at[i])
        for i, (src, dst) in enumerate(
            (
                (clean_in, clean), (corrupt_in, corrupt), (rims_in, rims), (conv_w_in, conv_w),
                (conv_b_in, conv_b), (x_w_in, x_w), (dt_w_in, dt_w), (dt_b_in, dt_b),
                (a_log_in, a_log), (d_skip_in, d_skip),
            )
        )
    ]
    for load in loads:
        load.start()

    def signal(peer, variant):
        pl.semaphore_signal(barrier, inc=1, device_id=(peer, variant), device_id_type=MESH)

    def greet(k, _):
        signal(2 * lax.rem(chip + k, CHIPS) + core, v)
        return 0

    lax.fori_loop(1, CHIPS, greet, 0)
    signal(mate, v)
    for k in range(1, 4):
        signal(lax.rem(mate + 16 * k, SHARDS), v)
    for k in range(1, VARS):
        signal(me, lax.rem(v + k, VARS))

    def to_variant(k, src, dst, send_sem, recv_sem):
        return pltpu.make_async_remote_copy(
            src_ref=src, dst_ref=dst, send_sem=send_sem, recv_sem=recv_sem,
            device_id=(me, lax.rem(v + k, VARS)), device_id_type=MESH,
        )

    def to_shard(peer, src, dst, send_sem, recv_sem):
        return pltpu.make_async_remote_copy(
            src_ref=src, dst_ref=dst, send_sem=send_sem, recv_sem=recv_sem,
            device_id=(peer, v), device_id_type=MESH,
        )

    first = me * ROWS
    inside = me > 0
    hits = hit_rows(pos, first, ROWS)[:, :1]
    take = hits & (mode[0] != 1)
    take_gate = hits & (mode[0] != 0)
    take_rim = hit_rows(pos, first - 8, 8)[:, :1] & (mode[0] != 1)

    for load in loads[:5]:
        load.wait()
    width = 512

    def conv(i, _):
        cols = pl.ds(pl.multiple_of(i * width, width), width)
        sig_clean = clean[:, cols].astype(F32)
        sig_corrupt = corrupt[:, cols].astype(F32)
        rim_clean = jnp.where(inside, rims[0, :, cols].astype(F32), 0.0)
        rim_corrupt = jnp.where(inside, rims[1, :, cols].astype(F32), 0.0)
        pieces = (
            (rim_clean, sig_clean),
            (rim_corrupt, sig_corrupt),
            (
                jnp.where(take_rim, rim_clean, rim_corrupt),
                jnp.where(take, sig_clean, sig_corrupt),
            ),
        )
        bias = conv_b[:, cols]
        for run, (rim, sig) in enumerate(pieces):
            pad[run, 0:8, :] = rim
            pad[run, 8:, :] = sig
            total = bias + conv_w[0:1, cols] * pad[run, 5 : 5 + ROWS, :]
            for k in range(1, TAPS):
                total = total + conv_w[k : k + 1, cols] * pad[run, 5 + k : 5 + k + ROWS, :]
            acts[run * ROWS : (run + 1) * ROWS, cols] = silu(total).astype(BF16)
        return 0

    lax.fori_loop(0, INNER // width, conv, 0)

    loads[5].wait()
    projected = lax.dot_general(
        acts[...], x_w[...], (((1,), (1,)), ((), ())), preferred_element_type=F32
    )
    low[...] = projected[:, :RANK].astype(BF16)
    for run in range(3):
        part = projected[run * ROWS : (run + 1) * ROWS]
        for n in range(STATE):
            at = run * ROWS * SPLAT + n
            bs[pl.ds(at, ROWS, stride=SPLAT), :] = jnp.broadcast_to(
                part[:, RANK + n : RANK + n + 1], (ROWS, LANES)
            )
            cs[pl.ds(at, ROWS, stride=SPLAT), :] = jnp.broadcast_to(
                part[:, RANK + STATE + n : RANK + STATE + n + 1], (ROWS, LANES)
            )

    for load in loads[6:9]:
        load.wait()

    def rate_at(slot):
        return pl.ds(lax.div(slot, 8) * (STATE * 8) + lax.rem(slot, 8), STATE, stride=8)

    def place(slot, steps, act, log_rate):
        dts[pl.ds(slot, ROWS, stride=PITCH), :] = steps
        us[pl.ds(slot, ROWS, stride=PITCH), :] = steps * act
        totals[slot] = jnp.sum(steps, axis=0, keepdims=True)
        rates[rate_at(slot), :] = jnp.exp(log_rate) * (-LOG2E)

    wide = 640

    def patched_steps(i, _):
        cols = pl.ds(pl.multiple_of(i * wide, wide), wide)
        raw = jnp.dot(low[2 * ROWS :, :], dt_w[:, cols], preferred_element_type=F32)
        steps = softplus(raw + dt_b[:, cols])
        act = acts[2 * ROWS :, cols].astype(F32)
        logs = a_log[:, cols]
        for k in range(wide // LANES):
            part = slice(k * LANES, (k + 1) * LANES)
            place(i * (wide // LANES) + k, steps[:, part], act[:, part], logs[:, part])
        return 0

    lax.fori_loop(0, INNER // wide, patched_steps, 0)

    cols = pl.ds(pl.multiple_of(v * SPAN, LANES), SPAN)
    raw = jnp.dot(low[: 2 * ROWS, :], dt_w[:, cols], preferred_element_type=F32)
    steps = softplus(raw + dt_b[:, cols])
    act = acts[: 2 * ROWS, cols].astype(F32)
    logs = a_log[:, cols]
    for run in (CLEAN, CORRUPT):
        rows = slice(run * ROWS, (run + 1) * ROWS)
        for tile in range(CUT_TILES):
            part = slice(tile * LANES, (tile + 1) * LANES)
            place(cut_slot(run, tile), steps[rows, part], act[rows, part], logs[:, part])
    blank = jnp.zeros((ROWS, LANES), F32)
    for slot in range(60, CHUNKS):
        place(slot, blank, blank, jnp.zeros((STATE, LANES), F32))

    pl.semaphore_wait(barrier, CHIPS - 1 + 1 + 3 + VARS - 1)
    theirs_3 = pl.ds(theirs, HALF)
    swap_totals = to_shard(mate, totals.at[theirs_3], pair_totals, send_pt, recv_pt)
    swap_totals.start()

    zero = jnp.zeros((8, LANES), F32)

    def rates_of(group):
        base = group * (STATE * 8)
        return [rates[pl.ds(pl.multiple_of(base + n * 8, 8), 8), :] for n in range(STATE)]

    def run_base(group):
        return jnp.where(group < 5, PATCHED, group - 5) * (ROWS * SPLAT)

    def local_group(group, drive):
        found = scan_group(
            dts, us, rates_of(group), group, (zero,) * STATE, drive, None, None
        )
        for n in range(STATE):
            ends[pl.ds(group * (STATE * 8) + n, 8, stride=STATE), :] = found[n]

    def local_pass(offset):
        def body(i, _):
            group = offset + i

            @pl.when(group < GROUPS - 1)
            def _():
                local_group(group, splat_reader(bs, run_base(group)))

            @pl.when(group == GROUPS - 1)
            def _():
                local_group(group, mixed_reader(bs))

            return 0

        lax.fori_loop(0, GROUPS // 2, body, 0)

    local_pass(lax.div(theirs, 8))
    theirs_2 = pl.ds(pl.multiple_of(theirs * STATE, 8), HALF * STATE)
    swap_ends = to_shard(mate, ends.at[theirs_2], pair_ends, send_pe, recv_pe)
    swap_ends.start()
    swap_totals.wait()

    def chip_total(k, _):
        chip_totals[k] = totals[mine + k] + pair_totals[k]
        return 0

    lax.fori_loop(0, HALF, chip_total, 0, unroll=4)
    row_x, line_z = lax.div(chip, 8), lax.rem(chip, 8)
    peers = [8 * lax.rem(row_x + dx, 4) + lax.rem(line_z + dz, 8) for dx, dz in STEPS]
    pltpu.make_async_copy(chip_totals.at[chip], got_totals.at[chip], recv_ct).start()
    for peer in peers:
        target = 2 * peer + core
        to_shard(target, chip_totals.at[peer], got_totals.at[chip], send_ct, recv_ct).start()
    local_pass(lax.div(mine, 8))
    leads = core == 0

    def my_summary(k):
        own = ends[pl.ds(pl.multiple_of((mine + k) * STATE, 8), STATE), :]
        return own, totals[mine + k]

    def pair_of(k):
        own_end, own_total = my_summary(k)
        other_end = pair_ends[pl.ds(pl.multiple_of(k * STATE, 8), STATE), :]
        other_total = pair_totals[k]
        return (
            jnp.where(leads, own_end, other_end), jnp.where(leads, own_total, other_total),
            jnp.where(leads, other_end, own_end), jnp.where(leads, other_total, own_total),
        )

    swap_ends.wait()

    def chip_end(k, _):
        end_a, total_a, end_b, total_b = pair_of(k)
        chip_ends[k] = jnp.exp2(rates[rate_at(mine + k), :] * total_b) * end_a + end_b
        return 0

    lax.fori_loop(0, HALF, chip_end, 0, unroll=4)
    pltpu.make_async_copy(chip_ends.at[chip], got_ends.at[chip], recv_ce).start()

    for peer in peers:
        target = 2 * peer + core
        to_shard(target, chip_ends.at[peer], got_ends.at[chip], send_ce, recv_ce).start()
    my_rate = rates[rate_at(mine + chip), :]
    wait_for(got_totals, recv_ct)
    wait_for(got_ends, recv_ce)

    def chain(s, state):
        leaving[s] = state
        return jnp.exp2(my_rate * got_totals[s]) * state + got_ends[s]

    lax.fori_loop(0, CHIPS, chain, jnp.zeros((STATE, LANES), F32), unroll=4)
    pltpu.make_async_copy(leaving.at[chip], landed.at[chip], recv_in).start()

    for peer in peers:
        to_shard(2 * peer + core, leaving.at[peer], landed.at[chip], send_in, recv_in).start()
    wait_for(landed, recv_in)

    def enter(k, _):
        end_a, total_a, _, _ = pair_of(k)
        before = landed[k]
        after = jnp.exp2(rates[rate_at(mine + k), :] * total_a) * before + end_a
        at = pl.ds(pl.multiple_of((mine + k) * STATE, 8), STATE)
        start[at, :] = jnp.where(leads, before, after)
        across[pl.ds(pl.multiple_of(k * STATE, 8), STATE), :] = jnp.where(leads, after, before)
        return 0

    lax.fori_loop(0, HALF, enter, 0, unroll=4)
    mine_2 = pl.ds(pl.multiple_of(mine * STATE, 8), HALF * STATE)
    swap_start = to_shard(mate, across, start.at[mine_2], send_st, recv_st)
    swap_start.start()
    loads[9].wait()
    swap_start.wait()

    def final_group(group, drive, readout):
        base = group * (STATE * 8)
        state = tuple(start[pl.ds(base + n, 8, stride=STATE), :] for n in range(STATE))
        scan_group(dts, us, rates_of(group), group, state, drive, readout, ys)

    def final_plain(group, _):
        base = run_base(group)
        final_group(group, splat_reader(bs, base), splat_reader(cs, base))
        return 0

    def result(slot, act, skip, gate):
        y = ys[pl.ds(slot, ROWS, stride=PITCH), :]
        return ((y + skip * act) * silu(gate)).astype(BF16)

    lax.fori_loop(5, GROUPS - 1, final_plain, 0)
    final_group(GROUPS - 1, mixed_reader(bs), mixed_reader(cs))
    squares[...] = jnp.zeros_like(squares)
    for tile in range(CUT_TILES):
        at = v * SPAN + tile * LANES
        cols = pl.ds(pl.multiple_of(at, LANES), LANES)
        gate_cols = pl.ds(pl.multiple_of(INNER + at, LANES), LANES)
        skip = d_skip[:, cols]
        clean_out = result(
            cut_slot(CLEAN, tile), acts[:ROWS, cols].astype(F32), skip,
            clean[:, gate_cols].astype(F32),
        )
        corrupt_out = result(
            cut_slot(CORRUPT, tile), acts[ROWS : 2 * ROWS, cols].astype(F32), skip,
            corrupt[:, gate_cols].astype(F32),
        )
        cut[:, tile * LANES : (tile + 1) * LANES] = corrupt_out
        gap = clean_out.astype(F32) - corrupt_out.astype(F32)
        squares[tile : tile + 1, :] = jnp.sum(gap * gap, axis=0, keepdims=True)

    for k in range(1, VARS):
        to_variant(k, cut, whole.at[v], send_cut.at[k], recv_cut.at[k]).start()

    plane_xc = 2 * lax.div(chip, 8) + core

    def along_z(k):
        return 16 * lax.div(chip, 8) + 2 * lax.rem(line_z + k, 8) + core

    def across_xc(k):
        other = lax.rem(plane_xc + k, 8)
        return 16 * lax.div(other, 2) + 2 * line_z + lax.rem(other, 2)

    def share(peer_of, slot, src, dst, send_sem, recv_sem):
        for k in range(1, 8):
            to_shard(peer_of(k), src, dst.at[slot], send_sem, recv_sem).start()
        dst[slot] = src[...]

    seven = pl.ds(0, 7)
    share(along_z, line_z, squares, squares_z, send_sz, recv_sz)
    whole[v] = cut[...]

    lax.fori_loop(0, 5, final_plain, 0)

    def patched_tile(tile, _):
        cols = pl.ds(pl.multiple_of(tile * LANES, LANES), LANES)
        gate_cols = pl.ds(pl.multiple_of(INNER + tile * LANES, LANES), LANES)
        gate = jnp.where(
            take_gate, clean[:, gate_cols].astype(F32), corrupt[:, gate_cols].astype(F32)
        )
        patched[:, cols] = result(tile, acts[2 * ROWS :, cols].astype(F32), d_skip[:, cols], gate)
        return 0

    lax.fori_loop(0, TILES, patched_tile, 0, unroll=2)

    save = pltpu.make_async_copy(patched, patched_out, load_sem.at[0])
    save.start()
    for k in range(1, VARS):
        to_variant(
            k, cut, whole.at[lax.rem(v + VARS - k, VARS)], send_cut.at[k], recv_cut.at[k]
        ).wait()

    for w in range(VARS):
        def peak_tile(i, _):
            here = pl.ds(pl.multiple_of(i * LANES, LANES), LANES)
            there = pl.ds(pl.multiple_of(w * SPAN + i * LANES, LANES), LANES)
            gap = jnp.abs(patched[:, there].astype(F32) - whole[w, :, here].astype(F32))
            peaks[pl.ds(w * CUT_TILES + i, 1), :] = jnp.max(gap, axis=0, keepdims=True)
            return 0

        lax.fori_loop(0, CUT_TILES, peak_tile, 0, unroll=2)

    share(along_z, line_z, peaks, peaks_z, send_pz, recv_pz)
    wait_for(squares_z.at[seven], recv_sz)
    line_squares[...] = jnp.sum(squares_z[...], axis=0)
    share(across_xc, plane_xc, line_squares, squares_x, send_sx, recv_sx)
    wait_for(peaks_z.at[seven], recv_pz)
    line_peaks[...] = jnp.max(peaks_z[...], axis=0)
    share(across_xc, plane_xc, line_peaks, peaks_x, send_px, recv_px)
    wait_for(squares_x.at[seven], recv_sx)
    spreads[v] = jnp.sqrt(jnp.sum(squares_x[...], axis=0) / (SHARDS * ROWS) + TINY)
    for k in range(1, VARS):
        to_variant(k, spreads.at[v], spreads.at[v], send_sp.at[k], recv_sp.at[k]).start()
    wait_for(peaks_x.at[seven], recv_px)
    for k in range(1, VARS):
        there = spreads.at[lax.rem(v + VARS - k, VARS)]
        to_variant(k, there, there, send_sp.at[k], recv_sp.at[k]).wait()
    peak = jnp.max(peaks_x[...], axis=0)
    for w in range(VARS):
        rows = slice(w * CUT_TILES, (w + 1) * CUT_TILES)
        effect[rows, :] = peak[rows, :] / spreads[w, :CUT_TILES, :]
    save.wait()
    wait_for(squares_z.at[seven], send_sz)
    wait_for(squares_x.at[seven], send_sx)
    wait_for(peaks_z.at[seven], send_pz)
    wait_for(peaks_x.at[seven], send_px)
    others = pl.ds(0, CHIPS - 1)
    wait_for(chip_totals.at[others], send_ct)
    wait_for(chip_ends.at[others], send_ce)
    wait_for(leaving.at[others], send_in)


SMEM = pl.BlockSpec(memory_space=pltpu.SMEM)
HBM = pl.BlockSpec(memory_space=pltpu.HBM)
VMEM = pl.BlockSpec(memory_space=pltpu.VMEM)
DMA = pltpu.SemaphoreType.DMA


def shards(
    clean_proj, corrupt_proj, patch_pos, patch_mode, a_log, dt_bias,
    conv_weight, conv_bias, x_weight, dt_weight, d_skip,
):
    rims = pl.pallas_call(
        halo_kernel,
        out_shape=jax.ShapeDtypeStruct((2, 8, INNER), BF16),
        in_specs=[HBM, HBM],
        out_specs=HBM,
        scratch_shapes=[DMA((2,)), DMA((2,))],
        compiler_params=pltpu.CompilerParams(
            collective_id=1, has_side_effects=True, vmem_limit_bytes=67_043_328
        ),
        name="halo",
    )(clean_proj, corrupt_proj)
    row = (1, LANES)
    tile = (STATE, LANES)
    patched, effect = pl.pallas_call(
        kernel,
        out_shape=(
            jax.ShapeDtypeStruct((ROWS, INNER), BF16),
            jax.ShapeDtypeStruct((TILES, LANES), F32),
        ),
        in_specs=[SMEM, SMEM] + [HBM] * 10,
        out_specs=(HBM, VMEM),
        scratch_shapes=[
            pltpu.VMEM((ROWS, INNER), BF16),
            pltpu.VMEM((ROWS, 2 * INNER), BF16),
            pltpu.VMEM((ROWS, 2 * INNER), BF16),
            pltpu.VMEM((2, 8, INNER), BF16),
            pltpu.VMEM((TAPS, INNER), F32),
            pltpu.VMEM((1, INNER), F32),
            pltpu.VMEM((RANK + 2 * STATE, INNER), BF16),
            pltpu.VMEM((RANK, INNER), BF16),
            pltpu.VMEM((1, INNER), F32),
            pltpu.VMEM((STATE, INNER), F32),
            pltpu.VMEM((1, INNER), F32),
            pltpu.VMEM((3, 8 + ROWS, 512), F32),
            pltpu.VMEM((3 * ROWS, INNER), BF16),
            pltpu.VMEM((3 * ROWS, RANK), BF16),
            pltpu.VMEM((ROWS * PITCH, LANES), F32),
            pltpu.VMEM((ROWS * PITCH, LANES), F32),
            pltpu.VMEM((3 * ROWS * SPLAT + 8, LANES), F32),
            pltpu.VMEM((3 * ROWS * SPLAT + 8, LANES), F32),
            pltpu.VMEM((CHUNKS * STATE, LANES), F32),
            pltpu.VMEM((CHUNKS * STATE, LANES), F32),
            pltpu.VMEM((CHUNKS, *row), F32),
            pltpu.VMEM((HALF * STATE, LANES), F32),
            pltpu.VMEM((HALF, *row), F32),
            pltpu.VMEM((HALF, *tile), F32),
            pltpu.VMEM((HALF, *row), F32),
            pltpu.VMEM((CHIPS, *tile), F32),
            pltpu.VMEM((CHIPS, *row), F32),
            pltpu.VMEM((CHIPS, *tile), F32),
            pltpu.VMEM((HALF, *tile), F32),
            pltpu.VMEM((HALF * STATE, LANES), F32),
            pltpu.VMEM((CHUNKS * STATE, LANES), F32),
            pltpu.VMEM((ROWS * PITCH, LANES), F32),
            pltpu.VMEM((ROWS, SPAN), BF16),
            pltpu.VMEM((STATE, LANES), F32),
            pltpu.VMEM((VARS, ROWS, SPAN), BF16),
            pltpu.VMEM((TILES, LANES), F32),
            pltpu.VMEM((8, STATE, LANES), F32),
            pltpu.VMEM((STATE, LANES), F32),
            pltpu.VMEM((8, STATE, LANES), F32),
            pltpu.VMEM((VARS, STATE, LANES), F32),
            pltpu.VMEM((8, TILES, LANES), F32),
            pltpu.VMEM((TILES, LANES), F32),
            pltpu.VMEM((8, TILES, LANES), F32),
            DMA((10,)),
        ]
        + [DMA] * 12
        + [DMA((VARS,)), DMA((VARS,))]
        + [DMA] * 4
        + [DMA((VARS,)), DMA((VARS,))]
        + [DMA] * 4,
        compiler_params=pltpu.CompilerParams(
            collective_id=0, has_side_effects=True, vmem_limit_bytes=67_043_328
        ),
        name="mixer",
    )(
        patch_pos, patch_mode, clean_proj, corrupt_proj, rims, conv_weight, conv_bias[None],
        x_weight.T, dt_weight, dt_bias[None], a_log, d_skip[None],
    )
    patched, effect = pl.pallas_call(
        emit_kernel,
        out_shape=(
            jax.ShapeDtypeStruct((ROWS, INNER), BF16),
            jax.ShapeDtypeStruct((TILES, LANES), F32),
        ),
        in_specs=[HBM, HBM],
        out_specs=(HBM, HBM),
        scratch_shapes=[
            pltpu.VMEM((ROWS, INNER), BF16), pltpu.VMEM((TILES, LANES), F32), DMA((3,)), DMA((3,)),
        ],
        compiler_params=pltpu.CompilerParams(vmem_limit_bytes=67_043_328),
        name="emit",
    )(patched, effect)
    return (patched[None], effect.reshape(1, INNER))


def solution(mesh):
    return jax.shard_map(
        shards,
        mesh=mesh,
        in_specs=(
            P("seq", None), P("seq", None), P("var", None), P("var"),
            P(), P(), P(), P(), P(), P(), P(),
        ),
        out_specs=(P("var", "seq", None), P("var", None)),
        check_vma=False,
    )
```

```python
import functools

import jax
import jax.numpy as jnp
from jax import lax
from jax.experimental import pallas as pl
from jax.experimental.pallas import tpu as pltpu
from jax.sharding import PartitionSpec as P

STATE = 16
RANK = 160
ROWS = 32
INNER = 5120
SPAN = 1280
TAPS = 4
LANES = 128
CHUNKS = 64
SHARDS = 64
VARS = 4
TILES = INNER // LANES
CUT_TILES = SPAN // LANES
GROUPS = CHUNKS // 8
HALF = CHUNKS // 2
CHIPS = SHARDS // 2
PITCH = 72
SPLAT = 17
MESH = pl.DeviceIdType.MESH
LOG2E = 1.4426950408889634
TINY = 1e-06
F32 = jnp.float32
BF16 = jnp.bfloat16
UNROLL = 8
CLEAN, CORRUPT, PATCHED = 0, 1, 2
STEPS = sorted(
    ((dx, dz) for dx in range(4) for dz in range(8) if dx or dz),
    key=lambda step: -(min(step[0], 4 - step[0]) + min(step[1], 8 - step[1])),
)


def cut_slot(run, tile):
    if tile < 8:
        return TILES + 8 * run + tile
    return 56 + 2 * run + (tile - 8)


def hit_rows(pos_ref, first, count):
    rows = first + lax.broadcasted_iota(jnp.int32, (count, LANES), 0)
    hits = rows == pos_ref[0, 0]
    for k in range(1, pos_ref.shape[1]):
        hits = hits | (rows == pos_ref[0, k])
    return hits


def silu(value):
    return value / (1.0 + jnp.exp(-value))


def softplus(value):
    return jnp.maximum(value, 0.0) + jnp.log1p(jnp.exp(-jnp.abs(value)))


def row_of(ref, row):
    return jnp.broadcast_to(ref[pl.ds(row, 1), :], (8, LANES))


def scan_group(dts, us, rate, group, state, drive, readout, out):
    def step(t, carry):
        row = pl.multiple_of(t * PITCH + group * 8, 8)
        steps = dts[pl.ds(row, 8), :]
        flow = us[pl.ds(row, 8), :]
        entries = []
        total = None
        for n in range(STATE):
            decay = jnp.exp2(steps * rate[n])
            entry = decay * carry[n] + flow * drive(t, n)
            entries.append(entry)
            if readout is not None:
                term = readout(t, n) * entry
                total = term if total is None else total + term
        if readout is not None:
            out[pl.ds(row, 8), :] = total
        return tuple(entries)

    return lax.fori_loop(0, ROWS, step, state, unroll=UNROLL)


def splat_reader(ref, base):
    return lambda t, n: row_of(ref, base + t * SPLAT + n)


def mixed_reader(ref):
    first = lax.broadcasted_iota(jnp.int32, (8, LANES), 0) < 2

    def read(t, n):
        return jnp.where(
            first,
            row_of(ref, CLEAN * ROWS * SPLAT + t * SPLAT + n),
            row_of(ref, CORRUPT * ROWS * SPLAT + t * SPLAT + n),
        )

    return read


def wait_for(ref, sem):
    pltpu.make_async_copy(ref, ref, sem).wait()


def halo_kernel(clean, corrupt, rims, send_sem, recv_sem):
    me = lax.axis_index("seq")
    v = lax.axis_index("var")
    after = lax.rem(me + 1, SHARDS)
    barrier = pltpu.get_barrier_semaphore()
    for peer in (after, lax.rem(me + SHARDS - 1, SHARDS)):
        pl.semaphore_signal(barrier, inc=1, device_id=(peer, v), device_id_type=MESH)
    pl.semaphore_wait(barrier, 2)
    copies = [
        pltpu.make_async_remote_copy(
            src_ref=src.at[ROWS - 8 :, :INNER], dst_ref=rims.at[i], send_sem=send_sem.at[i],
            recv_sem=recv_sem.at[i], device_id=(after, v), device_id_type=MESH,
        )
        for i, src in enumerate((clean, corrupt))
    ]
    for copy in copies:
        copy.start()
    for copy in copies:
        copy.wait()


def emit_kernel(patched_in, effect_in, patched_out, effect_out, patched, effect, sems_in, sems_out):
    cut = ROWS // 2
    pieces = [
        (patched_in.at[i * cut : (i + 1) * cut], patched.at[i * cut : (i + 1) * cut],
         patched_out.at[i * cut : (i + 1) * cut])
        for i in range(2)
    ]
    pieces.append((effect_in, effect, effect_out))
    arrivals = [
        pltpu.make_async_copy(src, here, sems_in.at[i]) for i, (src, here, _) in enumerate(pieces)
    ]
    departures = [
        pltpu.make_async_copy(here, dst, sems_out.at[i]) for i, (_, here, dst) in enumerate(pieces)
    ]
    for arrival in arrivals:
        arrival.start()
    for arrival, departure in zip(arrivals, departures):
        arrival.wait()
        departure.start()
    for departure in departures:
        departure.wait()


def kernel(
    pos, mode, clean_in, corrupt_in, rims_in, conv_w_in, conv_b_in, x_w_in, dt_w_in, dt_b_in,
    a_log_in, d_skip_in,
    patched_out, effect,
    patched, clean, corrupt, clean_gate, corrupt_gate, rims, conv_w, conv_b, x_w, dt_w, dt_b, a_log, d_skip,
    pad, acts, low, maps, weights, base, gates, dts, us, bs, cs, rates, ends, totals,
    pair_ends, pair_totals, chip_ends, chip_totals, got_ends, got_totals,
    leaving, landed, across, start, ys,
    cut, squares, whole, peaks, squares_z, line_squares, squares_x, spreads,
    peaks_z, line_peaks, peaks_x,
    load_sem, send_pt, recv_pt, send_pe, recv_pe, send_ct, recv_ct, send_ce, recv_ce,
    send_in, recv_in, send_st, recv_st,
    send_cut, recv_cut, send_sz, recv_sz, send_sx, recv_sx, send_sp, recv_sp,
    send_pz, recv_pz, send_px, recv_px,
):
    me = lax.axis_index("seq")
    v = lax.axis_index("var")
    chip = lax.div(me, 2)
    core = lax.rem(me, 2)
    mate = me + 1 - 2 * core
    mine = core * HALF
    theirs = HALF - mine
    barrier = pltpu.get_barrier_semaphore()

    loads = [
        pltpu.make_async_copy(src, dst, load_sem.at[i])
        for i, (src, dst) in enumerate(
            (
                (clean_in.at[:, :INNER], clean), (corrupt_in.at[:, :INNER], corrupt),
                (rims_in, rims), (conv_w_in, conv_w),
                (conv_b_in, conv_b), (x_w_in, x_w), (dt_w_in, dt_w), (dt_b_in, dt_b),
                (a_log_in, a_log), (d_skip_in, d_skip),
                (clean_in.at[:, INNER:], clean_gate), (corrupt_in.at[:, INNER:], corrupt_gate),
            )
        )
    ]
    for load in loads:
        load.start()

    def signal(peer, variant):
        pl.semaphore_signal(barrier, inc=1, device_id=(peer, variant), device_id_type=MESH)

    def greet(k, _):
        signal(2 * lax.rem(chip + k, CHIPS) + core, v)
        return 0

    lax.fori_loop(1, CHIPS, greet, 0)
    signal(mate, v)
    for k in range(1, 4):
        signal(lax.rem(mate + 16 * k, SHARDS), v)
    for k in range(1, VARS):
        signal(me, lax.rem(v + k, VARS))

    def to_variant(k, src, dst, send_sem, recv_sem):
        return pltpu.make_async_remote_copy(
            src_ref=src, dst_ref=dst, send_sem=send_sem, recv_sem=recv_sem,
            device_id=(me, lax.rem(v + k, VARS)), device_id_type=MESH,
        )

    def to_shard(peer, src, dst, send_sem, recv_sem):
        return pltpu.make_async_remote_copy(
            src_ref=src, dst_ref=dst, send_sem=send_sem, recv_sem=recv_sem,
            device_id=(peer, v), device_id_type=MESH,
        )

    first = me * ROWS
    inside = me > 0
    hits = hit_rows(pos, first, ROWS)[:, :1]
    take = hits & (mode[0] != 1)
    take_gate = hits & (mode[0] != 0)
    take_rim = hit_rows(pos, first - 8, 8)[:, :1] & (mode[0] != 1)

    for load in loads[:5]:
        load.wait()
    width = 512

    width = 512
    span = 8 + ROWS

    def fill(i, _):
        cols = pl.ds(pl.multiple_of(i * width, width), width)
        sig_clean = clean[:, cols].astype(F32)
        sig_corrupt = corrupt[:, cols].astype(F32)
        rim_clean = jnp.where(inside, rims[0, :, cols].astype(F32), 0.0)
        rim_corrupt = jnp.where(inside, rims[1, :, cols].astype(F32), 0.0)
        pieces = (
            (rim_clean, sig_clean),
            (rim_corrupt, sig_corrupt),
            (
                jnp.where(take_rim, rim_clean, rim_corrupt),
                jnp.where(take, sig_clean, sig_corrupt),
            ),
        )
        for run, (rim, sig) in enumerate(pieces):
            for k in range(width // LANES):
                part = slice(k * LANES, (k + 1) * LANES)
                at = pl.multiple_of((run * TILES + i * (width // LANES) + k) * span, 8)
                pad[pl.ds(at, 8), :] = rim[:, part]
                pad[pl.ds(at + 8, ROWS), :] = sig[:, part]
        return 0

    lax.fori_loop(0, INNER // width, fill, 0)

    def conv(tile, _):
        cols = pl.ds(pl.multiple_of(tile * LANES, LANES), LANES)
        bias = conv_b[:, cols]
        for run in range(3):
            at = (run * TILES + tile) * span + 8 - (TAPS - 1)
            total = bias + conv_w[0:1, cols] * pad[pl.ds(at, ROWS), :]
            for k in range(1, TAPS):
                total = total + conv_w[k : k + 1, cols] * pad[pl.ds(at + k, ROWS), :]
            acts[run * ROWS : (run + 1) * ROWS, cols] = silu(total).astype(BF16)
        return 0

    lax.fori_loop(0, TILES, conv, 0, unroll=4)

    loads[5].wait()
    projected = lax.dot_general(
        acts[...], x_w[...], (((1,), (1,)), ((), ())), preferred_element_type=F32
    )
    low[...] = projected[:, :RANK].astype(BF16)
    maps[...] = projected[:, RANK + STATE :]
    for run in range(3):
        part = projected[run * ROWS : (run + 1) * ROWS]
        for n in range(STATE):
            at = run * ROWS * SPLAT + n
            bs[pl.ds(at, ROWS, stride=SPLAT), :] = jnp.broadcast_to(
                part[:, RANK + n : RANK + n + 1], (ROWS, LANES)
            )

    for load in loads[6:9]:
        load.wait()

    def rate_at(slot):
        return pl.ds(lax.div(slot, 8) * (STATE * 8) + lax.rem(slot, 8), STATE, stride=8)

    def place(slot, steps, act, log_rate):
        dts[pl.ds(slot, ROWS, stride=PITCH), :] = steps
        us[pl.ds(slot, ROWS, stride=PITCH), :] = steps * act
        totals[slot] = jnp.sum(steps, axis=0, keepdims=True)
        rates[rate_at(slot), :] = jnp.exp(log_rate) * (-LOG2E)

    wide = 1280

    def patched_steps(i, _):
        cols = pl.ds(pl.multiple_of(i * wide, wide), wide)
        raw = jnp.dot(low[2 * ROWS :, :], dt_w[:, cols], preferred_element_type=F32)
        steps = softplus(raw + dt_b[:, cols])
        act = acts[2 * ROWS :, cols].astype(F32)
        logs = a_log[:, cols]
        for k in range(wide // LANES):
            part = slice(k * LANES, (k + 1) * LANES)
            place(i * (wide // LANES) + k, steps[:, part], act[:, part], logs[:, part])
        return 0

    lax.fori_loop(0, INNER // wide, patched_steps, 0)

    cols = pl.ds(pl.multiple_of(v * SPAN, LANES), SPAN)
    raw = jnp.dot(low[: 2 * ROWS, :], dt_w[:, cols], preferred_element_type=F32)
    steps = softplus(raw + dt_b[:, cols])
    act = acts[: 2 * ROWS, cols].astype(F32)
    logs = a_log[:, cols]
    for run in (CLEAN, CORRUPT):
        rows = slice(run * ROWS, (run + 1) * ROWS)
        for tile in range(CUT_TILES):
            part = slice(tile * LANES, (tile + 1) * LANES)
            place(cut_slot(run, tile), steps[rows, part], act[rows, part], logs[:, part])
    blank = jnp.zeros((ROWS, LANES), F32)
    for slot in range(60, CHUNKS):
        place(slot, blank, blank, jnp.zeros((STATE, LANES), F32))

    pl.semaphore_wait(barrier, CHIPS - 1 + 1 + 3 + VARS - 1)
    theirs_3 = pl.ds(theirs, HALF)
    swap_totals = to_shard(mate, totals.at[theirs_3], pair_totals, send_pt, recv_pt)
    swap_totals.start()

    zero = jnp.zeros((8, LANES), F32)

    def rates_of(group):
        base = group * (STATE * 8)
        return [rates[pl.ds(pl.multiple_of(base + n * 8, 8), 8), :] for n in range(STATE)]

    def run_base(group):
        return jnp.where(group < 5, PATCHED, group - 5) * (ROWS * SPLAT)

    def local_group(group, drive):
        found = scan_group(
            dts, us, rates_of(group), group, (zero,) * STATE, drive, None, None
        )
        for n in range(STATE):
            ends[pl.ds(group * (STATE * 8) + n, 8, stride=STATE), :] = found[n]

    def local_pass(offset):
        def body(i, _):
            group = offset + i

            @pl.when(group < GROUPS - 1)
            def _():
                local_group(group, splat_reader(bs, run_base(group)))

            @pl.when(group == GROUPS - 1)
            def _():
                local_group(group, mixed_reader(bs))

            return 0

        lax.fori_loop(0, GROUPS // 2, body, 0)

    local_pass(lax.div(theirs, 8))
    theirs_2 = pl.ds(pl.multiple_of(theirs * STATE, 8), HALF * STATE)
    swap_ends = to_shard(mate, ends.at[theirs_2], pair_ends, send_pe, recv_pe)
    swap_ends.start()
    swap_totals.wait()

    def chip_total(k, _):
        chip_totals[k] = totals[mine + k] + pair_totals[k]
        return 0

    lax.fori_loop(0, HALF, chip_total, 0, unroll=4)
    row_x, line_z = lax.div(chip, 8), lax.rem(chip, 8)
    peers = [8 * lax.rem(row_x + dx, 4) + lax.rem(line_z + dz, 8) for dx, dz in STEPS]
    pltpu.make_async_copy(chip_totals.at[chip], got_totals.at[chip], recv_ct).start()
    for peer in peers:
        target = 2 * peer + core
        to_shard(target, chip_totals.at[peer], got_totals.at[chip], send_ct, recv_ct).start()
    local_pass(lax.div(mine, 8))
    leads = core == 0

    def my_summary(k):
        own = ends[pl.ds(pl.multiple_of((mine + k) * STATE, 8), STATE), :]
        return own, totals[mine + k]

    def pair_of(k):
        own_end, own_total = my_summary(k)
        other_end = pair_ends[pl.ds(pl.multiple_of(k * STATE, 8), STATE), :]
        other_total = pair_totals[k]
        return (
            jnp.where(leads, own_end, other_end), jnp.where(leads, own_total, other_total),
            jnp.where(leads, other_end, own_end), jnp.where(leads, other_total, own_total),
        )

    swap_ends.wait()

    def chip_end(k, _):
        end_a, total_a, end_b, total_b = pair_of(k)
        chip_ends[k] = jnp.exp2(rates[rate_at(mine + k), :] * total_b) * end_a + end_b
        return 0

    lax.fori_loop(0, HALF, chip_end, 0, unroll=4)
    pltpu.make_async_copy(chip_ends.at[chip], got_ends.at[chip], recv_ce).start()

    for peer in peers:
        target = 2 * peer + core
        to_shard(target, chip_ends.at[peer], got_ends.at[chip], send_ce, recv_ce).start()
    my_rate = rates[rate_at(mine + chip), :]
    for run in range(3):
        for n in range(STATE):
            cs[pl.ds(run * ROWS * SPLAT + n, ROWS, stride=SPLAT), :] = jnp.broadcast_to(
                maps[run * ROWS : (run + 1) * ROWS, n : n + 1], (ROWS, LANES)
            )

    def local_readout(group, drive, read):
        scan_group(dts, us, rates_of(group), group, (zero,) * STATE, drive, read, ys)

    def plain_readout(group, _):
        at = run_base(group)
        local_readout(group, splat_reader(bs, at), splat_reader(cs, at))
        return 0

    lax.fori_loop(0, GROUPS - 1, plain_readout, 0)
    local_readout(GROUPS - 1, mixed_reader(bs), mixed_reader(cs))
    wait_for(got_totals, recv_ct)
    wait_for(got_ends, recv_ce)

    def chain(s, state):
        leaving[s] = state
        return jnp.exp2(my_rate * got_totals[s]) * state + got_ends[s]

    lax.fori_loop(0, CHIPS, chain, jnp.zeros((STATE, LANES), F32), unroll=4)
    pltpu.make_async_copy(leaving.at[chip], landed.at[chip], recv_in).start()

    for peer in peers:
        to_shard(2 * peer + core, leaving.at[peer], landed.at[chip], send_in, recv_in).start()
    def entry_weights(group, read):
        rate = rates_of(group)

        def step(t, run_total):
            row = pl.multiple_of(t * PITCH + group * 8, 8)
            run_total = run_total + dts[pl.ds(row, 8), :]
            at = (group * ROWS + t) * (STATE * 8)
            for n in range(STATE):
                weights[pl.ds(pl.multiple_of(at + n * 8, 8), 8), :] = read(t, n) * jnp.exp2(
                    run_total * rate[n]
                )
            return run_total

        lax.fori_loop(0, ROWS, step, zero, unroll=4)

    def plain_weights(group, _):
        entry_weights(group, splat_reader(cs, run_base(group)))
        return 0

    lax.fori_loop(0, GROUPS - 1, plain_weights, 0)
    entry_weights(GROUPS - 1, mixed_reader(cs))
    for load in loads[9:]:
        load.wait()

    def prepare(slot, act, skip, gate):
        rows = pl.ds(pl.multiple_of(slot * ROWS, 8), ROWS)
        base[rows, :] = ys[pl.ds(slot, ROWS, stride=PITCH), :] + skip * act
        gates[rows, :] = silu(gate)

    for run, gate_rows in ((CLEAN, clean_gate), (CORRUPT, corrupt_gate)):
        for tile in range(CUT_TILES):
            cols = pl.ds(pl.multiple_of(v * SPAN + tile * LANES, LANES), LANES)
            act = acts[run * ROWS : (run + 1) * ROWS, cols].astype(F32)
            prepare(cut_slot(run, tile), act, d_skip[:, cols], gate_rows[:, cols].astype(F32))

    def prepare_patched(tile, _):
        cols = pl.ds(pl.multiple_of(tile * LANES, LANES), LANES)
        gate = jnp.where(
            take_gate, clean_gate[:, cols].astype(F32), corrupt_gate[:, cols].astype(F32)
        )
        prepare(tile, acts[2 * ROWS :, cols].astype(F32), d_skip[:, cols], gate)
        return 0

    lax.fori_loop(0, TILES, prepare_patched, 0, unroll=2)
    wait_for(landed, recv_in)

    def enter(k, _):
        end_a, total_a, _, _ = pair_of(k)
        before = landed[k]
        after = jnp.exp2(rates[rate_at(mine + k), :] * total_a) * before + end_a
        at = pl.ds(pl.multiple_of((mine + k) * STATE, 8), STATE)
        start[at, :] = jnp.where(leads, before, after)
        across[pl.ds(pl.multiple_of(k * STATE, 8), STATE), :] = jnp.where(leads, after, before)
        return 0

    lax.fori_loop(0, HALF, enter, 0, unroll=4)
    mine_2 = pl.ds(pl.multiple_of(mine * STATE, 8), HALF * STATE)
    swap_start = to_shard(mate, across, start.at[mine_2], send_st, recv_st)
    swap_start.start()
    swap_start.wait()

    def final_group(group, _):
        at = group * (STATE * 8)
        state = [start[pl.ds(at + n, 8, stride=STATE), :] for n in range(STATE)]

        def step(t, _):
            at = (group * ROWS + t) * (STATE * 8)
            total = None
            for n in range(STATE):
                term = weights[pl.ds(pl.multiple_of(at + n * 8, 8), 8), :] * state[n]
                total = term if total is None else total + term
            ys[pl.ds(pl.multiple_of(t * PITCH + group * 8, 8), 8), :] = total
            return 0

        lax.fori_loop(0, ROWS, step, 0, unroll=8)
        return 0

    def result(slot):
        rows = pl.ds(pl.multiple_of(slot * ROWS, 8), ROWS)
        y = ys[pl.ds(slot, ROWS, stride=PITCH), :]
        return ((y + base[rows, :]) * gates[rows, :]).astype(BF16)

    lax.fori_loop(6, GROUPS, final_group, 0)

    for tile in range(CUT_TILES):
        cut[:, tile * LANES : (tile + 1) * LANES] = result(cut_slot(CORRUPT, tile))
    before, after = lax.rem(v + VARS - 1, VARS), lax.rem(v + 1, VARS)
    half = ROWS // 2
    upper, lower = pl.ds(0, half), pl.ds(half, half)

    def send_rows(k, i, slot, rows, src):
        dst = whole.at[slot, rows]
        return to_variant(k, src if src is not None else dst, dst, send_cut.at[i], recv_cut.at[i])

    directs = [
        send_rows(k, i, v, rows, cut.at[rows])
        for i, (k, rows) in enumerate(
            ((1, upper), (VARS - 1, lower), (1, lower), (VARS - 1, upper))
        )
    ]
    for direct in directs:
        direct.start()
    final_group(5, 0)
    squares[...] = jnp.zeros_like(squares)
    for tile in range(CUT_TILES):
        gap = result(cut_slot(CLEAN, tile)).astype(F32)
        gap = gap - cut[:, tile * LANES : (tile + 1) * LANES].astype(F32)
        squares[tile : tile + 1, :] = jnp.sum(gap * gap, axis=0, keepdims=True)

    plane_xc = 2 * lax.div(chip, 8) + core

    def along_z(k):
        return 16 * lax.div(chip, 8) + 2 * lax.rem(line_z + k, 8) + core

    def across_xc(k):
        other = lax.rem(plane_xc + k, 8)
        return 16 * lax.div(other, 2) + 2 * line_z + lax.rem(other, 2)

    def share(peer_of, slot, src, dst, send_sem, recv_sem):
        for k in range(1, 8):
            to_shard(peer_of(k), src, dst.at[slot], send_sem, recv_sem).start()
        dst[slot] = src[...]

    seven = pl.ds(0, 7)
    share(along_z, line_z, squares, squares_z, send_sz, recv_sz)
    whole[v] = cut[...]

    lax.fori_loop(0, 5, final_group, 0)
    def patched_tile(tile, _):
        cols = pl.ds(pl.multiple_of(tile * LANES, LANES), LANES)
        patched[:, cols] = result(tile)
        return 0

    lax.fori_loop(0, TILES, patched_tile, 0, unroll=4)

    save = pltpu.make_async_copy(patched, patched_out, load_sem.at[0])
    save.start()
    relays = [
        send_rows(1, 4, before, upper, None), send_rows(VARS - 1, 5, after, lower, None)
    ]
    for direct, relay in zip(directs, relays):
        direct.wait_recv()
        relay.start()
    for direct in directs[2:]:
        direct.wait_recv()
    for direct in directs:
        direct.wait_send()
    for relay in relays:
        relay.wait()

    for w in range(VARS):
        def peak_tile(i, _):
            here = pl.ds(pl.multiple_of(i * LANES, LANES), LANES)
            there = pl.ds(pl.multiple_of(w * SPAN + i * LANES, LANES), LANES)
            gap = jnp.abs(patched[:, there].astype(F32) - whole[w, :, here].astype(F32))
            peaks[pl.ds(w * CUT_TILES + i, 1), :] = jnp.max(gap, axis=0, keepdims=True)
            return 0

        lax.fori_loop(0, CUT_TILES, peak_tile, 0, unroll=2)

    share(along_z, line_z, peaks, peaks_z, send_pz, recv_pz)
    wait_for(squares_z.at[seven], recv_sz)
    line_squares[...] = jnp.sum(squares_z[...], axis=0)
    share(across_xc, plane_xc, line_squares, squares_x, send_sx, recv_sx)
    wait_for(peaks_z.at[seven], recv_pz)
    line_peaks[...] = jnp.max(peaks_z[...], axis=0)
    share(across_xc, plane_xc, line_peaks, peaks_x, send_px, recv_px)
    wait_for(squares_x.at[seven], recv_sx)
    spreads[v] = jnp.sqrt(jnp.sum(squares_x[...], axis=0) / (SHARDS * ROWS) + TINY)
    for k in range(1, VARS):
        to_variant(k, spreads.at[v], spreads.at[v], send_sp.at[k], recv_sp.at[k]).start()
    wait_for(peaks_x.at[seven], recv_px)
    for k in range(1, VARS):
        there = spreads.at[lax.rem(v + VARS - k, VARS)]
        to_variant(k, there, there, send_sp.at[k], recv_sp.at[k]).wait()
    peak = jnp.max(peaks_x[...], axis=0)
    for w in range(VARS):
        rows = slice(w * CUT_TILES, (w + 1) * CUT_TILES)
        effect[rows, :] = peak[rows, :] / spreads[w, :CUT_TILES, :]
    save.wait()
    wait_for(squares_z.at[seven], send_sz)
    wait_for(squares_x.at[seven], send_sx)
    wait_for(peaks_z.at[seven], send_pz)
    wait_for(peaks_x.at[seven], send_px)
    others = pl.ds(0, CHIPS - 1)
    wait_for(chip_totals.at[others], send_ct)
    wait_for(chip_ends.at[others], send_ce)
    wait_for(leaving.at[others], send_in)


SMEM = pl.BlockSpec(memory_space=pltpu.SMEM)
HBM = pl.BlockSpec(memory_space=pltpu.HBM)
VMEM = pl.BlockSpec(memory_space=pltpu.VMEM)
DMA = pltpu.SemaphoreType.DMA


def shards(
    clean_proj, corrupt_proj, patch_pos, patch_mode, a_log, dt_bias,
    conv_weight, conv_bias, x_weight, dt_weight, d_skip,
):
    rims = pl.pallas_call(
        halo_kernel,
        out_shape=jax.ShapeDtypeStruct((2, 8, INNER), BF16),
        in_specs=[HBM, HBM],
        out_specs=HBM,
        scratch_shapes=[DMA((2,)), DMA((2,))],
        compiler_params=pltpu.CompilerParams(
            collective_id=1, has_side_effects=True, vmem_limit_bytes=67_043_328
        ),
        name="halo",
    )(clean_proj, corrupt_proj)
    row = (1, LANES)
    tile = (STATE, LANES)
    patched, effect = pl.pallas_call(
        kernel,
        out_shape=(
            jax.ShapeDtypeStruct((ROWS, INNER), BF16),
            jax.ShapeDtypeStruct((TILES, LANES), F32),
        ),
        in_specs=[SMEM, SMEM] + [HBM] * 10,
        out_specs=(HBM, VMEM),
        scratch_shapes=[
            pltpu.VMEM((ROWS, INNER), BF16),
            pltpu.VMEM((ROWS, INNER), BF16),
            pltpu.VMEM((ROWS, INNER), BF16),
            pltpu.VMEM((ROWS, INNER), BF16),
            pltpu.VMEM((ROWS, INNER), BF16),
            pltpu.VMEM((2, 8, INNER), BF16),
            pltpu.VMEM((TAPS, INNER), F32),
            pltpu.VMEM((1, INNER), F32),
            pltpu.VMEM((RANK + 2 * STATE, INNER), BF16),
            pltpu.VMEM((RANK, INNER), BF16),
            pltpu.VMEM((1, INNER), F32),
            pltpu.VMEM((STATE, INNER), F32),
            pltpu.VMEM((1, INNER), F32),
            pltpu.VMEM((3 * TILES * (8 + ROWS), LANES), F32),
            pltpu.VMEM((3 * ROWS, INNER), BF16),
            pltpu.VMEM((3 * ROWS, RANK), BF16),
            pltpu.VMEM((3 * ROWS, STATE), F32),
            pltpu.VMEM((GROUPS * ROWS * STATE * 8, LANES), F32),
            pltpu.VMEM((CHUNKS * ROWS, LANES), F32),
            pltpu.VMEM((CHUNKS * ROWS, LANES), F32),
            pltpu.VMEM((ROWS * PITCH, LANES), F32),
            pltpu.VMEM((ROWS * PITCH, LANES), F32),
            pltpu.VMEM((3 * ROWS * SPLAT + 8, LANES), F32),
            pltpu.VMEM((3 * ROWS * SPLAT + 8, LANES), F32),
            pltpu.VMEM((CHUNKS * STATE, LANES), F32),
            pltpu.VMEM((CHUNKS * STATE, LANES), F32),
            pltpu.VMEM((CHUNKS, *row), F32),
            pltpu.VMEM((HALF * STATE, LANES), F32),
            pltpu.VMEM((HALF, *row), F32),
            pltpu.VMEM((HALF, *tile), F32),
            pltpu.VMEM((HALF, *row), F32),
            pltpu.VMEM((CHIPS, *tile), F32),
            pltpu.VMEM((CHIPS, *row), F32),
            pltpu.VMEM((CHIPS, *tile), F32),
            pltpu.VMEM((HALF, *tile), F32),
            pltpu.VMEM((HALF * STATE, LANES), F32),
            pltpu.VMEM((CHUNKS * STATE, LANES), F32),
            pltpu.VMEM((ROWS * PITCH, LANES), F32),
            pltpu.VMEM((ROWS, SPAN), BF16),
            pltpu.VMEM((STATE, LANES), F32),
            pltpu.VMEM((VARS, ROWS, SPAN), BF16),
            pltpu.VMEM((TILES, LANES), F32),
            pltpu.VMEM((8, STATE, LANES), F32),
            pltpu.VMEM((STATE, LANES), F32),
            pltpu.VMEM((8, STATE, LANES), F32),
            pltpu.VMEM((VARS, STATE, LANES), F32),
            pltpu.VMEM((8, TILES, LANES), F32),
            pltpu.VMEM((TILES, LANES), F32),
            pltpu.VMEM((8, TILES, LANES), F32),
            DMA((12,)),
        ]
        + [DMA] * 12
        + [DMA((6,)), DMA((6,))]
        + [DMA] * 4
        + [DMA((VARS,)), DMA((VARS,))]
        + [DMA] * 4,
        compiler_params=pltpu.CompilerParams(
            collective_id=0, has_side_effects=True, vmem_limit_bytes=67_043_328
        ),
        name="mixer",
    )(
        patch_pos, patch_mode, clean_proj, corrupt_proj, rims, conv_weight, conv_bias[None],
        x_weight.T, dt_weight, dt_bias[None], a_log, d_skip[None],
    )
    patched, effect = pl.pallas_call(
        emit_kernel,
        out_shape=(
            jax.ShapeDtypeStruct((ROWS, INNER), BF16),
            jax.ShapeDtypeStruct((TILES, LANES), F32),
        ),
        in_specs=[HBM, HBM],
        out_specs=(HBM, HBM),
        scratch_shapes=[
            pltpu.VMEM((ROWS, INNER), BF16), pltpu.VMEM((TILES, LANES), F32), DMA((3,)), DMA((3,)),
        ],
        compiler_params=pltpu.CompilerParams(vmem_limit_bytes=67_043_328),
        name="emit",
    )(patched, effect)
    return (patched[None], effect.reshape(1, INNER))


def solution(mesh):
    return jax.shard_map(
        shards,
        mesh=mesh,
        in_specs=(
            P("seq", None), P("seq", None), P("var", None), P("var"),
            P(), P(), P(), P(), P(), P(), P(),
        ),
        out_specs=(P("var", "seq", None), P("var", None)),
        check_vma=False,
    )
```

```python
import functools

import jax
import jax.numpy as jnp
from jax import lax
from jax.experimental import pallas as pl
from jax.experimental.pallas import tpu as pltpu
from jax.sharding import PartitionSpec as P

STATE = 16
RANK = 160
ROWS = 32
INNER = 5120
SPAN = 1280
TAPS = 4
LANES = 128
CHUNKS = 64
SHARDS = 64
VARS = 4
TILES = INNER // LANES
CUT_TILES = SPAN // LANES
GROUPS = CHUNKS // 8
HALF = CHUNKS // 2
CHIPS = SHARDS // 2
PITCH = 72
SPLAT = 17
MESH = pl.DeviceIdType.MESH
LOG2E = 1.4426950408889634
TINY = 1e-06
F32 = jnp.float32
BF16 = jnp.bfloat16
UNROLL = 8
CLEAN, CORRUPT, PATCHED = 0, 1, 2
STEPS = sorted(
    ((dx, dz) for dx in range(4) for dz in range(8) if dx or dz),
    key=lambda step: -(min(step[0], 4 - step[0]) + min(step[1], 8 - step[1])),
)


def cut_slot(run, tile):
    if tile < 8:
        return TILES + 8 * run + tile
    return 56 + 2 * run + (tile - 8)


def hit_rows(pos_ref, first, count):
    rows = first + lax.broadcasted_iota(jnp.int32, (count, LANES), 0)
    hits = rows == pos_ref[0, 0]
    for k in range(1, pos_ref.shape[1]):
        hits = hits | (rows == pos_ref[0, k])
    return hits


def silu(value):
    return value / (1.0 + jnp.exp(-value))


def softplus(value):
    return jnp.maximum(value, 0.0) + jnp.log1p(jnp.exp(-jnp.abs(value)))


def row_of(ref, row):
    return jnp.broadcast_to(ref[pl.ds(row, 1), :], (8, LANES))


def scan_group(dts, us, rate, group, state, drive, readout, out):
    def step(t, carry):
        row = pl.multiple_of(t * PITCH + group * 8, 8)
        steps = dts[pl.ds(row, 8), :]
        flow = us[pl.ds(row, 8), :]
        entries = []
        total = None
        for n in range(STATE):
            decay = jnp.exp2(steps * rate[n])
            entry = decay * carry[n] + flow * drive(t, n)
            entries.append(entry)
            if readout is not None:
                term = readout(t, n) * entry
                total = term if total is None else total + term
        if readout is not None:
            out[pl.ds(row, 8), :] = total
        return tuple(entries)

    return lax.fori_loop(0, ROWS, step, state, unroll=UNROLL)


def splat_reader(ref, base):
    return lambda t, n: row_of(ref, base + t * SPLAT + n)


def mixed_reader(ref):
    first = lax.broadcasted_iota(jnp.int32, (8, LANES), 0) < 2

    def read(t, n):
        return jnp.where(
            first,
            row_of(ref, CLEAN * ROWS * SPLAT + t * SPLAT + n),
            row_of(ref, CORRUPT * ROWS * SPLAT + t * SPLAT + n),
        )

    return read


def wait_for(ref, sem):
    pltpu.make_async_copy(ref, ref, sem).wait()


def halo_kernel(clean, corrupt, rims, ends, wide, packed, load_sem, send_sem, recv_sem):
    me = lax.axis_index("seq")
    v = lax.axis_index("var")
    after = lax.min(me + 1, SHARDS - 1)
    barrier = pltpu.get_barrier_semaphore()
    loads = [
        pltpu.make_async_copy(src.at[ROWS - 8 :, :INNER], ends.at[i], load_sem.at[i])
        for i, src in enumerate((clean, corrupt))
    ]
    for load in loads:
        load.start()
    has_next, has_last = me < SHARDS - 1, me > 0

    def signal(peer):
        pl.semaphore_signal(barrier, inc=1, device_id=(peer, v), device_id_type=MESH)

    @pl.when(has_next)
    def _():
        signal(me + 1)

    @pl.when(has_last)
    def _():
        signal(me - 1)

    for load in loads:
        load.wait()
    margin = TAPS - 1
    wide[...] = jnp.zeros_like(wide)
    for i in range(2):
        wide[i * margin : (i + 1) * margin, :] = ends[i].astype(F32)[8 - margin :, :]
    packed[...] = wide[...].astype(BF16)

    pl.semaphore_wait(barrier, lax.min(me, 1) + lax.min(SHARDS - 1 - me, 1))
    copy = pltpu.make_async_remote_copy(
        src_ref=packed, dst_ref=rims, send_sem=send_sem, recv_sem=recv_sem,
        device_id=(after, v), device_id_type=MESH,
    )

    @pl.when(has_next)
    def _():
        copy.start()
        copy.wait_send()

    @pl.when(has_last)
    def _():
        copy.wait_recv()


def emit_kernel(patched_in, effect_in, patched_out, effect_out, patched, effect, sems_in, sems_out):
    cut = ROWS // 2
    pieces = [
        (patched_in.at[i * cut : (i + 1) * cut], patched.at[i * cut : (i + 1) * cut],
         patched_out.at[i * cut : (i + 1) * cut])
        for i in range(2)
    ]
    pieces.append((effect_in, effect, effect_out))
    arrivals = [
        pltpu.make_async_copy(src, here, sems_in.at[i]) for i, (src, here, _) in enumerate(pieces)
    ]
    departures = [
        pltpu.make_async_copy(here, dst, sems_out.at[i]) for i, (_, here, dst) in enumerate(pieces)
    ]
    for arrival in arrivals:
        arrival.start()
    for arrival, departure in zip(arrivals, departures):
        arrival.wait()
        departure.start()
    for departure in departures:
        departure.wait()


def kernel(
    pos, mode, clean_in, corrupt_in, rims_in, conv_w_in, conv_b_in, x_w_in, dt_w_in, dt_b_in,
    a_log_in, d_skip_in,
    patched_out, effect,
    patched, clean, corrupt, clean_gate, corrupt_gate, rims, conv_w, conv_b, x_w, dt_w, dt_b, a_log, d_skip,
    pad, acts, low, maps, weights, base, gates, dts, us, bs, cs, rates, ends, totals,
    pair_ends, pair_totals, chip_ends, chip_totals, got_ends, got_totals,
    leaving, landed, across, start, ys,
    cut, squares, whole, peaks, squares_z, line_squares, squares_x, spreads,
    peaks_z, line_peaks, peaks_x, pair_squares, chip_squares, pair_peaks, chip_peaks, answer,
    load_sem, send_pt, recv_pt, send_pe, recv_pe, send_ct, recv_ct, send_ce, recv_ce,
    send_in, recv_in, send_st, recv_st,
    send_cut, recv_cut, send_sz, recv_sz, send_sx, recv_sx, send_sp, recv_sp,
    send_pz, recv_pz, send_px, recv_px, send_qq, recv_qq, send_pp, recv_pp, send_an, recv_an,
):
    me = lax.axis_index("seq")
    v = lax.axis_index("var")
    chip = lax.div(me, 2)
    core = lax.rem(me, 2)
    mate = me + 1 - 2 * core
    mine = core * HALF
    theirs = HALF - mine
    barrier = pltpu.get_barrier_semaphore()

    loads = [
        pltpu.make_async_copy(src, dst, load_sem.at[i])
        for i, (src, dst) in enumerate(
            (
                (clean_in.at[:, :INNER], clean), (corrupt_in.at[:, :INNER], corrupt),
                (rims_in, rims), (conv_w_in, conv_w),
                (conv_b_in, conv_b), (x_w_in, x_w), (dt_w_in, dt_w), (dt_b_in, dt_b),
                (a_log_in, a_log), (d_skip_in, d_skip),
                (clean_in.at[:, INNER:], clean_gate), (corrupt_in.at[:, INNER:], corrupt_gate),
            )
        )
    ]
    for load in loads:
        load.start()

    def signal(peer, variant):
        pl.semaphore_signal(barrier, inc=1, device_id=(peer, variant), device_id_type=MESH)

    def greet(k, _):
        signal(2 * lax.rem(chip + k, CHIPS) + core, v)
        return 0

    lax.fori_loop(1, CHIPS, greet, 0)
    signal(mate, v)
    for k in range(1, VARS):
        signal(me, lax.rem(v + k, VARS))

    def to_variant(k, src, dst, send_sem, recv_sem):
        return pltpu.make_async_remote_copy(
            src_ref=src, dst_ref=dst, send_sem=send_sem, recv_sem=recv_sem,
            device_id=(me, lax.rem(v + k, VARS)), device_id_type=MESH,
        )

    def to_shard(peer, src, dst, send_sem, recv_sem):
        return pltpu.make_async_remote_copy(
            src_ref=src, dst_ref=dst, send_sem=send_sem, recv_sem=recv_sem,
            device_id=(peer, v), device_id_type=MESH,
        )

    first = me * ROWS
    margin = TAPS - 1
    inside = me > 0
    hits = hit_rows(pos, first, ROWS)[:, :1]
    take = hits & (mode[0] != 1)
    take_gate = hits & (mode[0] != 0)
    take_rim = hit_rows(pos, first - margin, margin)[:, :1] & (mode[0] != 1)

    for load in loads[:5]:
        load.wait()
    width = 512

    width = 512
    span = 8 + ROWS

    def fill(i, _):
        cols = pl.ds(pl.multiple_of(i * width, width), width)
        sig_clean = clean[:, cols].astype(F32)
        sig_corrupt = corrupt[:, cols].astype(F32)
        rim = jnp.where(inside, rims[:, cols].astype(F32), 0.0)
        rim_clean, rim_corrupt = rim[:margin], rim[margin : 2 * margin]
        pieces = (
            (rim_clean, sig_clean),
            (rim_corrupt, sig_corrupt),
            (
                jnp.where(take_rim, rim_clean, rim_corrupt),
                jnp.where(take, sig_clean, sig_corrupt),
            ),
        )
        for run, (rim, sig) in enumerate(pieces):
            for k in range(width // LANES):
                part = slice(k * LANES, (k + 1) * LANES)
                at = pl.multiple_of((run * TILES + i * (width // LANES) + k) * span, 8)
                pad[pl.ds(at + 8 - margin, margin), :] = rim[:, part]
                pad[pl.ds(at + 8, ROWS), :] = sig[:, part]
        return 0

    lax.fori_loop(0, INNER // width, fill, 0)

    def conv(tile, _):
        cols = pl.ds(pl.multiple_of(tile * LANES, LANES), LANES)
        bias = conv_b[:, cols]
        for run in range(3):
            at = (run * TILES + tile) * span + 8 - (TAPS - 1)
            total = bias + conv_w[0:1, cols] * pad[pl.ds(at, ROWS), :]
            for k in range(1, TAPS):
                total = total + conv_w[k : k + 1, cols] * pad[pl.ds(at + k, ROWS), :]
            acts[run * ROWS : (run + 1) * ROWS, cols] = silu(total).astype(BF16)
        return 0

    lax.fori_loop(0, TILES, conv, 0, unroll=4)

    loads[5].wait()
    projected = lax.dot_general(
        acts[...], x_w[...], (((1,), (1,)), ((), ())), preferred_element_type=F32
    )
    low[...] = projected[:, :RANK].astype(BF16)
    maps[...] = projected[:, RANK + STATE :]
    for run in range(3):
        part = projected[run * ROWS : (run + 1) * ROWS]
        for n in range(STATE):
            at = run * ROWS * SPLAT + n
            bs[pl.ds(at, ROWS, stride=SPLAT), :] = jnp.broadcast_to(
                part[:, RANK + n : RANK + n + 1], (ROWS, LANES)
            )

    for load in loads[6:9]:
        load.wait()

    def rate_at(slot):
        return pl.ds(lax.div(slot, 8) * (STATE * 8) + lax.rem(slot, 8), STATE, stride=8)

    def place(slot, steps, act, log_rate):
        dts[pl.ds(slot, ROWS, stride=PITCH), :] = steps
        us[pl.ds(slot, ROWS, stride=PITCH), :] = steps * act
        totals[slot] = jnp.sum(steps, axis=0, keepdims=True)
        rates[rate_at(slot), :] = jnp.exp(log_rate) * (-LOG2E)

    wide = 1280

    def patched_steps(i, _):
        cols = pl.ds(pl.multiple_of(i * wide, wide), wide)
        raw = jnp.dot(low[2 * ROWS :, :], dt_w[:, cols], preferred_element_type=F32)
        steps = softplus(raw + dt_b[:, cols])
        act = acts[2 * ROWS :, cols].astype(F32)
        logs = a_log[:, cols]
        for k in range(wide // LANES):
            part = slice(k * LANES, (k + 1) * LANES)
            place(i * (wide // LANES) + k, steps[:, part], act[:, part], logs[:, part])
        return 0

    lax.fori_loop(0, INNER // wide, patched_steps, 0)

    cols = pl.ds(pl.multiple_of(v * SPAN, LANES), SPAN)
    raw = jnp.dot(low[: 2 * ROWS, :], dt_w[:, cols], preferred_element_type=F32)
    steps = softplus(raw + dt_b[:, cols])
    act = acts[: 2 * ROWS, cols].astype(F32)
    logs = a_log[:, cols]
    for run in (CLEAN, CORRUPT):
        rows = slice(run * ROWS, (run + 1) * ROWS)
        for tile in range(CUT_TILES):
            part = slice(tile * LANES, (tile + 1) * LANES)
            place(cut_slot(run, tile), steps[rows, part], act[rows, part], logs[:, part])
    blank = jnp.zeros((ROWS, LANES), F32)
    for slot in range(60, CHUNKS):
        place(slot, blank, blank, jnp.zeros((STATE, LANES), F32))

    pl.semaphore_wait(barrier, CHIPS - 1 + 1 + VARS - 1)
    theirs_3 = pl.ds(theirs, HALF)
    swap_totals = to_shard(mate, totals.at[theirs_3], pair_totals, send_pt, recv_pt)
    swap_totals.start()

    zero = jnp.zeros((8, LANES), F32)

    def rates_of(group):
        base = group * (STATE * 8)
        return [rates[pl.ds(pl.multiple_of(base + n * 8, 8), 8), :] for n in range(STATE)]

    def run_base(group):
        return jnp.where(group < 5, PATCHED, group - 5) * (ROWS * SPLAT)

    def local_group(group, drive):
        found = scan_group(
            dts, us, rates_of(group), group, (zero,) * STATE, drive, None, None
        )
        for n in range(STATE):
            ends[pl.ds(group * (STATE * 8) + n, 8, stride=STATE), :] = found[n]

    def local_pass(offset):
        def body(i, _):
            group = offset + i

            @pl.when(group < GROUPS - 1)
            def _():
                local_group(group, splat_reader(bs, run_base(group)))

            @pl.when(group == GROUPS - 1)
            def _():
                local_group(group, mixed_reader(bs))

            return 0

        lax.fori_loop(0, GROUPS // 2, body, 0)

    local_pass(lax.div(theirs, 8))
    theirs_2 = pl.ds(pl.multiple_of(theirs * STATE, 8), HALF * STATE)
    swap_ends = to_shard(mate, ends.at[theirs_2], pair_ends, send_pe, recv_pe)
    swap_ends.start()
    swap_totals.wait()

    def chip_total(k, _):
        chip_totals[k] = totals[mine + k] + pair_totals[k]
        return 0

    lax.fori_loop(0, HALF, chip_total, 0, unroll=4)
    row_x, line_z = lax.div(chip, 8), lax.rem(chip, 8)
    peers = [8 * lax.rem(row_x + dx, 4) + lax.rem(line_z + dz, 8) for dx, dz in STEPS]
    pltpu.make_async_copy(chip_totals.at[chip], got_totals.at[chip], recv_ct).start()
    for peer in peers:
        target = 2 * peer + core
        to_shard(target, chip_totals.at[peer], got_totals.at[chip], send_ct, recv_ct).start()
    local_pass(lax.div(mine, 8))
    leads = core == 0

    def my_summary(k):
        own = ends[pl.ds(pl.multiple_of((mine + k) * STATE, 8), STATE), :]
        return own, totals[mine + k]

    def pair_of(k):
        own_end, own_total = my_summary(k)
        other_end = pair_ends[pl.ds(pl.multiple_of(k * STATE, 8), STATE), :]
        other_total = pair_totals[k]
        return (
            jnp.where(leads, own_end, other_end), jnp.where(leads, own_total, other_total),
            jnp.where(leads, other_end, own_end), jnp.where(leads, other_total, own_total),
        )

    swap_ends.wait()

    def chip_end(k, _):
        end_a, total_a, end_b, total_b = pair_of(k)
        chip_ends[k] = jnp.exp2(rates[rate_at(mine + k), :] * total_b) * end_a + end_b
        return 0

    lax.fori_loop(0, HALF, chip_end, 0, unroll=4)
    pltpu.make_async_copy(chip_ends.at[chip], got_ends.at[chip], recv_ce).start()

    for peer in peers:
        target = 2 * peer + core
        to_shard(target, chip_ends.at[peer], got_ends.at[chip], send_ce, recv_ce).start()
    my_rate = rates[rate_at(mine + chip), :]
    for run in range(3):
        for n in range(STATE):
            cs[pl.ds(run * ROWS * SPLAT + n, ROWS, stride=SPLAT), :] = jnp.broadcast_to(
                maps[run * ROWS : (run + 1) * ROWS, n : n + 1], (ROWS, LANES)
            )

    def local_readout(group, drive, read):
        scan_group(dts, us, rates_of(group), group, (zero,) * STATE, drive, read, ys)

    def plain_readout(group, _):
        at = run_base(group)
        local_readout(group, splat_reader(bs, at), splat_reader(cs, at))
        return 0

    lax.fori_loop(0, GROUPS - 1, plain_readout, 0)
    local_readout(GROUPS - 1, mixed_reader(bs), mixed_reader(cs))
    wait_for(got_totals, recv_ct)
    wait_for(got_ends, recv_ce)

    def chain(s, state):
        leaving[s] = state
        return jnp.exp2(my_rate * got_totals[s]) * state + got_ends[s]

    lax.fori_loop(0, CHIPS, chain, jnp.zeros((STATE, LANES), F32), unroll=4)
    pltpu.make_async_copy(leaving.at[chip], landed.at[chip], recv_in).start()

    for peer in peers:
        to_shard(2 * peer + core, leaving.at[peer], landed.at[chip], send_in, recv_in).start()
    def entry_weights(group, read):
        rate = rates_of(group)

        def step(t, run_total):
            row = pl.multiple_of(t * PITCH + group * 8, 8)
            run_total = run_total + dts[pl.ds(row, 8), :]
            at = (group * ROWS + t) * (STATE * 8)
            for n in range(STATE):
                weights[pl.ds(pl.multiple_of(at + n * 8, 8), 8), :] = read(t, n) * jnp.exp2(
                    run_total * rate[n]
                )
            return run_total

        lax.fori_loop(0, ROWS, step, zero, unroll=4)

    def plain_weights(group, _):
        entry_weights(group, splat_reader(cs, run_base(group)))
        return 0

    lax.fori_loop(0, GROUPS - 1, plain_weights, 0)
    entry_weights(GROUPS - 1, mixed_reader(cs))
    for load in loads[9:]:
        load.wait()

    def prepare(slot, act, skip, gate):
        rows = pl.ds(pl.multiple_of(slot * ROWS, 8), ROWS)
        base[rows, :] = ys[pl.ds(slot, ROWS, stride=PITCH), :] + skip * act
        gates[rows, :] = silu(gate)

    for run, gate_rows in ((CLEAN, clean_gate), (CORRUPT, corrupt_gate)):
        for tile in range(CUT_TILES):
            cols = pl.ds(pl.multiple_of(v * SPAN + tile * LANES, LANES), LANES)
            act = acts[run * ROWS : (run + 1) * ROWS, cols].astype(F32)
            prepare(cut_slot(run, tile), act, d_skip[:, cols], gate_rows[:, cols].astype(F32))

    def prepare_patched(tile, _):
        cols = pl.ds(pl.multiple_of(tile * LANES, LANES), LANES)
        gate = jnp.where(
            take_gate, clean_gate[:, cols].astype(F32), corrupt_gate[:, cols].astype(F32)
        )
        prepare(tile, acts[2 * ROWS :, cols].astype(F32), d_skip[:, cols], gate)
        return 0

    lax.fori_loop(0, TILES, prepare_patched, 0, unroll=2)
    def enter(k, _):
        end_a, total_a, _, _ = pair_of(k)
        before = landed[k]
        after = jnp.exp2(rates[rate_at(mine + k), :] * total_a) * before + end_a
        at = pl.ds(pl.multiple_of((mine + k) * STATE, 8), STATE)
        start[at, :] = jnp.where(leads, before, after)
        across[pl.ds(pl.multiple_of(k * STATE, 8), STATE), :] = jnp.where(leads, after, before)
        return 0

    swap_start = to_shard(
        mate, across, start.at[pl.ds(pl.multiple_of(mine * STATE, 8), HALF * STATE)],
        send_st, recv_st,
    )

    def enter_half():
        wait_for(landed, recv_in)
        lax.fori_loop(0, HALF, enter, 0, unroll=4)
        swap_start.start()

    @pl.when(core == 1)
    def _():
        enter_half()

    @pl.when(core == 0)
    def _():
        swap_start.wait_recv()

    def final_group(group, _):
        at = group * (STATE * 8)
        state = [start[pl.ds(at + n, 8, stride=STATE), :] for n in range(STATE)]

        def step(t, _):
            at = (group * ROWS + t) * (STATE * 8)
            total = None
            for n in range(STATE):
                term = weights[pl.ds(pl.multiple_of(at + n * 8, 8), 8), :] * state[n]
                total = term if total is None else total + term
            ys[pl.ds(pl.multiple_of(t * PITCH + group * 8, 8), 8), :] = total
            return 0

        lax.fori_loop(0, ROWS, step, 0, unroll=8)
        return 0

    def result(slot):
        rows = pl.ds(pl.multiple_of(slot * ROWS, 8), ROWS)
        y = ys[pl.ds(slot, ROWS, stride=PITCH), :]
        return ((y + base[rows, :]) * gates[rows, :]).astype(BF16)

    lax.fori_loop(6, GROUPS, final_group, 0)

    for tile in range(CUT_TILES):
        cut[:, tile * LANES : (tile + 1) * LANES] = result(cut_slot(CORRUPT, tile))
    directs = [
        to_variant(k, cut, whole.at[v], send_cut.at[k], recv_cut.at[k]) for k in (2, 1, VARS - 1)
    ]
    for direct in directs:
        direct.start()
    @pl.when(core == 0)
    def _():
        enter_half()

    @pl.when(core == 1)
    def _():
        swap_start.wait_recv()

    final_group(5, 0)
    squares[...] = jnp.zeros_like(squares)
    for tile in range(CUT_TILES):
        gap = result(cut_slot(CLEAN, tile)).astype(F32)
        gap = gap - cut[:, tile * LANES : (tile + 1) * LANES].astype(F32)
        squares[tile : tile + 1, :] = jnp.sum(gap * gap, axis=0, keepdims=True)

    def along_z(k):
        return 16 * row_x + 2 * lax.rem(line_z + k, 8) + 1

    def along_x(k):
        return 16 * lax.rem(row_x + k, 4) + 2 * line_z + 1

    def share(peer_of, count, slot, src, dst, send_sem, recv_sem):
        for k in range(1, count):
            to_shard(peer_of(k), src, dst.at[slot], send_sem, recv_sem).start()
        dst[slot] = src[...]

    seven, three = pl.ds(0, 7), pl.ds(0, 3)
    squares_over = to_shard(mate, squares, pair_squares, send_qq, recv_qq)

    @pl.when(core == 0)
    def _():
        squares_over.start()

    whole[v] = cut[...]

    lax.fori_loop(0, 5, final_group, 0)
    def patched_tile(tile, _):
        cols = pl.ds(pl.multiple_of(tile * LANES, LANES), LANES)
        patched[:, cols] = result(tile)
        return 0

    lax.fori_loop(0, TILES, patched_tile, 0, unroll=4)

    save = pltpu.make_async_copy(patched, patched_out, load_sem.at[0])
    save.start()

    @pl.when(core == 1)
    def _():
        squares_over.wait_recv()
        chip_squares[...] = squares[...] + pair_squares[...]
        share(along_z, 8, line_z, chip_squares, squares_z, send_sz, recv_sz)

    for direct in directs:
        direct.wait()

    for w in range(VARS):
        def peak_tile(i, _):
            here = pl.ds(pl.multiple_of(i * LANES, LANES), LANES)
            there = pl.ds(pl.multiple_of(w * SPAN + i * LANES, LANES), LANES)
            gap = jnp.abs(patched[:, there].astype(F32) - whole[w, :, here].astype(F32))
            peaks[pl.ds(w * CUT_TILES + i, 1), :] = jnp.max(gap, axis=0, keepdims=True)
            return 0

        lax.fori_loop(0, CUT_TILES, peak_tile, 0, unroll=2)

    peaks_over = to_shard(mate, peaks, pair_peaks, send_pp, recv_pp)
    answer_over = to_shard(mate, answer, answer, send_an, recv_an)

    @pl.when(core == 0)
    def _():
        peaks_over.start()

    @pl.when(core == 1)
    def _():
        wait_for(squares_z.at[seven], recv_sz)
        line_squares[...] = jnp.sum(squares_z[...], axis=0)
        share(along_x, 4, row_x, line_squares, squares_x, send_sx, recv_sx)
        peaks_over.wait_recv()
        chip_peaks[...] = jnp.maximum(peaks[...], pair_peaks[...])
        share(along_z, 8, line_z, chip_peaks, peaks_z, send_pz, recv_pz)
        wait_for(squares_x.at[three], recv_sx)
        spreads[v] = jnp.sqrt(jnp.sum(squares_x[...], axis=0) / (SHARDS * ROWS) + TINY)
        for k in range(1, VARS):
            to_variant(k, spreads.at[v], spreads.at[v], send_sp.at[k], recv_sp.at[k]).start()
        wait_for(peaks_z.at[seven], recv_pz)
        line_peaks[...] = jnp.max(peaks_z[...], axis=0)
        share(along_x, 4, row_x, line_peaks, peaks_x, send_px, recv_px)
        wait_for(peaks_x.at[three], recv_px)
        for k in range(1, VARS):
            there = spreads.at[lax.rem(v + VARS - k, VARS)]
            to_variant(k, there, there, send_sp.at[k], recv_sp.at[k]).wait()
        peak = jnp.max(peaks_x[...], axis=0)
        for w in range(VARS):
            rows = slice(w * CUT_TILES, (w + 1) * CUT_TILES)
            answer[rows, :] = peak[rows, :] / spreads[w, :CUT_TILES, :]
        answer_over.start()
        wait_for(squares_z.at[seven], send_sz)
        wait_for(squares_x.at[three], send_sx)
        wait_for(peaks_z.at[seven], send_pz)
        wait_for(peaks_x.at[three], send_px)
        answer_over.wait_send()

    @pl.when(core == 0)
    def _():
        squares_over.wait_send()
        peaks_over.wait_send()
        answer_over.wait_recv()

    effect[...] = answer[...]
    save.wait()
    others = pl.ds(0, CHIPS - 1)
    wait_for(chip_totals.at[others], send_ct)
    wait_for(chip_ends.at[others], send_ce)
    wait_for(leaving.at[others], send_in)

    swap_start.wait_send()


SMEM = pl.BlockSpec(memory_space=pltpu.SMEM)
HBM = pl.BlockSpec(memory_space=pltpu.HBM)
VMEM = pl.BlockSpec(memory_space=pltpu.VMEM)
DMA = pltpu.SemaphoreType.DMA


def shards(
    clean_proj, corrupt_proj, patch_pos, patch_mode, a_log, dt_bias,
    conv_weight, conv_bias, x_weight, dt_weight, d_skip,
):
    rims = pl.pallas_call(
        halo_kernel,
        out_shape=jax.ShapeDtypeStruct((8, INNER), BF16),
        in_specs=[HBM, HBM],
        out_specs=HBM,
        scratch_shapes=[
            pltpu.VMEM((2, 8, INNER), BF16), pltpu.VMEM((8, INNER), F32),
            pltpu.VMEM((8, INNER), BF16), DMA((2,)), DMA, DMA,
        ],
        compiler_params=pltpu.CompilerParams(
            collective_id=1, has_side_effects=True, vmem_limit_bytes=67_043_328
        ),
        name="halo",
    )(clean_proj, corrupt_proj)
    row = (1, LANES)
    tile = (STATE, LANES)
    patched, effect = pl.pallas_call(
        kernel,
        out_shape=(
            jax.ShapeDtypeStruct((ROWS, INNER), BF16),
            jax.ShapeDtypeStruct((TILES, LANES), F32),
        ),
        in_specs=[SMEM, SMEM] + [HBM] * 10,
        out_specs=(HBM, VMEM),
        scratch_shapes=[
            pltpu.VMEM((ROWS, INNER), BF16),
            pltpu.VMEM((ROWS, INNER), BF16),
            pltpu.VMEM((ROWS, INNER), BF16),
            pltpu.VMEM((ROWS, INNER), BF16),
            pltpu.VMEM((ROWS, INNER), BF16),
            pltpu.VMEM((8, INNER), BF16),
            pltpu.VMEM((TAPS, INNER), F32),
            pltpu.VMEM((1, INNER), F32),
            pltpu.VMEM((RANK + 2 * STATE, INNER), BF16),
            pltpu.VMEM((RANK, INNER), BF16),
            pltpu.VMEM((1, INNER), F32),
            pltpu.VMEM((STATE, INNER), F32),
            pltpu.VMEM((1, INNER), F32),
            pltpu.VMEM((3 * TILES * (8 + ROWS), LANES), F32),
            pltpu.VMEM((3 * ROWS, INNER), BF16),
            pltpu.VMEM((3 * ROWS, RANK), BF16),
            pltpu.VMEM((3 * ROWS, STATE), F32),
            pltpu.VMEM((GROUPS * ROWS * STATE * 8, LANES), F32),
            pltpu.VMEM((CHUNKS * ROWS, LANES), F32),
            pltpu.VMEM((CHUNKS * ROWS, LANES), F32),
            pltpu.VMEM((ROWS * PITCH, LANES), F32),
            pltpu.VMEM((ROWS * PITCH, LANES), F32),
            pltpu.VMEM((3 * ROWS * SPLAT + 8, LANES), F32),
            pltpu.VMEM((3 * ROWS * SPLAT + 8, LANES), F32),
            pltpu.VMEM((CHUNKS * STATE, LANES), F32),
            pltpu.VMEM((CHUNKS * STATE, LANES), F32),
            pltpu.VMEM((CHUNKS, *row), F32),
            pltpu.VMEM((HALF * STATE, LANES), F32),
            pltpu.VMEM((HALF, *row), F32),
            pltpu.VMEM((HALF, *tile), F32),
            pltpu.VMEM((HALF, *row), F32),
            pltpu.VMEM((CHIPS, *tile), F32),
            pltpu.VMEM((CHIPS, *row), F32),
            pltpu.VMEM((CHIPS, *tile), F32),
            pltpu.VMEM((HALF, *tile), F32),
            pltpu.VMEM((HALF * STATE, LANES), F32),
            pltpu.VMEM((CHUNKS * STATE, LANES), F32),
            pltpu.VMEM((ROWS * PITCH, LANES), F32),
            pltpu.VMEM((ROWS, SPAN), BF16),
            pltpu.VMEM((STATE, LANES), F32),
            pltpu.VMEM((VARS, ROWS, SPAN), BF16),
            pltpu.VMEM((TILES, LANES), F32),
            pltpu.VMEM((8, STATE, LANES), F32),
            pltpu.VMEM((STATE, LANES), F32),
            pltpu.VMEM((4, STATE, LANES), F32),
            pltpu.VMEM((VARS, STATE, LANES), F32),
            pltpu.VMEM((8, TILES, LANES), F32),
            pltpu.VMEM((TILES, LANES), F32),
            pltpu.VMEM((4, TILES, LANES), F32),
            pltpu.VMEM((STATE, LANES), F32),
            pltpu.VMEM((STATE, LANES), F32),
            pltpu.VMEM((TILES, LANES), F32),
            pltpu.VMEM((TILES, LANES), F32),
            pltpu.VMEM((TILES, LANES), F32),
            DMA((12,)),
        ]
        + [DMA] * 12
        + [DMA((VARS,)), DMA((VARS,))]
        + [DMA] * 4
        + [DMA((VARS,)), DMA((VARS,))]
        + [DMA] * 10,
        compiler_params=pltpu.CompilerParams(
            collective_id=0, has_side_effects=True, vmem_limit_bytes=67_043_328
        ),
        name="mixer",
    )(
        patch_pos, patch_mode, clean_proj, corrupt_proj, rims, conv_weight, conv_bias[None],
        x_weight.T, dt_weight, dt_bias[None], a_log, d_skip[None],
    )
    patched, effect = pl.pallas_call(
        emit_kernel,
        out_shape=(
            jax.ShapeDtypeStruct((ROWS, INNER), BF16),
            jax.ShapeDtypeStruct((TILES, LANES), F32),
        ),
        in_specs=[HBM, HBM],
        out_specs=(HBM, HBM),
        scratch_shapes=[
            pltpu.VMEM((ROWS, INNER), BF16), pltpu.VMEM((TILES, LANES), F32), DMA((3,)), DMA((3,)),
        ],
        compiler_params=pltpu.CompilerParams(vmem_limit_bytes=67_043_328),
        name="emit",
    )(patched, effect)
    return (patched[None], effect.reshape(1, INNER))


def solution(mesh):
    return jax.shard_map(
        shards,
        mesh=mesh,
        in_specs=(
            P("seq", None), P("seq", None), P("var", None), P("var"),
            P(), P(), P(), P(), P(), P(), P(),
        ),
        out_specs=(P("var", "seq", None), P("var", None)),
        check_vma=False,
    )
```

```python
import functools

import jax
import jax.numpy as jnp
from jax import lax
from jax.experimental import pallas as pl
from jax.experimental.pallas import tpu as pltpu
from jax.sharding import PartitionSpec as P

STATE = 16
RANK = 160
ROWS = 32
INNER = 5120
SPAN = 1280
TAPS = 4
LANES = 128
CHUNKS = 64
SHARDS = 64
VARS = 4
TILES = INNER // LANES
CUT_TILES = SPAN // LANES
GROUPS = CHUNKS // 8
HALF = CHUNKS // 2
CHIPS = SHARDS // 2
PITCH = 72
SPLAT = 17
MESH = pl.DeviceIdType.MESH
LOG2E = 1.4426950408889634
TINY = 1e-06
F32 = jnp.float32
BF16 = jnp.bfloat16
UNROLL = 8
CLEAN, CORRUPT, PATCHED = 0, 1, 2
STEPS = sorted(
    ((dx, dz) for dx in range(4) for dz in range(8) if dx or dz),
    key=lambda step: -(min(step[0], 4 - step[0]) + min(step[1], 8 - step[1])),
)


def cut_slot(run, tile):
    if tile < 8:
        return TILES + 8 * run + tile
    return 56 + 2 * run + (tile - 8)


def hit_rows(pos_ref, first, count):
    rows = first + lax.broadcasted_iota(jnp.int32, (count, LANES), 0)
    hits = rows == pos_ref[0, 0]
    for k in range(1, pos_ref.shape[1]):
        hits = hits | (rows == pos_ref[0, k])
    return hits


def silu(value):
    return value / (1.0 + jnp.exp(-value))


def softplus(value):
    return jnp.maximum(value, 0.0) + jnp.log1p(jnp.exp(-jnp.abs(value)))


def row_of(ref, row):
    return jnp.broadcast_to(ref[pl.ds(row, 1), :], (8, LANES))


def scan_group(dts, us, rate, group, state, drive, readout, out):
    def step(t, carry):
        row = pl.multiple_of(t * PITCH + group * 8, 8)
        steps = dts[pl.ds(row, 8), :]
        flow = us[pl.ds(row, 8), :]
        entries = []
        total = None
        for n in range(STATE):
            decay = jnp.exp2(steps * rate[n])
            entry = decay * carry[n] + flow * drive(t, n)
            entries.append(entry)
            if readout is not None:
                term = readout(t, n) * entry
                total = term if total is None else total + term
        if readout is not None:
            out[pl.ds(row, 8), :] = total
        return tuple(entries)

    return lax.fori_loop(0, ROWS, step, state, unroll=UNROLL)


def splat_reader(ref, base):
    return lambda t, n: row_of(ref, base + t * SPLAT + n)


def mixed_reader(ref):
    first = lax.broadcasted_iota(jnp.int32, (8, LANES), 0) < 2

    def read(t, n):
        return jnp.where(
            first,
            row_of(ref, CLEAN * ROWS * SPLAT + t * SPLAT + n),
            row_of(ref, CORRUPT * ROWS * SPLAT + t * SPLAT + n),
        )

    return read


def wait_for(ref, sem):
    pltpu.make_async_copy(ref, ref, sem).wait()


def front_kernel(
    pos, mode, clean_in, corrupt_in, conv_w_in, conv_b_in, x_w_in, dt_w_in, dt_b_in, a_log_in,
    acts, x_w, dt_w, dt_b, a_log,
    rims, ends, wide, packed, clean, corrupt, conv_w, conv_b, pad, load_sem, send_sem, recv_sem,
):
    me = lax.axis_index("seq")
    v = lax.axis_index("var")
    after = lax.min(me + 1, SHARDS - 1)
    has_next, has_last = me < SHARDS - 1, me > 0
    barrier = pltpu.get_barrier_semaphore()
    loads = [
        pltpu.make_async_copy(src, dst, load_sem.at[i])
        for i, (src, dst) in enumerate(
            (
                (clean_in.at[ROWS - 8 :, :INNER], ends.at[0]),
                (corrupt_in.at[ROWS - 8 :, :INNER], ends.at[1]),
                (clean_in.at[:, :INNER], clean), (corrupt_in.at[:, :INNER], corrupt),
                (conv_w_in, conv_w), (conv_b_in, conv_b), (x_w_in, x_w), (dt_w_in, dt_w),
                (dt_b_in, dt_b), (a_log_in, a_log),
            )
        )
    ]
    for load in loads:
        load.start()

    def signal(peer):
        pl.semaphore_signal(barrier, inc=1, device_id=(peer, v), device_id_type=MESH)

    @pl.when(has_next)
    def _():
        signal(me + 1)

    @pl.when(has_last)
    def _():
        signal(me - 1)

    for load in loads[:2]:
        load.wait()
    margin = TAPS - 1
    wide[...] = jnp.zeros_like(wide)
    for i in range(2):
        wide[i * margin : (i + 1) * margin, :] = ends[i].astype(F32)[8 - margin :, :]
    packed[...] = wide[...].astype(BF16)
    first = me * ROWS
    take = hit_rows(pos, first, ROWS)[:, :1] & (mode[0] != 1)
    take_rim = hit_rows(pos, first - margin, margin)[:, :1] & (mode[0] != 1)
    pl.semaphore_wait(barrier, lax.min(me, 1) + lax.min(SHARDS - 1 - me, 1))
    copy = pltpu.make_async_remote_copy(
        src_ref=packed, dst_ref=rims, send_sem=send_sem, recv_sem=recv_sem,
        device_id=(after, v), device_id_type=MESH,
    )

    @pl.when(has_next)
    def _():
        copy.start()

    for load in loads[2:6]:
        load.wait()
    width = 512
    span = 8 + ROWS
    per = width // LANES

    def columns(i):
        return pl.ds(pl.multiple_of(i * width, width), width)

    def fill(i, _):
        sig_clean = clean[:, columns(i)].astype(F32)
        sig_corrupt = corrupt[:, columns(i)].astype(F32)
        pieces = (sig_clean, sig_corrupt, jnp.where(take, sig_clean, sig_corrupt))
        for run, sig in enumerate(pieces):
            for k in range(per):
                at = pl.multiple_of((run * TILES + i * per + k) * span, 8)
                pad[pl.ds(at, 8), :] = jnp.zeros((8, LANES), F32)
                pad[pl.ds(at + 8, ROWS), :] = sig[:, k * LANES : (k + 1) * LANES]
        return 0

    def convolve(rows):
        def body(tile, _):
            cols = pl.ds(pl.multiple_of(tile * LANES, LANES), LANES)
            bias = conv_b[:, cols]
            for run in range(3):
                at = (run * TILES + tile) * span + 8 - margin
                total = bias + conv_w[0:1, cols] * pad[pl.ds(at, rows), :]
                for k in range(1, TAPS):
                    total = total + conv_w[k : k + 1, cols] * pad[pl.ds(at + k, rows), :]
                acts[run * ROWS : run * ROWS + rows, cols] = silu(total).astype(BF16)
            return 0

        lax.fori_loop(0, TILES, body, 0, unroll=4)

    def fill_rim(i, _):
        rim = rims[:, columns(i)].astype(F32)
        rim_clean, rim_corrupt = rim[:margin], rim[margin : 2 * margin]
        pieces = (rim_clean, rim_corrupt, jnp.where(take_rim, rim_clean, rim_corrupt))
        for run, part in enumerate(pieces):
            for k in range(per):
                at = (run * TILES + i * per + k) * span + 8 - margin
                pad[pl.ds(at, margin), :] = part[:, k * LANES : (k + 1) * LANES]
        return 0

    lax.fori_loop(0, INNER // width, fill, 0)
    convolve(ROWS)

    @pl.when(has_last)
    def _():
        copy.wait_recv()
        lax.fori_loop(0, INNER // width, fill_rim, 0)
        convolve(8)

    for load in loads[6:]:
        load.wait()

    @pl.when(has_next)
    def _():
        copy.wait_send()


def emit_kernel(patched, effect, patched_out, effect_out, sems):
    copies = [
        pltpu.make_async_copy(patched, patched_out, sems.at[0]),
        pltpu.make_async_copy(effect, effect_out, sems.at[1]),
    ]
    for copy in copies:
        copy.start()
    for copy in copies:
        copy.wait()


def kernel(
    pos, mode, acts, x_w, dt_w, dt_b, a_log, clean_in, corrupt_in, d_skip_in,
    patched, effect,
    clean_gate, corrupt_gate, d_skip, low, maps, weights, base, gates, dts, us, bs, cs, rates, ends, totals,
    pair_ends, pair_totals, chip_ends, got_ends,
    leaving, landed, across, start, ys,
    cut, squares, whole, peaks, squares_z, line_squares, squares_x, spreads,
    peaks_z, line_peaks, peaks_x, pair_squares, chip_squares, pair_peaks, chip_peaks, answer,
    load_sem, send_pt, recv_pt, send_pe, recv_pe, send_ce, recv_ce,
    send_in, recv_in, send_st, recv_st,
    send_cut, recv_cut, send_sz, recv_sz, send_sx, recv_sx, send_sp, recv_sp,
    send_pz, recv_pz, send_px, recv_px, send_qq, recv_qq, send_pp, recv_pp, send_an, recv_an,
):
    me = lax.axis_index("seq")
    v = lax.axis_index("var")
    chip = lax.div(me, 2)
    core = lax.rem(me, 2)
    mate = me + 1 - 2 * core
    mine = core * HALF
    theirs = HALF - mine
    barrier = pltpu.get_barrier_semaphore()

    loads = [
        pltpu.make_async_copy(src, dst, load_sem.at[i])
        for i, (src, dst) in enumerate(
            (
                (d_skip_in, d_skip), (clean_in.at[:, INNER:], clean_gate),
                (corrupt_in.at[:, INNER:], corrupt_gate),
            )
        )
    ]
    for load in loads:
        load.start()

    def signal(peer, variant):
        pl.semaphore_signal(barrier, inc=1, device_id=(peer, variant), device_id_type=MESH)

    row_x, line_z = lax.div(chip, 8), lax.rem(chip, 8)
    peers = [8 * lax.rem(row_x + dx, 4) + lax.rem(line_z + dz, 8) for dx, dz in STEPS]
    for peer in peers:
        signal(2 * peer + core, v)
    signal(mate, v)
    for k in range(1, VARS):
        signal(me, lax.rem(v + k, VARS))

    def to_variant(k, src, dst, send_sem, recv_sem):
        return pltpu.make_async_remote_copy(
            src_ref=src, dst_ref=dst, send_sem=send_sem, recv_sem=recv_sem,
            device_id=(me, lax.rem(v + k, VARS)), device_id_type=MESH,
        )

    def to_shard(peer, src, dst, send_sem, recv_sem):
        return pltpu.make_async_remote_copy(
            src_ref=src, dst_ref=dst, send_sem=send_sem, recv_sem=recv_sem,
            device_id=(peer, v), device_id_type=MESH,
        )

    take_gate = hit_rows(pos, me * ROWS, ROWS)[:, :1] & (mode[0] != 0)

    projected = lax.dot_general(
        acts[...], x_w[...], (((1,), (1,)), ((), ())), preferred_element_type=F32
    )
    low[...] = projected[:, :RANK].astype(BF16)
    maps[...] = projected[:, RANK + STATE :]
    for run in range(3):
        part = projected[run * ROWS : (run + 1) * ROWS]
        for n in range(STATE):
            at = run * ROWS * SPLAT + n
            bs[pl.ds(at, ROWS, stride=SPLAT), :] = jnp.broadcast_to(
                part[:, RANK + n : RANK + n + 1], (ROWS, LANES)
            )


    def rate_at(slot):
        return pl.ds(lax.div(slot, 8) * (STATE * 8) + lax.rem(slot, 8), STATE, stride=8)

    def place(slot, steps, act, log_rate):
        dts[pl.ds(slot, ROWS, stride=PITCH), :] = steps
        us[pl.ds(slot, ROWS, stride=PITCH), :] = steps * act
        totals[slot] = jnp.sum(steps, axis=0, keepdims=True)
        rates[rate_at(slot), :] = jnp.exp(log_rate) * (-LOG2E)

    wide = 1280

    def patched_steps(i, _):
        cols = pl.ds(pl.multiple_of(i * wide, wide), wide)
        raw = jnp.dot(low[2 * ROWS :, :], dt_w[:, cols], preferred_element_type=F32)
        steps = softplus(raw + dt_b[:, cols])
        act = acts[2 * ROWS :, cols].astype(F32)
        logs = a_log[:, cols]
        for k in range(wide // LANES):
            part = slice(k * LANES, (k + 1) * LANES)
            place(i * (wide // LANES) + k, steps[:, part], act[:, part], logs[:, part])
        return 0

    lax.fori_loop(0, INNER // wide, patched_steps, 0)

    cols = pl.ds(pl.multiple_of(v * SPAN, LANES), SPAN)
    raw = jnp.dot(low[: 2 * ROWS, :], dt_w[:, cols], preferred_element_type=F32)
    steps = softplus(raw + dt_b[:, cols])
    act = acts[: 2 * ROWS, cols].astype(F32)
    logs = a_log[:, cols]
    for run in (CLEAN, CORRUPT):
        rows = slice(run * ROWS, (run + 1) * ROWS)
        for tile in range(CUT_TILES):
            part = slice(tile * LANES, (tile + 1) * LANES)
            place(cut_slot(run, tile), steps[rows, part], act[rows, part], logs[:, part])
    blank = jnp.zeros((ROWS, LANES), F32)
    for slot in range(60, CHUNKS):
        place(slot, blank, blank, jnp.zeros((STATE, LANES), F32))

    zero = jnp.zeros((8, LANES), F32)

    def rates_of(group):
        base = group * (STATE * 8)
        return [rates[pl.ds(pl.multiple_of(base + n * 8, 8), 8), :] for n in range(STATE)]

    def run_base(group):
        return jnp.where(group < 5, PATCHED, group - 5) * (ROWS * SPLAT)

    def local_group(group, drive):
        found = scan_group(
            dts, us, rates_of(group), group, (zero,) * STATE, drive, None, None
        )
        for n in range(STATE):
            ends[pl.ds(group * (STATE * 8) + n, 8, stride=STATE), :] = found[n]

    def local_pass(offset):
        def body(i, _):
            group = offset + i

            @pl.when(group < GROUPS - 1)
            def _():
                local_group(group, splat_reader(bs, run_base(group)))

            @pl.when(group == GROUPS - 1)
            def _():
                local_group(group, mixed_reader(bs))

            return 0

        lax.fori_loop(0, GROUPS // 2, body, 0)

    local_pass(lax.div(theirs, 8))
    pl.semaphore_wait(barrier, CHIPS - 1 + 1 + VARS - 1)
    theirs_3 = pl.ds(theirs, HALF)
    swap_totals = to_shard(mate, totals.at[theirs_3], pair_totals, send_pt, recv_pt)
    swap_totals.start()

    theirs_2 = pl.ds(pl.multiple_of(theirs * STATE, 8), HALF * STATE)
    swap_ends = to_shard(mate, ends.at[theirs_2], pair_ends, send_pe, recv_pe)
    swap_ends.start()
    local_pass(lax.div(mine, 8))
    swap_totals.wait()

    leads = core == 0

    def my_summary(k):
        own = ends[pl.ds(pl.multiple_of((mine + k) * STATE, 8), STATE), :]
        return own, totals[mine + k]

    def pair_of(k):
        own_end, own_total = my_summary(k)
        other_end = pair_ends[pl.ds(pl.multiple_of(k * STATE, 8), STATE), :]
        other_total = pair_totals[k]
        return (
            jnp.where(leads, own_end, other_end), jnp.where(leads, own_total, other_total),
            jnp.where(leads, other_end, own_end), jnp.where(leads, other_total, own_total),
        )

    swap_ends.wait()

    def chip_end(k, _):
        end_a, total_a, end_b, total_b = pair_of(k)
        chip_ends[k, :STATE] = jnp.exp2(rates[rate_at(mine + k), :] * total_b) * end_a + end_b
        chip_ends[k, STATE:] = total_a + total_b
        return 0

    lax.fori_loop(0, HALF, chip_end, 0, unroll=4)
    pltpu.make_async_copy(chip_ends.at[chip], got_ends.at[chip], recv_ce).start()

    for peer in peers:
        target = 2 * peer + core
        to_shard(target, chip_ends.at[peer], got_ends.at[chip], send_ce, recv_ce).start()
    my_rate = rates[rate_at(mine + chip), :]
    for run in range(3):
        for n in range(STATE):
            cs[pl.ds(run * ROWS * SPLAT + n, ROWS, stride=SPLAT), :] = jnp.broadcast_to(
                maps[run * ROWS : (run + 1) * ROWS, n : n + 1], (ROWS, LANES)
            )

    def local_readout(group, drive, read):
        scan_group(dts, us, rates_of(group), group, (zero,) * STATE, drive, read, ys)

    def plain_readout(group, _):
        at = run_base(group)
        local_readout(group, splat_reader(bs, at), splat_reader(cs, at))
        return 0

    lax.fori_loop(0, GROUPS - 1, plain_readout, 0)
    local_readout(GROUPS - 1, mixed_reader(bs), mixed_reader(cs))
    wait_for(got_ends, recv_ce)

    def chain(s, state):
        leaving[s] = state
        return jnp.exp2(my_rate * got_ends[s, STATE:]) * state + got_ends[s, :STATE]

    lax.fori_loop(0, CHIPS, chain, jnp.zeros((STATE, LANES), F32), unroll=4)
    pltpu.make_async_copy(leaving.at[chip], landed.at[chip], recv_in).start()

    for peer in peers:
        to_shard(2 * peer + core, leaving.at[peer], landed.at[chip], send_in, recv_in).start()
    def entry_weights(group, read):
        rate = rates_of(group)

        def step(t, run_total):
            row = pl.multiple_of(t * PITCH + group * 8, 8)
            run_total = run_total + dts[pl.ds(row, 8), :]
            at = (group * ROWS + t) * (STATE * 8)
            for n in range(STATE):
                weights[pl.ds(pl.multiple_of(at + n * 8, 8), 8), :] = read(t, n) * jnp.exp2(
                    run_total * rate[n]
                )
            return run_total

        lax.fori_loop(0, ROWS, step, zero, unroll=4)

    def plain_weights(group, _):
        entry_weights(group, splat_reader(cs, run_base(group)))
        return 0

    lax.fori_loop(0, GROUPS - 1, plain_weights, 0)
    entry_weights(GROUPS - 1, mixed_reader(cs))
    for load in loads:
        load.wait()

    def prepare(slot, act, skip, gate):
        rows = pl.ds(pl.multiple_of(slot * ROWS, 8), ROWS)
        base[rows, :] = ys[pl.ds(slot, ROWS, stride=PITCH), :] + skip * act
        gates[rows, :] = silu(gate)

    for run, gate_rows in ((CLEAN, clean_gate), (CORRUPT, corrupt_gate)):
        for tile in range(CUT_TILES):
            cols = pl.ds(pl.multiple_of(v * SPAN + tile * LANES, LANES), LANES)
            act = acts[run * ROWS : (run + 1) * ROWS, cols].astype(F32)
            prepare(cut_slot(run, tile), act, d_skip[:, cols], gate_rows[:, cols].astype(F32))

    def prepare_patched(tile, _):
        cols = pl.ds(pl.multiple_of(tile * LANES, LANES), LANES)
        gate = jnp.where(
            take_gate, clean_gate[:, cols].astype(F32), corrupt_gate[:, cols].astype(F32)
        )
        prepare(tile, acts[2 * ROWS :, cols].astype(F32), d_skip[:, cols], gate)
        return 0

    lax.fori_loop(0, TILES, prepare_patched, 0, unroll=2)
    def enter(k, _):
        end_a, total_a, _, _ = pair_of(k)
        before = landed[k]
        after = jnp.exp2(rates[rate_at(mine + k), :] * total_a) * before + end_a
        at = pl.ds(pl.multiple_of((mine + k) * STATE, 8), STATE)
        start[at, :] = jnp.where(leads, before, after)
        across[pl.ds(pl.multiple_of(k * STATE, 8), STATE), :] = jnp.where(leads, after, before)
        return 0

    swap_start = to_shard(
        mate, across, start.at[pl.ds(pl.multiple_of(mine * STATE, 8), HALF * STATE)],
        send_st, recv_st,
    )

    def enter_half():
        wait_for(landed, recv_in)
        lax.fori_loop(0, HALF, enter, 0, unroll=4)
        swap_start.start()

    @pl.when(core == 1)
    def _():
        enter_half()

    @pl.when(core == 0)
    def _():
        swap_start.wait_recv()

    def final_group(group, _):
        at = group * (STATE * 8)
        state = [start[pl.ds(at + n, 8, stride=STATE), :] for n in range(STATE)]

        def step(t, _):
            at = (group * ROWS + t) * (STATE * 8)
            total = None
            for n in range(STATE):
                term = weights[pl.ds(pl.multiple_of(at + n * 8, 8), 8), :] * state[n]
                total = term if total is None else total + term
            ys[pl.ds(pl.multiple_of(t * PITCH + group * 8, 8), 8), :] = total
            return 0

        lax.fori_loop(0, ROWS, step, 0, unroll=8)
        return 0

    def result(slot):
        rows = pl.ds(pl.multiple_of(slot * ROWS, 8), ROWS)
        y = ys[pl.ds(slot, ROWS, stride=PITCH), :]
        return ((y + base[rows, :]) * gates[rows, :]).astype(BF16)

    lax.fori_loop(6, GROUPS, final_group, 0)

    for tile in range(CUT_TILES):
        cut[:, tile * LANES : (tile + 1) * LANES] = result(cut_slot(CORRUPT, tile))
    directs = [
        to_variant(k, cut, whole.at[v], send_cut.at[k], recv_cut.at[k]) for k in (2, 1, VARS - 1)
    ]
    for direct in directs:
        direct.start()
    @pl.when(core == 0)
    def _():
        enter_half()

    @pl.when(core == 1)
    def _():
        swap_start.wait_recv()

    final_group(5, 0)
    squares[...] = jnp.zeros_like(squares)
    for tile in range(CUT_TILES):
        gap = result(cut_slot(CLEAN, tile)).astype(F32)
        gap = gap - cut[:, tile * LANES : (tile + 1) * LANES].astype(F32)
        squares[tile : tile + 1, :] = jnp.sum(gap * gap, axis=0, keepdims=True)

    def along_z(k):
        return 16 * row_x + 2 * lax.rem(line_z + k, 8) + 1

    def along_x(k):
        return 16 * lax.rem(row_x + k, 4) + 2 * line_z + 1

    def share(peer_of, count, slot, src, dst, send_sem, recv_sem):
        for k in range(1, count):
            to_shard(peer_of(k), src, dst.at[slot], send_sem, recv_sem).start()
        dst[slot] = src[...]

    seven, three = pl.ds(0, 7), pl.ds(0, 3)
    squares_over = to_shard(mate, squares, pair_squares, send_qq, recv_qq)

    @pl.when(core == 0)
    def _():
        squares_over.start()

    whole[v] = cut[...]

    lax.fori_loop(0, 5, final_group, 0)
    def patched_tile(tile, _):
        cols = pl.ds(pl.multiple_of(tile * LANES, LANES), LANES)
        patched[:, cols] = result(tile)
        return 0

    lax.fori_loop(0, TILES, patched_tile, 0, unroll=4)


    @pl.when(core == 1)
    def _():
        squares_over.wait_recv()
        chip_squares[...] = squares[...] + pair_squares[...]
        share(along_z, 8, line_z, chip_squares, squares_z, send_sz, recv_sz)

    for direct in directs:
        direct.wait()

    for w in range(VARS):
        def peak_tile(i, _):
            here = pl.ds(pl.multiple_of(i * LANES, LANES), LANES)
            there = pl.ds(pl.multiple_of(w * SPAN + i * LANES, LANES), LANES)
            gap = jnp.abs(patched[:, there].astype(F32) - whole[w, :, here].astype(F32))
            peaks[pl.ds(w * CUT_TILES + i, 1), :] = jnp.max(gap, axis=0, keepdims=True)
            return 0

        lax.fori_loop(0, CUT_TILES, peak_tile, 0, unroll=2)

    peaks_over = to_shard(mate, peaks, pair_peaks, send_pp, recv_pp)
    answer_over = to_shard(mate, answer, answer, send_an, recv_an)

    @pl.when(core == 0)
    def _():
        peaks_over.start()

    @pl.when(core == 1)
    def _():
        wait_for(squares_z.at[seven], recv_sz)
        line_squares[...] = jnp.sum(squares_z[...], axis=0)
        share(along_x, 4, row_x, line_squares, squares_x, send_sx, recv_sx)
        peaks_over.wait_recv()
        chip_peaks[...] = jnp.maximum(peaks[...], pair_peaks[...])
        share(along_z, 8, line_z, chip_peaks, peaks_z, send_pz, recv_pz)
        wait_for(squares_x.at[three], recv_sx)
        spreads[v] = jnp.sqrt(jnp.sum(squares_x[...], axis=0) / (SHARDS * ROWS) + TINY)
        for k in range(1, VARS):
            to_variant(k, spreads.at[v], spreads.at[v], send_sp.at[k], recv_sp.at[k]).start()
        wait_for(peaks_z.at[seven], recv_pz)
        line_peaks[...] = jnp.max(peaks_z[...], axis=0)
        share(along_x, 4, row_x, line_peaks, peaks_x, send_px, recv_px)
        wait_for(peaks_x.at[three], recv_px)
        for k in range(1, VARS):
            there = spreads.at[lax.rem(v + VARS - k, VARS)]
            to_variant(k, there, there, send_sp.at[k], recv_sp.at[k]).wait()
        peak = jnp.max(peaks_x[...], axis=0)
        for w in range(VARS):
            rows = slice(w * CUT_TILES, (w + 1) * CUT_TILES)
            answer[rows, :] = peak[rows, :] / spreads[w, :CUT_TILES, :]
        answer_over.start()
        wait_for(squares_z.at[seven], send_sz)
        wait_for(squares_x.at[three], send_sx)
        wait_for(peaks_z.at[seven], send_pz)
        wait_for(peaks_x.at[three], send_px)
        answer_over.wait_send()

    @pl.when(core == 0)
    def _():
        squares_over.wait_send()
        peaks_over.wait_send()
        answer_over.wait_recv()

    effect[...] = answer[...]
    others = pl.ds(0, CHIPS - 1)
    wait_for(chip_ends.at[others], send_ce)
    wait_for(leaving.at[others], send_in)

    swap_start.wait_send()


SMEM = pl.BlockSpec(memory_space=pltpu.SMEM)
HBM = pl.BlockSpec(memory_space=pltpu.HBM)
VMEM = pl.BlockSpec(memory_space=pltpu.VMEM)
DMA = pltpu.SemaphoreType.DMA


def shards(
    clean_proj, corrupt_proj, patch_pos, patch_mode, a_log, dt_bias,
    conv_weight, conv_bias, x_weight, dt_weight, d_skip,
):
    hold = functools.partial(pltpu.with_memory_space_constraint, memory_space=pltpu.HBM)
    keep = functools.partial(pltpu.with_memory_space_constraint, memory_space=pltpu.VMEM)
    front = pl.pallas_call(
        front_kernel,
        out_shape=(
            pltpu.VMEM((3 * ROWS, INNER), BF16),
            pltpu.VMEM((RANK + 2 * STATE, INNER), BF16),
            pltpu.VMEM((RANK, INNER), BF16),
            pltpu.VMEM((1, INNER), F32),
            pltpu.VMEM((STATE, INNER), F32),
        ),
        in_specs=[SMEM, SMEM] + [HBM] * 8,
        out_specs=(VMEM,) * 5,
        scratch_shapes=[
            pltpu.VMEM((8, INNER), BF16),
            pltpu.VMEM((2, 8, INNER), BF16),
            pltpu.VMEM((8, INNER), F32),
            pltpu.VMEM((8, INNER), BF16),
            pltpu.VMEM((ROWS, INNER), BF16),
            pltpu.VMEM((ROWS, INNER), BF16),
            pltpu.VMEM((TAPS, INNER), F32),
            pltpu.VMEM((1, INNER), F32),
            pltpu.VMEM((3 * TILES * (8 + ROWS), LANES), F32),
            DMA((10,)),
            DMA,
            DMA,
        ],
        compiler_params=pltpu.CompilerParams(
            collective_id=1, has_side_effects=True, vmem_limit_bytes=40_000_000
        ),
        name="front",
    )(
        hold(patch_pos), patch_mode,
        *map(
            hold,
            (
                clean_proj, corrupt_proj, conv_weight, conv_bias[None], x_weight.T, dt_weight,
                dt_bias[None], a_log,
            ),
        ),
    )
    row = (1, LANES)
    tile = (STATE, LANES)
    patched, effect = pl.pallas_call(
        kernel,
        out_shape=(pltpu.VMEM((ROWS, INNER), BF16), pltpu.VMEM((TILES, LANES), F32)),
        in_specs=[SMEM, SMEM] + [VMEM] * 5 + [HBM] * 3,
        out_specs=(VMEM, VMEM),
        scratch_shapes=[
            pltpu.VMEM((ROWS, INNER), BF16),
            pltpu.VMEM((ROWS, INNER), BF16),
            pltpu.VMEM((1, INNER), F32),
            pltpu.VMEM((3 * ROWS, RANK), BF16),
            pltpu.VMEM((3 * ROWS, STATE), F32),
            pltpu.VMEM((GROUPS * ROWS * STATE * 8, LANES), F32),
            pltpu.VMEM((CHUNKS * ROWS, LANES), F32),
            pltpu.VMEM((CHUNKS * ROWS, LANES), F32),
            pltpu.VMEM((ROWS * PITCH, LANES), F32),
            pltpu.VMEM((ROWS * PITCH, LANES), F32),
            pltpu.VMEM((3 * ROWS * SPLAT + 8, LANES), F32),
            pltpu.VMEM((3 * ROWS * SPLAT + 8, LANES), F32),
            pltpu.VMEM((CHUNKS * STATE, LANES), F32),
            pltpu.VMEM((CHUNKS * STATE, LANES), F32),
            pltpu.VMEM((CHUNKS, *row), F32),
            pltpu.VMEM((HALF * STATE, LANES), F32),
            pltpu.VMEM((HALF, *row), F32),
            pltpu.VMEM((HALF, STATE + 1, LANES), F32),
            pltpu.VMEM((CHIPS, STATE + 1, LANES), F32),
            pltpu.VMEM((CHIPS, *tile), F32),
            pltpu.VMEM((HALF, *tile), F32),
            pltpu.VMEM((HALF * STATE, LANES), F32),
            pltpu.VMEM((CHUNKS * STATE, LANES), F32),
            pltpu.VMEM((ROWS * PITCH, LANES), F32),
            pltpu.VMEM((ROWS, SPAN), BF16),
            pltpu.VMEM((STATE, LANES), F32),
            pltpu.VMEM((VARS, ROWS, SPAN), BF16),
            pltpu.VMEM((TILES, LANES), F32),
            pltpu.VMEM((8, STATE, LANES), F32),
            pltpu.VMEM((STATE, LANES), F32),
            pltpu.VMEM((4, STATE, LANES), F32),
            pltpu.VMEM((VARS, STATE, LANES), F32),
            pltpu.VMEM((8, TILES, LANES), F32),
            pltpu.VMEM((TILES, LANES), F32),
            pltpu.VMEM((4, TILES, LANES), F32),
            pltpu.VMEM((STATE, LANES), F32),
            pltpu.VMEM((STATE, LANES), F32),
            pltpu.VMEM((TILES, LANES), F32),
            pltpu.VMEM((TILES, LANES), F32),
            pltpu.VMEM((TILES, LANES), F32),
            DMA((3,)),
        ]
        + [DMA] * 10
        + [DMA((VARS,)), DMA((VARS,))]
        + [DMA] * 4
        + [DMA((VARS,)), DMA((VARS,))]
        + [DMA] * 10,
        compiler_params=pltpu.CompilerParams(
            collective_id=0, has_side_effects=True, vmem_limit_bytes=54_000_000
        ),
        name="mixer",
    )(
        hold(patch_pos), patch_mode, *map(keep, front),
        *map(hold, (clean_proj, corrupt_proj, d_skip[None])),
    )
    patched, effect = pl.pallas_call(
        emit_kernel,
        out_shape=(
            jax.ShapeDtypeStruct((ROWS, INNER), BF16),
            jax.ShapeDtypeStruct((TILES, LANES), F32),
        ),
        in_specs=[VMEM, VMEM],
        out_specs=(HBM, HBM),
        scratch_shapes=[DMA((2,))],
        compiler_params=pltpu.CompilerParams(vmem_limit_bytes=16_000_000),
        name="emit",
    )(
        keep(patched), keep(effect),
    )
    return (patched[None], effect.reshape(1, INNER))


def solution(mesh):
    return jax.shard_map(
        shards,
        mesh=mesh,
        in_specs=(
            P("seq", None), P("seq", None), P("var", None), P("var"),
            P(), P(), P(), P(), P(), P(), P(),
        ),
        out_specs=(P("var", "seq", None), P("var", None)),
        check_vma=False,
    )
```

```python
import functools

import jax
import jax.numpy as jnp
from jax import lax
from jax.experimental import pallas as pl
from jax.experimental.pallas import tpu as pltpu
from jax.sharding import PartitionSpec as P

STATE = 16
RANK = 160
ROWS = 32
INNER = 5120
SPAN = 1280
TAPS = 4
LANES = 128
CHUNKS = 64
SHARDS = 64
VARS = 4
TILES = INNER // LANES
CUT_TILES = SPAN // LANES
GROUPS = CHUNKS // 8
BUSY = 28
HALF = CHUNKS // 2
CHIPS = SHARDS // 2
PITCH = 72
SPLAT = 17
MESH = pl.DeviceIdType.MESH
LOG2E = 1.4426950408889634
TINY = 1e-06
F32 = jnp.float32
BF16 = jnp.bfloat16
UNROLL = 8
CLEAN, CORRUPT, PATCHED = 0, 1, 2
STEPS = sorted(
    ((dx, dz) for dx in range(4) for dz in range(8) if dx or dz),
    key=lambda step: -(min(step[0], 4 - step[0]) + min(step[1], 8 - step[1])),
)


def cut_slot(run, tile):
    if tile < 8:
        return TILES + 8 * run + tile
    return 56 + 2 * run + (tile - 8)


def rate_at(slot):
    return pl.ds(lax.div(slot, 8) * (STATE * 8) + lax.rem(slot, 8), STATE, stride=8)


def hit_rows(pos_ref, first, count):
    rows = first + lax.broadcasted_iota(jnp.int32, (count, LANES), 0)
    hits = rows == pos_ref[0, 0]
    for k in range(1, pos_ref.shape[1]):
        hits = hits | (rows == pos_ref[0, k])
    return hits


def silu(value):
    return value / (1.0 + jnp.exp(-value))


def softplus(value):
    return jnp.maximum(value, 0.0) + jnp.log1p(jnp.exp(-jnp.abs(value)))


def row_of(ref, row):
    return jnp.broadcast_to(ref[pl.ds(row, 1), :], (8, LANES))


def scan_group(dts, us, rate, group, state, drive, readout, out):
    def step(t, carry):
        row = pl.multiple_of(t * PITCH + group * 8, 8)
        steps = dts[pl.ds(row, 8), :]
        flow = us[pl.ds(row, 8), :]
        entries = []
        total = None
        for n in range(STATE):
            decay = jnp.exp2(steps * rate[n])
            entry = decay * carry[n] + flow * drive(t, n)
            entries.append(entry)
            if readout is not None:
                term = readout(t, n) * entry
                total = term if total is None else total + term
        if readout is not None:
            out[pl.ds(row, 8), :] = total
        return tuple(entries)

    return lax.fori_loop(0, ROWS, step, state, unroll=UNROLL)


def splat_reader(ref, base):
    return lambda t, n: row_of(ref, base + t * SPLAT + n)


def mixed_reader(ref):
    first = lax.broadcasted_iota(jnp.int32, (8, LANES), 0) < 2

    def read(t, n):
        return jnp.where(
            first,
            row_of(ref, CLEAN * ROWS * SPLAT + t * SPLAT + n),
            row_of(ref, CORRUPT * ROWS * SPLAT + t * SPLAT + n),
        )

    return read


def wait_for(ref, sem):
    pltpu.make_async_copy(ref, ref, sem).wait()


def front_kernel(
    pos, mode, clean_in, corrupt_in, conv_w_in, conv_b_in, x_w_in, dt_w_in, dt_b_in, a_log_in,
    acts, x_w, dt_w, dt_b, rates,
    rims, a_log, ends, wide, packed, clean, corrupt, conv_w, conv_b, pad, load_sem, send_sem, recv_sem,
):
    me = lax.axis_index("seq")
    v = lax.axis_index("var")
    after = lax.min(me + 1, SHARDS - 1)
    has_next, has_last = me < SHARDS - 1, me > 0
    barrier = pltpu.get_barrier_semaphore()
    loads = [
        pltpu.make_async_copy(src, dst, load_sem.at[i])
        for i, (src, dst) in enumerate(
            (
                (clean_in.at[ROWS - 8 :, :INNER], ends.at[0]),
                (corrupt_in.at[ROWS - 8 :, :INNER], ends.at[1]),
                (clean_in.at[:, :INNER], clean), (corrupt_in.at[:, :INNER], corrupt),
                (conv_w_in, conv_w), (conv_b_in, conv_b), (x_w_in, x_w), (dt_w_in, dt_w),
                (dt_b_in, dt_b), (a_log_in, a_log),
            )
        )
    ]
    for load in loads:
        load.start()

    def signal(peer):
        pl.semaphore_signal(barrier, inc=1, device_id=(peer, v), device_id_type=MESH)

    @pl.when(has_next)
    def _():
        signal(me + 1)

    @pl.when(has_last)
    def _():
        signal(me - 1)

    for load in loads[:2]:
        load.wait()
    margin = TAPS - 1
    wide[...] = jnp.zeros_like(wide)
    for i in range(2):
        wide[i * margin : (i + 1) * margin, :] = ends[i].astype(F32)[8 - margin :, :]
    packed[...] = wide[...].astype(BF16)
    first = me * ROWS
    take = hit_rows(pos, first, ROWS)[:, :1] & (mode[0] != 1)
    take_rim = hit_rows(pos, first - margin, margin)[:, :1] & (mode[0] != 1)
    pl.semaphore_wait(barrier, lax.min(me, 1) + lax.min(SHARDS - 1 - me, 1))
    copy = pltpu.make_async_remote_copy(
        src_ref=packed, dst_ref=rims, send_sem=send_sem, recv_sem=recv_sem,
        device_id=(after, v), device_id_type=MESH,
    )

    @pl.when(has_next)
    def _():
        copy.start()

    for load in loads[2:6]:
        load.wait()
    width = 512
    span = 8 + ROWS
    per = width // LANES

    def columns(i):
        return pl.ds(pl.multiple_of(i * width, width), width)

    def fill(i, _):
        sig_clean = clean[:, columns(i)].astype(F32)
        sig_corrupt = corrupt[:, columns(i)].astype(F32)
        pieces = (sig_clean, sig_corrupt, jnp.where(take, sig_clean, sig_corrupt))
        for run, sig in enumerate(pieces):
            for k in range(per):
                at = pl.multiple_of((run * TILES + i * per + k) * span, 8)
                pad[pl.ds(at, 8), :] = jnp.zeros((8, LANES), F32)
                pad[pl.ds(at + 8, ROWS), :] = sig[:, k * LANES : (k + 1) * LANES]
        return 0

    def convolve(rows):
        def body(tile, _):
            cols = pl.ds(pl.multiple_of(tile * LANES, LANES), LANES)
            bias = conv_b[:, cols]
            for run in range(3):
                at = (run * TILES + tile) * span + 8 - margin
                total = bias + conv_w[0:1, cols] * pad[pl.ds(at, rows), :]
                for k in range(1, TAPS):
                    total = total + conv_w[k : k + 1, cols] * pad[pl.ds(at + k, rows), :]
                acts[run * ROWS : run * ROWS + rows, cols] = silu(total).astype(BF16)
            return 0

        lax.fori_loop(0, TILES, body, 0, unroll=4)

    def fill_rim(i, _):
        rim = rims[:, columns(i)].astype(F32)
        rim_clean, rim_corrupt = rim[:margin], rim[margin : 2 * margin]
        pieces = (rim_clean, rim_corrupt, jnp.where(take_rim, rim_clean, rim_corrupt))
        for run, part in enumerate(pieces):
            for k in range(per):
                at = (run * TILES + i * per + k) * span + 8 - margin
                pad[pl.ds(at, margin), :] = part[:, k * LANES : (k + 1) * LANES]
        return 0

    lax.fori_loop(0, INNER // width, fill, 0)
    convolve(ROWS)
    for load in loads[6:]:
        load.wait()

    def rate_of(slot, cols):
        rates[rate_at(slot), :] = jnp.exp(a_log[:, cols]) * (-LOG2E)

    def patched_rate(tile, _):
        rate_of(tile, pl.ds(pl.multiple_of(tile * LANES, LANES), LANES))
        return 0

    lax.fori_loop(0, TILES, patched_rate, 0, unroll=4)
    for tile in range(CUT_TILES):
        for run in (CLEAN, CORRUPT):
            cols = pl.ds(pl.multiple_of(v * SPAN + tile * LANES, LANES), LANES)
            rate_of(cut_slot(run, tile), cols)
    for slot in range(60, CHUNKS):
        rates[rate_at(slot), :] = jnp.zeros((STATE, LANES), F32)

    @pl.when(has_last)
    def _():
        copy.wait_recv()
        lax.fori_loop(0, INNER // width, fill_rim, 0)
        convolve(8)

    @pl.when(has_next)
    def _():
        copy.wait_send()


def emit_kernel(patched, effect, patched_out, effect_out, sems):
    copies = [
        pltpu.make_async_copy(patched, patched_out, sems.at[0]),
        pltpu.make_async_copy(effect, effect_out, sems.at[1]),
    ]
    for copy in copies:
        copy.start()
    for copy in copies:
        copy.wait()


def kernel(
    pos, mode, acts, x_w, dt_w, dt_b, rates, clean_in, corrupt_in, d_skip_in,
    patched, effect,
    clean_gate, corrupt_gate, d_skip, low, maps, weights, base, gates, dts, us, bs, cs, ends, totals,
    pair_ends, pair_totals, chip_ends, got_ends,
    leaving, landed, across, start, ys,
    cut, squares, whole, peaks, squares_z, line_squares, squares_x, spreads,
    peaks_z, line_peaks, peaks_x, pair_squares, chip_squares, pair_peaks, chip_peaks, sent_peaks, answer,
    load_sem, send_pt, recv_pt, send_pe, recv_pe, send_ce, recv_ce,
    send_in, recv_in, send_st, recv_st,
    send_cut, recv_cut, send_sz, recv_sz, send_sx, recv_sx, send_sp, recv_sp,
    send_pz, recv_pz, send_px, recv_px, send_qq, recv_qq, send_pp, recv_pp, send_an, recv_an,
):
    me = lax.axis_index("seq")
    v = lax.axis_index("var")
    chip = lax.div(me, 2)
    core = lax.rem(me, 2)
    mate = me + 1 - 2 * core
    mine = core * HALF
    theirs = HALF - mine
    barrier = pltpu.get_barrier_semaphore()

    loads = [
        pltpu.make_async_copy(src, dst, load_sem.at[i])
        for i, (src, dst) in enumerate(
            (
                (d_skip_in, d_skip), (clean_in.at[:, INNER:], clean_gate),
                (corrupt_in.at[:, INNER:], corrupt_gate),
            )
        )
    ]
    for load in loads:
        load.start()

    def signal(peer, variant):
        pl.semaphore_signal(barrier, inc=1, device_id=(peer, variant), device_id_type=MESH)

    row_x, line_z = lax.div(chip, 8), lax.rem(chip, 8)
    peers = [8 * lax.rem(row_x + dx, 4) + lax.rem(line_z + dz, 8) for dx, dz in STEPS]
    for peer in peers:
        signal(2 * peer + core, v)
    signal(mate, v)
    for k in range(1, VARS):
        signal(me, lax.rem(v + k, VARS))

    def to_variant(k, src, dst, send_sem, recv_sem):
        return pltpu.make_async_remote_copy(
            src_ref=src, dst_ref=dst, send_sem=send_sem, recv_sem=recv_sem,
            device_id=(me, lax.rem(v + k, VARS)), device_id_type=MESH,
        )

    def to_shard(peer, src, dst, send_sem, recv_sem):
        return pltpu.make_async_remote_copy(
            src_ref=src, dst_ref=dst, send_sem=send_sem, recv_sem=recv_sem,
            device_id=(peer, v), device_id_type=MESH,
        )

    take_gate = hit_rows(pos, me * ROWS, ROWS)[:, :1] & (mode[0] != 0)

    projected = lax.dot_general(
        acts[...], x_w[...], (((1,), (1,)), ((), ())), preferred_element_type=F32
    )
    low[...] = projected[:, :RANK].astype(BF16)
    maps[...] = projected[:, RANK + STATE :]
    for run in range(3):
        part = projected[run * ROWS : (run + 1) * ROWS]
        for n in range(STATE):
            at = run * ROWS * SPLAT + n
            bs[pl.ds(at, ROWS, stride=SPLAT), :] = jnp.broadcast_to(
                part[:, RANK + n : RANK + n + 1], (ROWS, LANES)
            )


    def place(slot, steps, act):
        dts[pl.ds(slot, ROWS, stride=PITCH), :] = steps
        us[pl.ds(slot, ROWS, stride=PITCH), :] = steps * act
        totals[slot] = jnp.sum(steps, axis=0, keepdims=True)

    wide = 2560

    def patched_steps(i, _):
        cols = pl.ds(pl.multiple_of(i * wide, wide), wide)
        raw = jnp.dot(low[2 * ROWS :, :], dt_w[:, cols], preferred_element_type=F32)
        steps = softplus(raw + dt_b[:, cols])
        act = acts[2 * ROWS :, cols].astype(F32)
        for k in range(wide // LANES):
            part = slice(k * LANES, (k + 1) * LANES)
            place(i * (wide // LANES) + k, steps[:, part], act[:, part])
        return 0

    lax.fori_loop(0, INNER // wide, patched_steps, 0)

    cols = pl.ds(pl.multiple_of(v * SPAN, LANES), SPAN)
    raw = jnp.dot(low[: 2 * ROWS, :], dt_w[:, cols], preferred_element_type=F32)
    steps = softplus(raw + dt_b[:, cols])
    act = acts[: 2 * ROWS, cols].astype(F32)
    for run in (CLEAN, CORRUPT):
        rows = slice(run * ROWS, (run + 1) * ROWS)
        for tile in range(CUT_TILES):
            part = slice(tile * LANES, (tile + 1) * LANES)
            place(cut_slot(run, tile), steps[rows, part], act[rows, part])
    blank = jnp.zeros((ROWS, LANES), F32)
    for slot in range(60, CHUNKS):
        place(slot, blank, blank)

    zero = jnp.zeros((8, LANES), F32)

    def rates_of(group):
        base = group * (STATE * 8)
        return [rates[pl.ds(pl.multiple_of(base + n * 8, 8), 8), :] for n in range(STATE)]

    def run_base(group):
        return jnp.where(group < 5, PATCHED, group - 5) * (ROWS * SPLAT)

    def local_group(group, drive):
        found = scan_group(
            dts, us, rates_of(group), group, (zero,) * STATE, drive, None, None
        )
        for n in range(STATE):
            ends[pl.ds(group * (STATE * 8) + n, 8, stride=STATE), :] = found[n]

    def local_pass(offset):
        def body(i, _):
            group = offset + i

            @pl.when(group < GROUPS - 1)
            def _():
                local_group(group, splat_reader(bs, run_base(group)))

            @pl.when(group == GROUPS - 1)
            def _():
                local_group(group, mixed_reader(bs))

            return 0

        lax.fori_loop(0, GROUPS // 2, body, 0)

    local_pass(lax.div(theirs, 8))
    pl.semaphore_wait(barrier, CHIPS - 1 + 1 + VARS - 1)
    theirs_3 = pl.ds(theirs, HALF)
    swap_totals = to_shard(mate, totals.at[theirs_3], pair_totals, send_pt, recv_pt)
    swap_totals.start()

    theirs_2 = pl.ds(pl.multiple_of(theirs * STATE, 8), HALF * STATE)
    swap_ends = to_shard(mate, ends.at[theirs_2], pair_ends, send_pe, recv_pe)
    swap_ends.start()
    local_pass(lax.div(mine, 8))
    swap_totals.wait()

    leads = core == 0

    def my_summary(k):
        own = ends[pl.ds(pl.multiple_of((mine + k) * STATE, 8), STATE), :]
        return own, totals[mine + k]

    def pair_of(k):
        own_end, own_total = my_summary(k)
        other_end = pair_ends[pl.ds(pl.multiple_of(k * STATE, 8), STATE), :]
        other_total = pair_totals[k]
        return (
            jnp.where(leads, own_end, other_end), jnp.where(leads, own_total, other_total),
            jnp.where(leads, other_end, own_end), jnp.where(leads, other_total, own_total),
        )

    swap_ends.wait()

    def chip_end(k, _):
        end_a, total_a, end_b, total_b = pair_of(k)
        chip_ends[k, :STATE] = jnp.exp2(rates[rate_at(mine + k), :] * total_b) * end_a + end_b
        chip_ends[k, STATE:] = total_a + total_b
        return 0

    lax.fori_loop(0, HALF, chip_end, 0, unroll=4)
    owns = (core == 0) | (chip < BUSY)
    others = pl.ds(0, CHIPS - 1)

    @pl.when(owns)
    def _():
        pltpu.make_async_copy(chip_ends.at[chip], got_ends.at[chip], recv_ce).start()

    for peer in peers:
        @pl.when((core == 0) | (peer < BUSY))
        def _():
            target = 2 * peer + core
            to_shard(target, chip_ends.at[peer], got_ends.at[chip], send_ce, recv_ce).start()

    my_rate = rates[rate_at(mine + chip), :]
    for run in range(3):
        for n in range(STATE):
            cs[pl.ds(run * ROWS * SPLAT + n, ROWS, stride=SPLAT), :] = jnp.broadcast_to(
                maps[run * ROWS : (run + 1) * ROWS, n : n + 1], (ROWS, LANES)
            )

    def local_readout(group, drive, read):
        scan_group(dts, us, rates_of(group), group, (zero,) * STATE, drive, read, ys)

    def plain_readout(group, _):
        at = run_base(group)
        local_readout(group, splat_reader(bs, at), splat_reader(cs, at))
        return 0

    lax.fori_loop(0, GROUPS - 1, plain_readout, 0)
    local_readout(GROUPS - 1, mixed_reader(bs), mixed_reader(cs))
    def chain(s, state):
        leaving[s] = state
        return jnp.exp2(my_rate * got_ends[s, STATE:]) * state + got_ends[s, :STATE]

    @pl.when(owns)
    def _():
        wait_for(got_ends, recv_ce)
        lax.fori_loop(0, CHIPS, chain, jnp.zeros((STATE, LANES), F32), unroll=4)
        pltpu.make_async_copy(leaving.at[chip], landed.at[chip], recv_in).start()
        for peer in peers:
            to_shard(2 * peer + core, leaving.at[peer], landed.at[chip], send_in, recv_in).start()

    def entry_weights(group, read):
        rate = rates_of(group)

        def step(t, run_total):
            row = pl.multiple_of(t * PITCH + group * 8, 8)
            run_total = run_total + dts[pl.ds(row, 8), :]
            at = (group * ROWS + t) * (STATE * 8)
            for n in range(STATE):
                weights[pl.ds(pl.multiple_of(at + n * 8, 8), 8), :] = read(t, n) * jnp.exp2(
                    run_total * rate[n]
                )
            return run_total

        lax.fori_loop(0, ROWS, step, zero, unroll=4)

    def plain_weights(group, _):
        entry_weights(group, splat_reader(cs, run_base(group)))
        return 0

    lax.fori_loop(0, GROUPS - 1, plain_weights, 0)
    entry_weights(GROUPS - 1, mixed_reader(cs))
    for load in loads:
        load.wait()

    def prepare(slot, act, skip, gate):
        rows = pl.ds(pl.multiple_of(slot * ROWS, 8), ROWS)
        base[rows, :] = ys[pl.ds(slot, ROWS, stride=PITCH), :] + skip * act
        gates[rows, :] = silu(gate)

    for run, gate_rows in ((CLEAN, clean_gate), (CORRUPT, corrupt_gate)):
        for tile in range(CUT_TILES):
            cols = pl.ds(pl.multiple_of(v * SPAN + tile * LANES, LANES), LANES)
            act = acts[run * ROWS : (run + 1) * ROWS, cols].astype(F32)
            prepare(cut_slot(run, tile), act, d_skip[:, cols], gate_rows[:, cols].astype(F32))

    def prepare_patched(tile, _):
        cols = pl.ds(pl.multiple_of(tile * LANES, LANES), LANES)
        gate = jnp.where(
            take_gate, clean_gate[:, cols].astype(F32), corrupt_gate[:, cols].astype(F32)
        )
        prepare(tile, acts[2 * ROWS :, cols].astype(F32), d_skip[:, cols], gate)
        return 0

    lax.fori_loop(0, TILES, prepare_patched, 0, unroll=2)
    def enter(k, _):
        end_a, total_a, _, _ = pair_of(k)
        before = landed[k]
        after = jnp.exp2(rates[rate_at(mine + k), :] * total_a) * before + end_a
        at = pl.ds(pl.multiple_of((mine + k) * STATE, 8), STATE)
        start[at, :] = jnp.where(leads, before, after)
        across[pl.ds(pl.multiple_of(k * STATE, 8), STATE), :] = jnp.where(leads, after, before)
        return 0

    swap_start = to_shard(
        mate, across, start.at[pl.ds(pl.multiple_of(mine * STATE, 8), HALF * STATE)],
        send_st, recv_st,
    )

    def enter_half(sources):
        wait_for(landed.at[pl.ds(0, sources)], recv_in)
        lax.fori_loop(0, HALF, enter, 0, unroll=4)
        swap_start.start()

    @pl.when(core == 1)
    def _():
        enter_half(BUSY)

    @pl.when(core == 0)
    def _():
        swap_start.wait_recv()

    def final_group(group, _):
        at = group * (STATE * 8)
        state = [start[pl.ds(at + n, 8, stride=STATE), :] for n in range(STATE)]

        def step(t, _):
            at = (group * ROWS + t) * (STATE * 8)
            total = None
            for n in range(STATE):
                term = weights[pl.ds(pl.multiple_of(at + n * 8, 8), 8), :] * state[n]
                total = term if total is None else total + term
            ys[pl.ds(pl.multiple_of(t * PITCH + group * 8, 8), 8), :] = total
            return 0

        lax.fori_loop(0, ROWS, step, 0, unroll=8)
        return 0

    def result(slot):
        rows = pl.ds(pl.multiple_of(slot * ROWS, 8), ROWS)
        y = ys[pl.ds(slot, ROWS, stride=PITCH), :]
        return ((y + base[rows, :]) * gates[rows, :]).astype(BF16)

    lax.fori_loop(6, GROUPS, final_group, 0)

    for tile in range(CUT_TILES):
        cut[:, tile * LANES : (tile + 1) * LANES] = result(cut_slot(CORRUPT, tile))
    directs = [
        to_variant(k, cut, whole.at[v], send_cut.at[k], recv_cut.at[k]) for k in (2, 1, VARS - 1)
    ]
    for direct in directs:
        direct.start()
    @pl.when(core == 0)
    def _():
        enter_half(CHIPS)

    @pl.when(core == 1)
    def _():
        swap_start.wait_recv()

    final_group(5, 0)
    squares[...] = jnp.zeros_like(squares)
    for tile in range(CUT_TILES):
        gap = result(cut_slot(CLEAN, tile)).astype(F32)
        gap = gap - cut[:, tile * LANES : (tile + 1) * LANES].astype(F32)
        squares[tile : tile + 1, :] = jnp.sum(gap * gap, axis=0, keepdims=True)

    def along_z(k):
        return 16 * row_x + 2 * lax.rem(line_z + k, 8) + 1

    def along_x(k):
        return 16 * lax.rem(row_x + k, 4) + 2 * line_z + 1

    def share(peer_of, count, slot, src, dst, send_sem, recv_sem):
        for k in range(1, count):
            to_shard(peer_of(k), src, dst.at[slot], send_sem, recv_sem).start()
        dst[slot] = src[...]

    seven, three = pl.ds(0, 7), pl.ds(0, 3)
    squares_over = to_shard(mate, squares, pair_squares, send_qq, recv_qq)

    @pl.when(core == 0)
    def _():
        squares_over.start()

    whole[v] = cut[...]

    lax.fori_loop(0, 5, final_group, 0)
    def patched_tile(tile, _):
        cols = pl.ds(pl.multiple_of(tile * LANES, LANES), LANES)
        patched[:, cols] = result(tile)
        return 0

    lax.fori_loop(0, TILES, patched_tile, 0, unroll=4)


    @pl.when(core == 1)
    def _():
        squares_over.wait_recv()
        chip_squares[...] = squares[...] + pair_squares[...]
        share(along_z, 8, line_z, chip_squares, squares_z, send_sz, recv_sz)

    for direct in directs:
        direct.wait()

    for w in range(VARS):
        def peak_tile(i, _):
            here = pl.ds(pl.multiple_of(i * LANES, LANES), LANES)
            there = pl.ds(pl.multiple_of(w * SPAN + i * LANES, LANES), LANES)
            gap = jnp.abs(patched[:, there].astype(F32) - whole[w, :, here].astype(F32))
            peaks[pl.ds(w * CUT_TILES + i, 1), :] = jnp.max(gap, axis=0, keepdims=True)
            return 0

        lax.fori_loop(0, CUT_TILES, peak_tile, 0, unroll=2)

    sent_peaks[...] = peaks[...].astype(BF16)
    peaks_over = to_shard(mate, sent_peaks, pair_peaks, send_pp, recv_pp)
    answer_over = to_shard(mate, answer, answer, send_an, recv_an)

    @pl.when(core == 0)
    def _():
        peaks_over.start()

    @pl.when(core == 1)
    def _():
        wait_for(squares_z.at[seven], recv_sz)
        line_squares[...] = jnp.sum(squares_z[...], axis=0)
        share(along_x, 4, row_x, line_squares, squares_x, send_sx, recv_sx)
        peaks_over.wait_recv()
        both = jnp.maximum(sent_peaks[...].astype(F32), pair_peaks[...].astype(F32))
        chip_peaks[...] = both.astype(BF16)
        share(along_z, 8, line_z, chip_peaks, peaks_z, send_pz, recv_pz)
        wait_for(squares_x.at[three], recv_sx)
        spreads[v] = jnp.sqrt(jnp.sum(squares_x[...], axis=0) / (SHARDS * ROWS) + TINY)
        for k in range(1, VARS):
            to_variant(k, spreads.at[v], spreads.at[v], send_sp.at[k], recv_sp.at[k]).start()
        wait_for(peaks_z.at[seven], recv_pz)
        line_peaks[...] = jnp.max(peaks_z[...].astype(F32), axis=0).astype(BF16)
        share(along_x, 4, row_x, line_peaks, peaks_x, send_px, recv_px)
        wait_for(peaks_x.at[three], recv_px)
        for k in range(1, VARS):
            there = spreads.at[lax.rem(v + VARS - k, VARS)]
            to_variant(k, there, there, send_sp.at[k], recv_sp.at[k]).wait()
        peak = jnp.max(peaks_x[...].astype(F32), axis=0)
        for w in range(VARS):
            rows = slice(w * CUT_TILES, (w + 1) * CUT_TILES)
            answer[rows, :] = peak[rows, :] / spreads[w, :CUT_TILES, :]
        answer_over.start()
        wait_for(squares_z.at[seven], send_sz)
        wait_for(squares_x.at[three], send_sx)
        wait_for(peaks_z.at[seven], send_pz)
        wait_for(peaks_x.at[three], send_px)
        answer_over.wait_send()

    @pl.when(core == 0)
    def _():
        squares_over.wait_send()
        peaks_over.wait_send()
        answer_over.wait_recv()

    effect[...] = answer[...]
    @pl.when(core == 0)
    def _():
        wait_for(chip_ends.at[others], send_ce)

    @pl.when((core == 1) & (chip < BUSY))
    def _():
        wait_for(chip_ends.at[pl.ds(0, BUSY - 1)], send_ce)

    @pl.when((core == 1) & (chip >= BUSY))
    def _():
        wait_for(chip_ends.at[pl.ds(0, BUSY)], send_ce)

    @pl.when(owns)
    def _():
        wait_for(leaving.at[others], send_in)

    swap_start.wait_send()


SMEM = pl.BlockSpec(memory_space=pltpu.SMEM)
HBM = pl.BlockSpec(memory_space=pltpu.HBM)
VMEM = pl.BlockSpec(memory_space=pltpu.VMEM)
DMA = pltpu.SemaphoreType.DMA


def shards(
    clean_proj, corrupt_proj, patch_pos, patch_mode, a_log, dt_bias,
    conv_weight, conv_bias, x_weight, dt_weight, d_skip,
):
    hold = functools.partial(pltpu.with_memory_space_constraint, memory_space=pltpu.HBM)
    keep = functools.partial(pltpu.with_memory_space_constraint, memory_space=pltpu.VMEM)
    front = pl.pallas_call(
        front_kernel,
        out_shape=(
            pltpu.VMEM((3 * ROWS, INNER), BF16),
            pltpu.VMEM((RANK + 2 * STATE, INNER), BF16),
            pltpu.VMEM((RANK, INNER), BF16),
            pltpu.VMEM((1, INNER), F32),
            pltpu.VMEM((CHUNKS * STATE, LANES), F32),
        ),
        in_specs=[SMEM, SMEM] + [HBM] * 8,
        out_specs=(VMEM,) * 5,
        scratch_shapes=[
            pltpu.VMEM((8, INNER), BF16),
            pltpu.VMEM((STATE, INNER), F32),
            pltpu.VMEM((2, 8, INNER), BF16),
            pltpu.VMEM((8, INNER), F32),
            pltpu.VMEM((8, INNER), BF16),
            pltpu.VMEM((ROWS, INNER), BF16),
            pltpu.VMEM((ROWS, INNER), BF16),
            pltpu.VMEM((TAPS, INNER), F32),
            pltpu.VMEM((1, INNER), F32),
            pltpu.VMEM((3 * TILES * (8 + ROWS), LANES), F32),
            DMA((10,)),
            DMA,
            DMA,
        ],
        compiler_params=pltpu.CompilerParams(
            collective_id=1, has_side_effects=True, vmem_limit_bytes=40_000_000
        ),
        name="front",
    )(
        hold(patch_pos), patch_mode,
        *map(
            hold,
            (
                clean_proj, corrupt_proj, conv_weight, conv_bias[None], x_weight.T, dt_weight,
                dt_bias[None], a_log,
            ),
        ),
    )
    row = (1, LANES)
    tile = (STATE, LANES)
    patched, effect = pl.pallas_call(
        kernel,
        out_shape=(pltpu.VMEM((ROWS, INNER), BF16), pltpu.VMEM((TILES, LANES), F32)),
        in_specs=[SMEM, SMEM] + [VMEM] * 5 + [HBM] * 3,
        out_specs=(VMEM, VMEM),
        scratch_shapes=[
            pltpu.VMEM((ROWS, INNER), BF16),
            pltpu.VMEM((ROWS, INNER), BF16),
            pltpu.VMEM((1, INNER), F32),
            pltpu.VMEM((3 * ROWS, RANK), BF16),
            pltpu.VMEM((3 * ROWS, STATE), F32),
            pltpu.VMEM((GROUPS * ROWS * STATE * 8, LANES), F32),
            pltpu.VMEM((CHUNKS * ROWS, LANES), F32),
            pltpu.VMEM((CHUNKS * ROWS, LANES), F32),
            pltpu.VMEM((ROWS * PITCH, LANES), F32),
            pltpu.VMEM((ROWS * PITCH, LANES), F32),
            pltpu.VMEM((3 * ROWS * SPLAT + 8, LANES), F32),
            pltpu.VMEM((3 * ROWS * SPLAT + 8, LANES), F32),
            pltpu.VMEM((CHUNKS * STATE, LANES), F32),
            pltpu.VMEM((CHUNKS, *row), F32),
            pltpu.VMEM((HALF * STATE, LANES), F32),
            pltpu.VMEM((HALF, *row), F32),
            pltpu.VMEM((HALF, STATE + 1, LANES), F32),
            pltpu.VMEM((CHIPS, STATE + 1, LANES), F32),
            pltpu.VMEM((CHIPS, *tile), F32),
            pltpu.VMEM((HALF, *tile), F32),
            pltpu.VMEM((HALF * STATE, LANES), F32),
            pltpu.VMEM((CHUNKS * STATE, LANES), F32),
            pltpu.VMEM((ROWS * PITCH, LANES), F32),
            pltpu.VMEM((ROWS, SPAN), BF16),
            pltpu.VMEM((STATE, LANES), F32),
            pltpu.VMEM((VARS, ROWS, SPAN), BF16),
            pltpu.VMEM((TILES, LANES), F32),
            pltpu.VMEM((8, STATE, LANES), F32),
            pltpu.VMEM((STATE, LANES), F32),
            pltpu.VMEM((4, STATE, LANES), F32),
            pltpu.VMEM((VARS, STATE, LANES), F32),
            pltpu.VMEM((8, TILES, LANES), BF16),
            pltpu.VMEM((TILES, LANES), BF16),
            pltpu.VMEM((4, TILES, LANES), BF16),
            pltpu.VMEM((STATE, LANES), F32),
            pltpu.VMEM((STATE, LANES), F32),
            pltpu.VMEM((TILES, LANES), BF16),
            pltpu.VMEM((TILES, LANES), BF16),
            pltpu.VMEM((TILES, LANES), BF16),
            pltpu.VMEM((TILES, LANES), F32),
            DMA((3,)),
        ]
        + [DMA] * 10
        + [DMA((VARS,)), DMA((VARS,))]
        + [DMA] * 4
        + [DMA((VARS,)), DMA((VARS,))]
        + [DMA] * 10,
        compiler_params=pltpu.CompilerParams(
            collective_id=0, has_side_effects=True, vmem_limit_bytes=54_000_000
        ),
        name="mixer",
    )(
        hold(patch_pos), patch_mode, *map(keep, front),
        *map(hold, (clean_proj, corrupt_proj, d_skip[None])),
    )
    patched, effect = pl.pallas_call(
        emit_kernel,
        out_shape=(
            jax.ShapeDtypeStruct((ROWS, INNER), BF16),
            jax.ShapeDtypeStruct((TILES, LANES), F32),
        ),
        in_specs=[VMEM, VMEM],
        out_specs=(HBM, HBM),
        scratch_shapes=[DMA((2,))],
        compiler_params=pltpu.CompilerParams(vmem_limit_bytes=16_000_000),
        name="emit",
    )(
        keep(patched), keep(effect),
    )
    return (patched[None], effect.reshape(1, INNER))


def solution(mesh):
    return jax.shard_map(
        shards,
        mesh=mesh,
        in_specs=(
            P("seq", None), P("seq", None), P("var", None), P("var"),
            P(), P(), P(), P(), P(), P(), P(),
        ),
        out_specs=(P("var", "seq", None), P("var", None)),
        check_vma=False,
    )
```

```python
import functools

import jax
import jax.numpy as jnp
from jax import lax
from jax.experimental import pallas as pl
from jax.experimental.pallas import tpu as pltpu
from jax.sharding import PartitionSpec as P

STATE = 16
RANK = 160
ROWS = 32
INNER = 5120
SPAN = 1280
TAPS = 4
LANES = 128
CHUNKS = 64
SHARDS = 64
VARS = 4
TILES = INNER // LANES
CUT_TILES = SPAN // LANES
GROUPS = CHUNKS // 8
BUSY = 28
HALF = CHUNKS // 2
CHIPS = SHARDS // 2
PITCH = 72
SPLAT = 17
MESH = pl.DeviceIdType.MESH
LOG2E = 1.4426950408889634
TINY = 1e-06
F32 = jnp.float32
BF16 = jnp.bfloat16
UNROLL = 8
CLEAN, CORRUPT, PATCHED = 0, 1, 2
STEPS = sorted(
    ((dx, dz) for dx in range(4) for dz in range(8) if dx or dz),
    key=lambda step: -(min(step[0], 4 - step[0]) + min(step[1], 8 - step[1])),
)


def cut_slot(run, tile):
    if tile < 8:
        return TILES + 8 * run + tile
    return 56 + 2 * run + (tile - 8)


def rate_at(slot):
    return pl.ds(lax.div(slot, 8) * (STATE * 8) + lax.rem(slot, 8), STATE, stride=8)


def hit_rows(pos_ref, first, count):
    rows = first + lax.broadcasted_iota(jnp.int32, (count, LANES), 0)
    hits = rows == pos_ref[0, 0]
    for k in range(1, pos_ref.shape[1]):
        hits = hits | (rows == pos_ref[0, k])
    return hits


def silu(value):
    return value / (1.0 + jnp.exp(-value))


def softplus(value):
    return jnp.maximum(value, 0.0) + jnp.log1p(jnp.exp(-jnp.abs(value)))


def row_of(ref, row):
    return jnp.broadcast_to(ref[pl.ds(row, 1), :], (8, LANES))


def scan_group(dts, us, rate, group, state, drive, readout, out):
    def step(t, carry):
        row = pl.multiple_of(t * PITCH + group * 8, 8)
        steps = dts[pl.ds(row, 8), :]
        flow = us[pl.ds(row, 8), :]
        entries = []
        total = None
        for n in range(STATE):
            decay = jnp.exp2(steps * rate[n])
            entry = decay * carry[n] + flow * drive(t, n)
            entries.append(entry)
            if readout is not None:
                term = readout(t, n) * entry
                total = term if total is None else total + term
        if readout is not None:
            out[pl.ds(row, 8), :] = total
        return tuple(entries)

    return lax.fori_loop(0, ROWS, step, state, unroll=UNROLL)


def splat_reader(ref, base):
    return lambda t, n: row_of(ref, base + t * SPLAT + n)


def mixed_reader(ref):
    first = lax.broadcasted_iota(jnp.int32, (8, LANES), 0) < 2

    def read(t, n):
        return jnp.where(
            first,
            row_of(ref, CLEAN * ROWS * SPLAT + t * SPLAT + n),
            row_of(ref, CORRUPT * ROWS * SPLAT + t * SPLAT + n),
        )

    return read


def wait_for(ref, sem):
    pltpu.make_async_copy(ref, ref, sem).wait()


def front_kernel(
    pos, mode, clean_in, corrupt_in, conv_w_in, conv_b_in, x_w_in, dt_w_in, dt_b_in, a_log_in,
    acts, x_w, dt_w, dt_b, rates,
    rims, a_log, ends, wide, packed, clean, corrupt, conv_w, conv_b, pad, load_sem, send_sem, recv_sem,
):
    me = lax.axis_index("seq")
    v = lax.axis_index("var")
    after = lax.min(me + 1, SHARDS - 1)
    has_next, has_last = me < SHARDS - 1, me > 0
    barrier = pltpu.get_barrier_semaphore()
    loads = [
        pltpu.make_async_copy(src, dst, load_sem.at[i])
        for i, (src, dst) in enumerate(
            (
                (clean_in.at[ROWS - 8 :, :INNER], ends.at[0]),
                (corrupt_in.at[ROWS - 8 :, :INNER], ends.at[1]),
                (clean_in.at[:, :INNER], clean), (corrupt_in.at[:, :INNER], corrupt),
                (conv_w_in, conv_w), (conv_b_in, conv_b), (x_w_in, x_w), (dt_w_in, dt_w),
                (dt_b_in, dt_b), (a_log_in, a_log),
            )
        )
    ]
    for load in loads:
        load.start()

    def signal(peer):
        pl.semaphore_signal(barrier, inc=1, device_id=(peer, v), device_id_type=MESH)

    @pl.when(has_next)
    def _():
        signal(me + 1)

    @pl.when(has_last)
    def _():
        signal(me - 1)

    for load in loads[:2]:
        load.wait()
    margin = TAPS - 1
    wide[...] = jnp.zeros_like(wide)
    for i in range(2):
        wide[i * margin : (i + 1) * margin, :] = ends[i].astype(F32)[8 - margin :, :]
    packed[...] = wide[...].astype(BF16)
    first = me * ROWS
    take = hit_rows(pos, first, ROWS)[:, :1] & (mode[0] != 1)
    take_rim = hit_rows(pos, first - margin, margin)[:, :1] & (mode[0] != 1)
    pl.semaphore_wait(barrier, lax.min(me, 1) + lax.min(SHARDS - 1 - me, 1))
    copy = pltpu.make_async_remote_copy(
        src_ref=packed, dst_ref=rims, send_sem=send_sem, recv_sem=recv_sem,
        device_id=(after, v), device_id_type=MESH,
    )

    @pl.when(has_next)
    def _():
        copy.start()

    for load in loads[2:6]:
        load.wait()
    width = 512
    span = 8 + ROWS
    per = width // LANES

    def columns(i):
        return pl.ds(pl.multiple_of(i * width, width), width)

    def fill(i, _):
        sig_clean = clean[:, columns(i)].astype(F32)
        sig_corrupt = corrupt[:, columns(i)].astype(F32)
        pieces = (sig_clean, sig_corrupt, jnp.where(take, sig_clean, sig_corrupt))
        for run, sig in enumerate(pieces):
            for k in range(per):
                at = pl.multiple_of((run * TILES + i * per + k) * span, 8)
                pad[pl.ds(at, 8), :] = jnp.zeros((8, LANES), F32)
                pad[pl.ds(at + 8, ROWS), :] = sig[:, k * LANES : (k + 1) * LANES]
        return 0

    def convolve(rows):
        def body(tile, _):
            cols = pl.ds(pl.multiple_of(tile * LANES, LANES), LANES)
            bias = conv_b[:, cols]
            for run in range(3):
                at = (run * TILES + tile) * span + 8 - margin
                total = bias + conv_w[0:1, cols] * pad[pl.ds(at, rows), :]
                for k in range(1, TAPS):
                    total = total + conv_w[k : k + 1, cols] * pad[pl.ds(at + k, rows), :]
                acts[run * ROWS : run * ROWS + rows, cols] = silu(total).astype(BF16)
            return 0

        lax.fori_loop(0, TILES, body, 0, unroll=4 if rows == ROWS else 10)

    def fill_rim(i, _):
        rim = rims[:, columns(i)].astype(F32)
        rim_clean, rim_corrupt = rim[:margin], rim[margin : 2 * margin]
        pieces = (rim_clean, rim_corrupt, jnp.where(take_rim, rim_clean, rim_corrupt))
        for run, part in enumerate(pieces):
            for k in range(per):
                at = (run * TILES + i * per + k) * span + 8 - margin
                pad[pl.ds(at, margin), :] = part[:, k * LANES : (k + 1) * LANES]
        return 0

    lax.fori_loop(0, INNER // width, fill, 0)
    convolve(ROWS)
    for load in loads[6:]:
        load.wait()

    def rate_of(slot, cols):
        rates[rate_at(slot), :] = jnp.exp(a_log[:, cols]) * (-LOG2E)

    def patched_rate(tile, _):
        rate_of(tile, pl.ds(pl.multiple_of(tile * LANES, LANES), LANES))
        return 0

    lax.fori_loop(0, TILES, patched_rate, 0, unroll=4)
    for tile in range(CUT_TILES):
        for run in (CLEAN, CORRUPT):
            cols = pl.ds(pl.multiple_of(v * SPAN + tile * LANES, LANES), LANES)
            rate_of(cut_slot(run, tile), cols)
    for slot in range(60, CHUNKS):
        rates[rate_at(slot), :] = jnp.zeros((STATE, LANES), F32)

    @pl.when(has_last)
    def _():
        copy.wait_recv()
        lax.fori_loop(0, INNER // width, fill_rim, 0, unroll=5)
        convolve(8)

    @pl.when(has_next)
    def _():
        copy.wait_send()


def emit_kernel(patched, effect, patched_out, effect_out, sems):
    copies = [
        pltpu.make_async_copy(patched, patched_out, sems.at[0]),
        pltpu.make_async_copy(effect, effect_out, sems.at[1]),
    ]
    for copy in copies:
        copy.start()
    for copy in copies:
        copy.wait()


def kernel(
    pos, mode, acts, x_w, dt_w, dt_b, rates, clean_in, corrupt_in, d_skip_in,
    patched, effect,
    clean_gate, corrupt_gate, d_skip, low, maps, weights, base, gates, dts, us, bs, cs, ends, totals,
    pair_ends, pair_totals, chip_ends, got_ends,
    leaving, landed, across, start, ys,
    cut, squares, whole, peaks, squares_z, line_squares, squares_x, spreads,
    peaks_z, line_peaks, peaks_x, pair_squares, chip_squares, pair_peaks, chip_peaks, sent_peaks, answer,
    load_sem, send_pt, recv_pt, send_pe, recv_pe, send_ce, recv_ce,
    send_in, recv_in, send_st, recv_st,
    send_cut, recv_cut, send_sz, recv_sz, send_sx, recv_sx, send_sp, recv_sp,
    send_pz, recv_pz, send_px, recv_px, send_qq, recv_qq, send_pp, recv_pp, send_an, recv_an,
):
    me = lax.axis_index("seq")
    v = lax.axis_index("var")
    chip = lax.div(me, 2)
    core = lax.rem(me, 2)
    mate = me + 1 - 2 * core
    mine = core * HALF
    theirs = HALF - mine
    barrier = pltpu.get_barrier_semaphore()

    loads = [
        pltpu.make_async_copy(src, dst, load_sem.at[i])
        for i, (src, dst) in enumerate(
            (
                (d_skip_in, d_skip), (clean_in.at[:, INNER:], clean_gate),
                (corrupt_in.at[:, INNER:], corrupt_gate),
            )
        )
    ]
    for load in loads:
        load.start()

    def signal(peer, variant):
        pl.semaphore_signal(barrier, inc=1, device_id=(peer, variant), device_id_type=MESH)

    row_x, line_z = lax.div(chip, 8), lax.rem(chip, 8)
    peers = [8 * lax.rem(row_x + dx, 4) + lax.rem(line_z + dz, 8) for dx, dz in STEPS]
    for peer in peers:
        signal(2 * peer + core, v)
    signal(mate, v)
    for k in range(1, VARS):
        signal(me, lax.rem(v + k, VARS))

    def to_variant(k, src, dst, send_sem, recv_sem):
        return pltpu.make_async_remote_copy(
            src_ref=src, dst_ref=dst, send_sem=send_sem, recv_sem=recv_sem,
            device_id=(me, lax.rem(v + k, VARS)), device_id_type=MESH,
        )

    def to_shard(peer, src, dst, send_sem, recv_sem):
        return pltpu.make_async_remote_copy(
            src_ref=src, dst_ref=dst, send_sem=send_sem, recv_sem=recv_sem,
            device_id=(peer, v), device_id_type=MESH,
        )

    take_gate = hit_rows(pos, me * ROWS, ROWS)[:, :1] & (mode[0] != 0)

    projected = lax.dot_general(
        acts[...], x_w[...], (((1,), (1,)), ((), ())), preferred_element_type=F32
    )
    low[...] = projected[:, :RANK].astype(BF16)
    maps[...] = projected[:, RANK + STATE :]
    for run in range(3):
        part = projected[run * ROWS : (run + 1) * ROWS]
        for n in range(STATE):
            at = run * ROWS * SPLAT + n
            bs[pl.ds(at, ROWS, stride=SPLAT), :] = jnp.broadcast_to(
                part[:, RANK + n : RANK + n + 1], (ROWS, LANES)
            )


    def place(slot, steps, act):
        dts[pl.ds(slot, ROWS, stride=PITCH), :] = steps
        us[pl.ds(slot, ROWS, stride=PITCH), :] = steps * act
        totals[slot] = jnp.sum(steps, axis=0, keepdims=True)

    wide = 5120

    def patched_steps(i, _):
        cols = pl.ds(pl.multiple_of(i * wide, wide), wide)
        raw = jnp.dot(low[2 * ROWS :, :], dt_w[:, cols], preferred_element_type=F32)
        steps = softplus(raw + dt_b[:, cols])
        act = acts[2 * ROWS :, cols].astype(F32)
        for k in range(wide // LANES):
            part = slice(k * LANES, (k + 1) * LANES)
            place(i * (wide // LANES) + k, steps[:, part], act[:, part])
        return 0

    lax.fori_loop(0, INNER // wide, patched_steps, 0)

    cols = pl.ds(pl.multiple_of(v * SPAN, LANES), SPAN)
    raw = jnp.dot(low[: 2 * ROWS, :], dt_w[:, cols], preferred_element_type=F32)
    steps = softplus(raw + dt_b[:, cols])
    act = acts[: 2 * ROWS, cols].astype(F32)
    for run in (CLEAN, CORRUPT):
        rows = slice(run * ROWS, (run + 1) * ROWS)
        for tile in range(CUT_TILES):
            part = slice(tile * LANES, (tile + 1) * LANES)
            place(cut_slot(run, tile), steps[rows, part], act[rows, part])
    blank = jnp.zeros((ROWS, LANES), F32)
    for slot in range(60, CHUNKS):
        place(slot, blank, blank)

    zero = jnp.zeros((8, LANES), F32)

    def rates_of(group):
        base = group * (STATE * 8)
        return [rates[pl.ds(pl.multiple_of(base + n * 8, 8), 8), :] for n in range(STATE)]

    def run_base(group):
        return jnp.where(group < 5, PATCHED, group - 5) * (ROWS * SPLAT)

    def local_group(group, drive):
        found = scan_group(
            dts, us, rates_of(group), group, (zero,) * STATE, drive, None, None
        )
        for n in range(STATE):
            ends[pl.ds(group * (STATE * 8) + n, 8, stride=STATE), :] = found[n]

    def local_pass(offset):
        def body(i, _):
            group = offset + i

            @pl.when(group < GROUPS - 1)
            def _():
                local_group(group, splat_reader(bs, run_base(group)))

            @pl.when(group == GROUPS - 1)
            def _():
                local_group(group, mixed_reader(bs))

            return 0

        lax.fori_loop(0, GROUPS // 2, body, 0)

    local_pass(lax.div(theirs, 8))
    pl.semaphore_wait(barrier, CHIPS - 1 + 1 + VARS - 1)
    theirs_3 = pl.ds(theirs, HALF)
    swap_totals = to_shard(mate, totals.at[theirs_3], pair_totals, send_pt, recv_pt)
    swap_totals.start()

    theirs_2 = pl.ds(pl.multiple_of(theirs * STATE, 8), HALF * STATE)
    swap_ends = to_shard(mate, ends.at[theirs_2], pair_ends, send_pe, recv_pe)
    swap_ends.start()
    local_pass(lax.div(mine, 8))
    swap_totals.wait()

    leads = core == 0

    def my_summary(k):
        own = ends[pl.ds(pl.multiple_of((mine + k) * STATE, 8), STATE), :]
        return own, totals[mine + k]

    def pair_of(k):
        own_end, own_total = my_summary(k)
        other_end = pair_ends[pl.ds(pl.multiple_of(k * STATE, 8), STATE), :]
        other_total = pair_totals[k]
        return (
            jnp.where(leads, own_end, other_end), jnp.where(leads, own_total, other_total),
            jnp.where(leads, other_end, own_end), jnp.where(leads, other_total, own_total),
        )

    swap_ends.wait()

    def chip_end(k, _):
        end_a, total_a, end_b, total_b = pair_of(k)
        chip_ends[k, :STATE] = jnp.exp2(rates[rate_at(mine + k), :] * total_b) * end_a + end_b
        chip_ends[k, STATE:] = total_a + total_b
        return 0

    lax.fori_loop(0, HALF, chip_end, 0, unroll=8)
    owns = (core == 0) | (chip < BUSY)
    others = pl.ds(0, CHIPS - 1)

    @pl.when(owns)
    def _():
        pltpu.make_async_copy(chip_ends.at[chip], got_ends.at[chip], recv_ce).start()

    for peer in peers:
        @pl.when((core == 0) | (peer < BUSY))
        def _():
            target = 2 * peer + core
            to_shard(target, chip_ends.at[peer], got_ends.at[chip], send_ce, recv_ce).start()

    my_rate = rates[rate_at(mine + chip), :]
    for run in range(3):
        for n in range(STATE):
            cs[pl.ds(run * ROWS * SPLAT + n, ROWS, stride=SPLAT), :] = jnp.broadcast_to(
                maps[run * ROWS : (run + 1) * ROWS, n : n + 1], (ROWS, LANES)
            )

    def local_readout(group, drive, read):
        scan_group(dts, us, rates_of(group), group, (zero,) * STATE, drive, read, ys)

    def plain_readout(group, _):
        at = run_base(group)
        local_readout(group, splat_reader(bs, at), splat_reader(cs, at))
        return 0

    lax.fori_loop(0, GROUPS - 1, plain_readout, 0)
    local_readout(GROUPS - 1, mixed_reader(bs), mixed_reader(cs))
    def chain(s, state):
        leaving[s] = state
        return jnp.exp2(my_rate * got_ends[s, STATE:]) * state + got_ends[s, :STATE]

    @pl.when(owns)
    def _():
        wait_for(got_ends, recv_ce)
        lax.fori_loop(0, CHIPS, chain, jnp.zeros((STATE, LANES), F32), unroll=4)
        pltpu.make_async_copy(leaving.at[chip], landed.at[chip], recv_in).start()
        for peer in peers:
            to_shard(2 * peer + core, leaving.at[peer], landed.at[chip], send_in, recv_in).start()

    def entry_weights(group, read):
        rate = rates_of(group)

        def step(t, run_total):
            row = pl.multiple_of(t * PITCH + group * 8, 8)
            run_total = run_total + dts[pl.ds(row, 8), :]
            at = (group * ROWS + t) * (STATE * 8)
            for n in range(STATE):
                weights[pl.ds(pl.multiple_of(at + n * 8, 8), 8), :] = read(t, n) * jnp.exp2(
                    run_total * rate[n]
                )
            return run_total

        lax.fori_loop(0, ROWS, step, zero, unroll=4)

    def plain_weights(group, _):
        entry_weights(group, splat_reader(cs, run_base(group)))
        return 0

    lax.fori_loop(0, GROUPS - 1, plain_weights, 0)
    entry_weights(GROUPS - 1, mixed_reader(cs))
    for load in loads:
        load.wait()

    def prepare(slot, act, skip, gate):
        rows = pl.ds(pl.multiple_of(slot * ROWS, 8), ROWS)
        base[rows, :] = ys[pl.ds(slot, ROWS, stride=PITCH), :] + skip * act
        gates[rows, :] = silu(gate)

    for run, gate_rows in ((CLEAN, clean_gate), (CORRUPT, corrupt_gate)):
        for tile in range(CUT_TILES):
            cols = pl.ds(pl.multiple_of(v * SPAN + tile * LANES, LANES), LANES)
            act = acts[run * ROWS : (run + 1) * ROWS, cols].astype(F32)
            prepare(cut_slot(run, tile), act, d_skip[:, cols], gate_rows[:, cols].astype(F32))

    def prepare_patched(tile, _):
        cols = pl.ds(pl.multiple_of(tile * LANES, LANES), LANES)
        gate = jnp.where(
            take_gate, clean_gate[:, cols].astype(F32), corrupt_gate[:, cols].astype(F32)
        )
        prepare(tile, acts[2 * ROWS :, cols].astype(F32), d_skip[:, cols], gate)
        return 0

    lax.fori_loop(0, TILES, prepare_patched, 0, unroll=2)
    def enter(k, _):
        end_a, total_a, _, _ = pair_of(k)
        before = landed[k]
        after = jnp.exp2(rates[rate_at(mine + k), :] * total_a) * before + end_a
        at = pl.ds(pl.multiple_of((mine + k) * STATE, 8), STATE)
        start[at, :] = jnp.where(leads, before, after)
        across[pl.ds(pl.multiple_of(k * STATE, 8), STATE), :] = jnp.where(leads, after, before)
        return 0

    swap_start = to_shard(
        mate, across, start.at[pl.ds(pl.multiple_of(mine * STATE, 8), HALF * STATE)],
        send_st, recv_st,
    )

    def enter_half(sources):
        wait_for(landed.at[pl.ds(0, sources)], recv_in)
        lax.fori_loop(0, HALF, enter, 0, unroll=8)
        swap_start.start()

    @pl.when(core == 1)
    def _():
        enter_half(BUSY)

    @pl.when(core == 0)
    def _():
        swap_start.wait_recv()

    def final_group(group, _):
        at = group * (STATE * 8)
        state = [start[pl.ds(at + n, 8, stride=STATE), :] for n in range(STATE)]

        def step(t, _):
            at = (group * ROWS + t) * (STATE * 8)
            total = None
            for n in range(STATE):
                term = weights[pl.ds(pl.multiple_of(at + n * 8, 8), 8), :] * state[n]
                total = term if total is None else total + term
            ys[pl.ds(pl.multiple_of(t * PITCH + group * 8, 8), 8), :] = total
            return 0

        lax.fori_loop(0, ROWS, step, 0, unroll=8)
        return 0

    def result(slot):
        rows = pl.ds(pl.multiple_of(slot * ROWS, 8), ROWS)
        y = ys[pl.ds(slot, ROWS, stride=PITCH), :]
        return ((y + base[rows, :]) * gates[rows, :]).astype(BF16)

    lax.fori_loop(6, GROUPS, final_group, 0)

    for tile in range(CUT_TILES):
        cut[:, tile * LANES : (tile + 1) * LANES] = result(cut_slot(CORRUPT, tile))
    directs = [
        to_variant(k, cut, whole.at[v], send_cut.at[k], recv_cut.at[k]) for k in (2, 1, VARS - 1)
    ]
    for direct in directs:
        direct.start()
    @pl.when(core == 0)
    def _():
        enter_half(CHIPS)

    @pl.when(core == 1)
    def _():
        swap_start.wait_recv()

    final_group(5, 0)
    squares[...] = jnp.zeros_like(squares)
    for tile in range(CUT_TILES):
        gap = result(cut_slot(CLEAN, tile)).astype(F32)
        gap = gap - cut[:, tile * LANES : (tile + 1) * LANES].astype(F32)
        squares[tile : tile + 1, :] = jnp.sum(gap * gap, axis=0, keepdims=True)

    def along_z(k):
        return 16 * row_x + 2 * lax.rem(line_z + k, 8) + 1

    def along_x(k):
        return 16 * lax.rem(row_x + k, 4) + 2 * line_z + 1

    def share(peer_of, count, slot, src, dst, send_sem, recv_sem):
        for k in range(1, count):
            to_shard(peer_of(k), src, dst.at[slot], send_sem, recv_sem).start()
        dst[slot] = src[...]

    seven, three = pl.ds(0, 7), pl.ds(0, 3)
    squares_over = to_shard(mate, squares, pair_squares, send_qq, recv_qq)

    @pl.when(core == 0)
    def _():
        squares_over.start()

    whole[v] = cut[...]

    lax.fori_loop(0, 5, final_group, 0)
    def patched_tile(tile, _):
        cols = pl.ds(pl.multiple_of(tile * LANES, LANES), LANES)
        patched[:, cols] = result(tile)
        return 0

    lax.fori_loop(0, TILES, patched_tile, 0, unroll=4)


    @pl.when(core == 1)
    def _():
        squares_over.wait_recv()
        chip_squares[...] = squares[...] + pair_squares[...]
        share(along_z, 8, line_z, chip_squares, squares_z, send_sz, recv_sz)

    for direct in directs:
        direct.wait()

    for w in range(VARS):
        def peak_tile(i, _):
            here = pl.ds(pl.multiple_of(i * LANES, LANES), LANES)
            there = pl.ds(pl.multiple_of(w * SPAN + i * LANES, LANES), LANES)
            gap = jnp.abs(patched[:, there].astype(F32) - whole[w, :, here].astype(F32))
            peaks[pl.ds(w * CUT_TILES + i, 1), :] = jnp.max(gap, axis=0, keepdims=True)
            return 0

        lax.fori_loop(0, CUT_TILES, peak_tile, 0, unroll=2)

    sent_peaks[...] = peaks[...].astype(BF16)
    peaks_over = to_shard(mate, sent_peaks, pair_peaks, send_pp, recv_pp)
    answer_over = to_shard(mate, answer, answer, send_an, recv_an)

    @pl.when(core == 0)
    def _():
        peaks_over.start()

    @pl.when(core == 1)
    def _():
        wait_for(squares_z.at[seven], recv_sz)
        line_squares[...] = jnp.sum(squares_z[...], axis=0)
        share(along_x, 4, row_x, line_squares, squares_x, send_sx, recv_sx)
        peaks_over.wait_recv()
        both = jnp.maximum(sent_peaks[...].astype(F32), pair_peaks[...].astype(F32))
        chip_peaks[...] = both.astype(BF16)
        share(along_z, 8, line_z, chip_peaks, peaks_z, send_pz, recv_pz)
        wait_for(squares_x.at[three], recv_sx)
        spreads[v] = jnp.sqrt(jnp.sum(squares_x[...], axis=0) / (SHARDS * ROWS) + TINY)
        for k in range(1, VARS):
            to_variant(k, spreads.at[v], spreads.at[v], send_sp.at[k], recv_sp.at[k]).start()
        wait_for(peaks_z.at[seven], recv_pz)
        line_peaks[...] = jnp.max(peaks_z[...].astype(F32), axis=0).astype(BF16)
        share(along_x, 4, row_x, line_peaks, peaks_x, send_px, recv_px)
        wait_for(peaks_x.at[three], recv_px)
        for k in range(1, VARS):
            there = spreads.at[lax.rem(v + VARS - k, VARS)]
            to_variant(k, there, there, send_sp.at[k], recv_sp.at[k]).wait()
        peak = jnp.max(peaks_x[...].astype(F32), axis=0)
        for w in range(VARS):
            rows = slice(w * CUT_TILES, (w + 1) * CUT_TILES)
            answer[rows, :] = peak[rows, :] / spreads[w, :CUT_TILES, :]
        answer_over.start()
        wait_for(squares_z.at[seven], send_sz)
        wait_for(squares_x.at[three], send_sx)
        wait_for(peaks_z.at[seven], send_pz)
        wait_for(peaks_x.at[three], send_px)
        answer_over.wait_send()

    @pl.when(core == 0)
    def _():
        squares_over.wait_send()
        peaks_over.wait_send()
        answer_over.wait_recv()

    effect[...] = answer[...]
    @pl.when(core == 0)
    def _():
        wait_for(chip_ends.at[others], send_ce)

    @pl.when((core == 1) & (chip < BUSY))
    def _():
        wait_for(chip_ends.at[pl.ds(0, BUSY - 1)], send_ce)

    @pl.when((core == 1) & (chip >= BUSY))
    def _():
        wait_for(chip_ends.at[pl.ds(0, BUSY)], send_ce)

    @pl.when(owns)
    def _():
        wait_for(leaving.at[others], send_in)

    swap_start.wait_send()


SMEM = pl.BlockSpec(memory_space=pltpu.SMEM)
HBM = pl.BlockSpec(memory_space=pltpu.HBM)
VMEM = pl.BlockSpec(memory_space=pltpu.VMEM)
DMA = pltpu.SemaphoreType.DMA


def shards(
    clean_proj, corrupt_proj, patch_pos, patch_mode, a_log, dt_bias,
    conv_weight, conv_bias, x_weight, dt_weight, d_skip,
):
    hold = functools.partial(pltpu.with_memory_space_constraint, memory_space=pltpu.HBM)
    keep = functools.partial(pltpu.with_memory_space_constraint, memory_space=pltpu.VMEM)
    front = pl.pallas_call(
        front_kernel,
        out_shape=(
            pltpu.VMEM((3 * ROWS, INNER), BF16),
            pltpu.VMEM((RANK + 2 * STATE, INNER), BF16),
            pltpu.VMEM((RANK, INNER), BF16),
            pltpu.VMEM((1, INNER), F32),
            pltpu.VMEM((CHUNKS * STATE, LANES), F32),
        ),
        in_specs=[SMEM, SMEM] + [HBM] * 8,
        out_specs=(VMEM,) * 5,
        scratch_shapes=[
            pltpu.VMEM((8, INNER), BF16),
            pltpu.VMEM((STATE, INNER), F32),
            pltpu.VMEM((2, 8, INNER), BF16),
            pltpu.VMEM((8, INNER), F32),
            pltpu.VMEM((8, INNER), BF16),
            pltpu.VMEM((ROWS, INNER), BF16),
            pltpu.VMEM((ROWS, INNER), BF16),
            pltpu.VMEM((TAPS, INNER), F32),
            pltpu.VMEM((1, INNER), F32),
            pltpu.VMEM((3 * TILES * (8 + ROWS), LANES), F32),
            DMA((10,)),
            DMA,
            DMA,
        ],
        compiler_params=pltpu.CompilerParams(
            collective_id=1, has_side_effects=True, vmem_limit_bytes=40_000_000
        ),
        name="front",
    )(
        hold(patch_pos), patch_mode,
        *map(
            hold,
            (
                clean_proj, corrupt_proj, conv_weight, conv_bias[None], x_weight.T, dt_weight,
                dt_bias[None], a_log,
            ),
        ),
    )
    row = (1, LANES)
    tile = (STATE, LANES)
    patched, effect = pl.pallas_call(
        kernel,
        out_shape=(pltpu.VMEM((ROWS, INNER), BF16), pltpu.VMEM((TILES, LANES), F32)),
        in_specs=[SMEM, SMEM] + [VMEM] * 5 + [HBM] * 3,
        out_specs=(VMEM, VMEM),
        scratch_shapes=[
            pltpu.VMEM((ROWS, INNER), BF16),
            pltpu.VMEM((ROWS, INNER), BF16),
            pltpu.VMEM((1, INNER), F32),
            pltpu.VMEM((3 * ROWS, RANK), BF16),
            pltpu.VMEM((3 * ROWS, STATE), F32),
            pltpu.VMEM((GROUPS * ROWS * STATE * 8, LANES), F32),
            pltpu.VMEM((CHUNKS * ROWS, LANES), F32),
            pltpu.VMEM((CHUNKS * ROWS, LANES), F32),
            pltpu.VMEM((ROWS * PITCH, LANES), F32),
            pltpu.VMEM((ROWS * PITCH, LANES), F32),
            pltpu.VMEM((3 * ROWS * SPLAT + 8, LANES), F32),
            pltpu.VMEM((3 * ROWS * SPLAT + 8, LANES), F32),
            pltpu.VMEM((CHUNKS * STATE, LANES), F32),
            pltpu.VMEM((CHUNKS, *row), F32),
            pltpu.VMEM((HALF * STATE, LANES), F32),
            pltpu.VMEM((HALF, *row), F32),
            pltpu.VMEM((HALF, STATE + 1, LANES), F32),
            pltpu.VMEM((CHIPS, STATE + 1, LANES), F32),
            pltpu.VMEM((CHIPS, *tile), F32),
            pltpu.VMEM((HALF, *tile), F32),
            pltpu.VMEM((HALF * STATE, LANES), F32),
            pltpu.VMEM((CHUNKS * STATE, LANES), F32),
            pltpu.VMEM((ROWS * PITCH, LANES), F32),
            pltpu.VMEM((ROWS, SPAN), BF16),
            pltpu.VMEM((STATE, LANES), F32),
            pltpu.VMEM((VARS, ROWS, SPAN), BF16),
            pltpu.VMEM((TILES, LANES), F32),
            pltpu.VMEM((8, STATE, LANES), F32),
            pltpu.VMEM((STATE, LANES), F32),
            pltpu.VMEM((4, STATE, LANES), F32),
            pltpu.VMEM((VARS, STATE, LANES), F32),
            pltpu.VMEM((8, TILES, LANES), BF16),
            pltpu.VMEM((TILES, LANES), BF16),
            pltpu.VMEM((4, TILES, LANES), BF16),
            pltpu.VMEM((STATE, LANES), F32),
            pltpu.VMEM((STATE, LANES), F32),
            pltpu.VMEM((TILES, LANES), BF16),
            pltpu.VMEM((TILES, LANES), BF16),
            pltpu.VMEM((TILES, LANES), BF16),
            pltpu.VMEM((TILES, LANES), F32),
            DMA((3,)),
        ]
        + [DMA] * 10
        + [DMA((VARS,)), DMA((VARS,))]
        + [DMA] * 4
        + [DMA((VARS,)), DMA((VARS,))]
        + [DMA] * 10,
        compiler_params=pltpu.CompilerParams(
            collective_id=0, has_side_effects=True, vmem_limit_bytes=54_000_000
        ),
        name="mixer",
    )(
        hold(patch_pos), patch_mode, *map(keep, front),
        *map(hold, (clean_proj, corrupt_proj, d_skip[None])),
    )
    patched, effect = pl.pallas_call(
        emit_kernel,
        out_shape=(
            jax.ShapeDtypeStruct((ROWS, INNER), BF16),
            jax.ShapeDtypeStruct((TILES, LANES), F32),
        ),
        in_specs=[VMEM, VMEM],
        out_specs=(HBM, HBM),
        scratch_shapes=[DMA((2,))],
        compiler_params=pltpu.CompilerParams(vmem_limit_bytes=16_000_000),
        name="emit",
    )(
        keep(patched), keep(effect),
    )
    return (patched[None], effect.reshape(1, INNER))


def solution(mesh):
    return jax.shard_map(
        shards,
        mesh=mesh,
        in_specs=(
            P("seq", None), P("seq", None), P("var", None), P("var"),
            P(), P(), P(), P(), P(), P(), P(),
        ),
        out_specs=(P("var", "seq", None), P("var", None)),
        check_vma=False,
    )
```

```python
import functools

import jax
import jax.numpy as jnp
from jax import lax
from jax.experimental import pallas as pl
from jax.experimental.pallas import tpu as pltpu
from jax.sharding import PartitionSpec as P

STATE = 16
RANK = 160
ROWS = 32
INNER = 5120
SPAN = 1280
TAPS = 4
LANES = 128
CHUNKS = 64
SHARDS = 64
VARS = 4
TILES = INNER // LANES
CUT_TILES = SPAN // LANES
GROUPS = CHUNKS // 8
BUSY = 28
HALF = CHUNKS // 2
CHIPS = SHARDS // 2
PITCH = 72
SPLAT = 17
MESH = pl.DeviceIdType.MESH
LOG2E = 1.4426950408889634
TINY = 1e-06
F32 = jnp.float32
BF16 = jnp.bfloat16
UNROLL = 8
CLEAN, CORRUPT, PATCHED = 0, 1, 2
STEPS = sorted(
    ((dx, dz) for dx in range(4) for dz in range(8) if dx or dz),
    key=lambda step: -(min(step[0], 4 - step[0]) + min(step[1], 8 - step[1])),
)


def cut_slot(run, tile):
    if tile < 8:
        return TILES + 8 * run + tile
    return 56 + 2 * run + (tile - 8)


def rate_at(slot):
    return pl.ds(lax.div(slot, 8) * (STATE * 8) + lax.rem(slot, 8), STATE, stride=8)


def hit_rows(pos_ref, first, count):
    rows = first + lax.broadcasted_iota(jnp.int32, (count, LANES), 0)
    hits = rows == pos_ref[0, 0]
    for k in range(1, pos_ref.shape[1]):
        hits = hits | (rows == pos_ref[0, k])
    return hits


def silu(value):
    return value / (1.0 + jnp.exp(-value))


def softplus(value):
    return jnp.maximum(value, 0.0) + jnp.log1p(jnp.exp(-jnp.abs(value)))


def row_of(ref, row):
    return jnp.broadcast_to(ref[pl.ds(row, 1), :], (8, LANES))


def scan_group(dts, us, rate, group, state, drive, readout, out):
    def step(t, carry):
        row = pl.multiple_of(t * PITCH + group * 8, 8)
        steps = dts[pl.ds(row, 8), :]
        flow = us[pl.ds(row, 8), :]
        entries = []
        total = None
        for n in range(STATE):
            decay = jnp.exp2(steps * rate[n])
            entry = decay * carry[n] + flow * drive(t, n)
            entries.append(entry)
            if readout is not None:
                term = readout(t, n) * entry
                total = term if total is None else total + term
        if readout is not None:
            out[pl.ds(row, 8), :] = total
        return tuple(entries)

    return lax.fori_loop(0, ROWS, step, state, unroll=UNROLL)


def splat_reader(ref, base):
    return lambda t, n: row_of(ref, base + t * SPLAT + n)


def mixed_reader(ref):
    first = lax.broadcasted_iota(jnp.int32, (8, LANES), 0) < 2

    def read(t, n):
        return jnp.where(
            first,
            row_of(ref, CLEAN * ROWS * SPLAT + t * SPLAT + n),
            row_of(ref, CORRUPT * ROWS * SPLAT + t * SPLAT + n),
        )

    return read


def wait_for(ref, sem):
    pltpu.make_async_copy(ref, ref, sem).wait()


def front_kernel(
    pos, mode, clean_in, corrupt_in, conv_w_in, conv_b_in, x_w_in, dt_w_in, dt_b_in, a_log_in,
    acts, x_w, dt_w, dt_b, rates,
    rims, a_log, ends, wide, packed, clean, corrupt, conv_w, conv_b, pad, load_sem, send_sem, recv_sem,
):
    me = lax.axis_index("seq")
    v = lax.axis_index("var")
    after = lax.min(me + 1, SHARDS - 1)
    has_next, has_last = me < SHARDS - 1, me > 0
    barrier = pltpu.get_barrier_semaphore()
    loads = [
        pltpu.make_async_copy(src, dst, load_sem.at[i])
        for i, (src, dst) in enumerate(
            (
                (clean_in.at[ROWS - 8 :, :INNER], ends.at[0]),
                (corrupt_in.at[ROWS - 8 :, :INNER], ends.at[1]),
                (clean_in.at[:, :INNER], clean), (corrupt_in.at[:, :INNER], corrupt),
                (conv_w_in, conv_w), (conv_b_in, conv_b), (x_w_in, x_w), (dt_w_in, dt_w),
                (dt_b_in, dt_b), (a_log_in, a_log),
            )
        )
    ]
    for load in loads:
        load.start()

    def signal(peer):
        pl.semaphore_signal(barrier, inc=1, device_id=(peer, v), device_id_type=MESH)

    @pl.when(has_next)
    def _():
        signal(me + 1)

    @pl.when(has_last)
    def _():
        signal(me - 1)

    for load in loads[:2]:
        load.wait()
    margin = TAPS - 1
    wide[...] = jnp.zeros_like(wide)
    for i in range(2):
        wide[i * margin : (i + 1) * margin, :] = ends[i].astype(F32)[8 - margin :, :]
    packed[...] = wide[...].astype(BF16)
    first = me * ROWS
    take = hit_rows(pos, first, ROWS)[:, :1] & (mode[0] != 1)
    take_rim = hit_rows(pos, first - margin, margin)[:, :1] & (mode[0] != 1)
    pl.semaphore_wait(barrier, lax.min(me, 1) + lax.min(SHARDS - 1 - me, 1))
    copy = pltpu.make_async_remote_copy(
        src_ref=packed, dst_ref=rims, send_sem=send_sem, recv_sem=recv_sem,
        device_id=(after, v), device_id_type=MESH,
    )

    @pl.when(has_next)
    def _():
        copy.start()

    for load in loads[2:6]:
        load.wait()
    width = 512
    span = 8 + ROWS
    per = width // LANES

    def columns(i):
        return pl.ds(pl.multiple_of(i * width, width), width)

    def fill(i, _):
        sig_clean = clean[:, columns(i)].astype(F32)
        sig_corrupt = corrupt[:, columns(i)].astype(F32)
        pieces = (sig_clean, sig_corrupt, jnp.where(take, sig_clean, sig_corrupt))
        for run, sig in enumerate(pieces):
            for k in range(per):
                at = pl.multiple_of((run * TILES + i * per + k) * span, 8)
                pad[pl.ds(at, 8), :] = jnp.zeros((8, LANES), F32)
                pad[pl.ds(at + 8, ROWS), :] = sig[:, k * LANES : (k + 1) * LANES]
        return 0

    def convolve(rows):
        def body(tile, _):
            cols = pl.ds(pl.multiple_of(tile * LANES, LANES), LANES)
            bias = conv_b[:, cols]
            for run in range(3):
                at = (run * TILES + tile) * span + 8 - margin
                total = bias + conv_w[0:1, cols] * pad[pl.ds(at, rows), :]
                for k in range(1, TAPS):
                    total = total + conv_w[k : k + 1, cols] * pad[pl.ds(at + k, rows), :]
                acts[run * ROWS : run * ROWS + rows, cols] = silu(total).astype(BF16)
            return 0

        lax.fori_loop(0, TILES, body, 0, unroll=4 if rows == ROWS else 10)

    def fill_rim(i, _):
        rim = rims[:, columns(i)].astype(F32)
        rim_clean, rim_corrupt = rim[:margin], rim[margin : 2 * margin]
        pieces = (rim_clean, rim_corrupt, jnp.where(take_rim, rim_clean, rim_corrupt))
        for run, part in enumerate(pieces):
            for k in range(per):
                at = (run * TILES + i * per + k) * span + 8 - margin
                pad[pl.ds(at, margin), :] = part[:, k * LANES : (k + 1) * LANES]
        return 0

    lax.fori_loop(0, INNER // width, fill, 0)
    convolve(ROWS)
    for load in loads[6:]:
        load.wait()

    def rate_of(slot, cols):
        rates[rate_at(slot), :] = jnp.exp(a_log[:, cols]) * (-LOG2E)

    def patched_rate(tile, _):
        rate_of(tile, pl.ds(pl.multiple_of(tile * LANES, LANES), LANES))
        return 0

    lax.fori_loop(0, TILES, patched_rate, 0, unroll=4)
    for tile in range(CUT_TILES):
        for run in (CLEAN, CORRUPT):
            cols = pl.ds(pl.multiple_of(v * SPAN + tile * LANES, LANES), LANES)
            rate_of(cut_slot(run, tile), cols)
    for slot in range(60, CHUNKS):
        rates[rate_at(slot), :] = jnp.zeros((STATE, LANES), F32)

    @pl.when(has_last)
    def _():
        copy.wait_recv()
        lax.fori_loop(0, INNER // width, fill_rim, 0, unroll=5)
        convolve(8)

    @pl.when(has_next)
    def _():
        copy.wait_send()


def emit_kernel(patched, effect, patched_out, effect_out, sems):
    copies = [
        pltpu.make_async_copy(patched, patched_out, sems.at[0]),
        pltpu.make_async_copy(effect, effect_out, sems.at[1]),
    ]
    for copy in copies:
        copy.start()
    for copy in copies:
        copy.wait()


def kernel(
    pos, mode, acts, x_w, dt_w, dt_b, rates, clean_in, corrupt_in, d_skip_in,
    patched, effect,
    clean_gate, corrupt_gate, d_skip, low, maps, weights, base, gates, dts, us, bs, cs, ends, totals,
    pair_ends, pair_totals, chip_ends, got_ends,
    leaving, landed, across, start, ys,
    cut, squares, whole, peaks, squares_z, line_squares, squares_x, spreads,
    peaks_z, line_peaks, peaks_x, pair_squares, chip_squares, pair_peaks, chip_peaks, sent_peaks, answer,
    load_sem, send_pt, recv_pt, send_pe, recv_pe, send_ce, recv_ce,
    send_in, recv_in, send_st, recv_st,
    send_cut, recv_cut, send_sz, recv_sz, send_sx, recv_sx, send_sp, recv_sp,
    send_pz, recv_pz, send_px, recv_px, send_qq, recv_qq, send_pp, recv_pp, send_an, recv_an,
):
    me = lax.axis_index("seq")
    v = lax.axis_index("var")
    chip = lax.div(me, 2)
    core = lax.rem(me, 2)
    mate = me + 1 - 2 * core
    mine = core * HALF
    theirs = HALF - mine
    barrier = pltpu.get_barrier_semaphore()

    loads = [
        pltpu.make_async_copy(src, dst, load_sem.at[i])
        for i, (src, dst) in enumerate(
            (
                (d_skip_in, d_skip), (clean_in.at[:, INNER:], clean_gate),
                (corrupt_in.at[:, INNER:], corrupt_gate),
            )
        )
    ]
    for load in loads:
        load.start()

    def signal(peer, variant):
        pl.semaphore_signal(barrier, inc=1, device_id=(peer, variant), device_id_type=MESH)

    row_x, line_z = lax.div(chip, 8), lax.rem(chip, 8)
    peers = [8 * lax.rem(row_x + dx, 4) + lax.rem(line_z + dz, 8) for dx, dz in STEPS]
    for peer in peers:
        signal(2 * peer + core, v)
    signal(mate, v)
    for k in range(1, VARS):
        signal(me, lax.rem(v + k, VARS))

    def to_variant(k, src, dst, send_sem, recv_sem):
        return pltpu.make_async_remote_copy(
            src_ref=src, dst_ref=dst, send_sem=send_sem, recv_sem=recv_sem,
            device_id=(me, lax.rem(v + k, VARS)), device_id_type=MESH,
        )

    def to_shard(peer, src, dst, send_sem, recv_sem):
        return pltpu.make_async_remote_copy(
            src_ref=src, dst_ref=dst, send_sem=send_sem, recv_sem=recv_sem,
            device_id=(peer, v), device_id_type=MESH,
        )

    take_gate = hit_rows(pos, me * ROWS, ROWS)[:, :1] & (mode[0] != 0)

    projected = lax.dot_general(
        acts[...], x_w[...], (((1,), (1,)), ((), ())), preferred_element_type=F32
    )
    low[...] = projected[:, :RANK].astype(BF16)
    maps[...] = projected[:, RANK + STATE :]
    for run in range(3):
        part = projected[run * ROWS : (run + 1) * ROWS]
        for n in range(STATE):
            at = run * ROWS * SPLAT + n
            bs[pl.ds(at, ROWS, stride=SPLAT), :] = jnp.broadcast_to(
                part[:, RANK + n : RANK + n + 1], (ROWS, LANES)
            )


    def place(slot, steps, act):
        dts[pl.ds(slot, ROWS, stride=PITCH), :] = steps
        us[pl.ds(slot, ROWS, stride=PITCH), :] = steps * act
        totals[slot] = jnp.sum(steps, axis=0, keepdims=True)

    wide = 5120

    def patched_steps(i, _):
        cols = pl.ds(pl.multiple_of(i * wide, wide), wide)
        raw = jnp.dot(low[2 * ROWS :, :], dt_w[:, cols], preferred_element_type=F32)
        steps = softplus(raw + dt_b[:, cols])
        act = acts[2 * ROWS :, cols].astype(F32)
        for k in range(wide // LANES):
            part = slice(k * LANES, (k + 1) * LANES)
            place(i * (wide // LANES) + k, steps[:, part], act[:, part])
        return 0

    lax.fori_loop(0, INNER // wide, patched_steps, 0)

    cols = pl.ds(pl.multiple_of(v * SPAN, LANES), SPAN)
    raw = jnp.dot(low[: 2 * ROWS, :], dt_w[:, cols], preferred_element_type=F32)
    steps = softplus(raw + dt_b[:, cols])
    act = acts[: 2 * ROWS, cols].astype(F32)
    for run in (CLEAN, CORRUPT):
        rows = slice(run * ROWS, (run + 1) * ROWS)
        for tile in range(CUT_TILES):
            part = slice(tile * LANES, (tile + 1) * LANES)
            place(cut_slot(run, tile), steps[rows, part], act[rows, part])
    blank = jnp.zeros((ROWS, LANES), F32)
    for slot in range(60, CHUNKS):
        place(slot, blank, blank)

    zero = jnp.zeros((8, LANES), F32)

    def rates_of(group):
        base = group * (STATE * 8)
        return [rates[pl.ds(pl.multiple_of(base + n * 8, 8), 8), :] for n in range(STATE)]

    def run_base(group):
        return jnp.where(group < 5, PATCHED, group - 5) * (ROWS * SPLAT)

    def local_group(group, drive):
        found = scan_group(
            dts, us, rates_of(group), group, (zero,) * STATE, drive, None, None
        )
        for n in range(STATE):
            ends[pl.ds(group * (STATE * 8) + n, 8, stride=STATE), :] = found[n]

    def local_pass(offset):
        def body(i, _):
            group = offset + i

            @pl.when(group < GROUPS - 1)
            def _():
                local_group(group, splat_reader(bs, run_base(group)))

            @pl.when(group == GROUPS - 1)
            def _():
                local_group(group, mixed_reader(bs))

            return 0

        lax.fori_loop(0, GROUPS // 2, body, 0)

    local_pass(lax.div(theirs, 8))
    pl.semaphore_wait(barrier, CHIPS - 1 + 1 + VARS - 1)
    theirs_3 = pl.ds(theirs, HALF)
    swap_totals = to_shard(mate, totals.at[theirs_3], pair_totals, send_pt, recv_pt)
    swap_totals.start()

    theirs_2 = pl.ds(pl.multiple_of(theirs * STATE, 8), HALF * STATE)
    swap_ends = to_shard(mate, ends.at[theirs_2], pair_ends, send_pe, recv_pe)
    swap_ends.start()
    local_pass(lax.div(mine, 8))
    swap_totals.wait()

    leads = core == 0

    def my_summary(k):
        own = ends[pl.ds(pl.multiple_of((mine + k) * STATE, 8), STATE), :]
        return own, totals[mine + k]

    def pair_of(k):
        own_end, own_total = my_summary(k)
        other_end = pair_ends[pl.ds(pl.multiple_of(k * STATE, 8), STATE), :]
        other_total = pair_totals[k]
        return (
            jnp.where(leads, own_end, other_end), jnp.where(leads, own_total, other_total),
            jnp.where(leads, other_end, own_end), jnp.where(leads, other_total, own_total),
        )

    swap_ends.wait()

    def chip_end(k, _):
        end_a, total_a, end_b, total_b = pair_of(k)
        chip_ends[k, :STATE] = jnp.exp2(rates[rate_at(mine + k), :] * total_b) * end_a + end_b
        chip_ends[k, STATE:] = total_a + total_b
        return 0

    lax.fori_loop(0, HALF, chip_end, 0, unroll=8)
    owns = (core == 0) | (chip < BUSY)
    others = pl.ds(0, CHIPS - 1)

    @pl.when(owns)
    def _():
        pltpu.make_async_copy(chip_ends.at[chip], got_ends.at[chip], recv_ce).start()

    for peer in peers:
        @pl.when((core == 0) | (peer < BUSY))
        def _():
            target = 2 * peer + core
            to_shard(target, chip_ends.at[peer], got_ends.at[chip], send_ce, recv_ce).start()

    my_rate = rates[rate_at(mine + chip), :]
    for run in range(3):
        for n in range(STATE):
            cs[pl.ds(run * ROWS * SPLAT + n, ROWS, stride=SPLAT), :] = jnp.broadcast_to(
                maps[run * ROWS : (run + 1) * ROWS, n : n + 1], (ROWS, LANES)
            )

    def local_readout(group, drive, read):
        scan_group(dts, us, rates_of(group), group, (zero,) * STATE, drive, read, ys)

    def plain_readout(group, _):
        at = run_base(group)
        local_readout(group, splat_reader(bs, at), splat_reader(cs, at))
        return 0

    lax.fori_loop(0, GROUPS - 1, plain_readout, 0)
    local_readout(GROUPS - 1, mixed_reader(bs), mixed_reader(cs))
    def chain(s, state):
        leaving[s] = state
        return jnp.exp2(my_rate * got_ends[s, STATE:]) * state + got_ends[s, :STATE]

    @pl.when(owns)
    def _():
        wait_for(got_ends, recv_ce)
        lax.fori_loop(0, CHIPS, chain, jnp.zeros((STATE, LANES), F32), unroll=4)
        pltpu.make_async_copy(leaving.at[chip], landed.at[chip], recv_in).start()
        for peer in peers:
            to_shard(2 * peer + core, leaving.at[peer], landed.at[chip], send_in, recv_in).start()

    def entry_weights(group, read):
        rate = rates_of(group)

        def step(t, run_total):
            row = pl.multiple_of(t * PITCH + group * 8, 8)
            run_total = run_total + dts[pl.ds(row, 8), :]
            at = (group * ROWS + t) * (STATE * 8)
            for n in range(STATE):
                weights[pl.ds(pl.multiple_of(at + n * 8, 8), 8), :] = read(t, n) * jnp.exp2(
                    run_total * rate[n]
                )
            return run_total

        lax.fori_loop(0, ROWS, step, zero, unroll=4)

    def plain_weights(group, _):
        entry_weights(group, splat_reader(cs, run_base(group)))
        return 0

    lax.fori_loop(0, GROUPS - 1, plain_weights, 0)
    entry_weights(GROUPS - 1, mixed_reader(cs))
    for load in loads:
        load.wait()

    def prepare(slot, act, skip, gate):
        rows = pl.ds(pl.multiple_of(slot * ROWS, 8), ROWS)
        base[rows, :] = ys[pl.ds(slot, ROWS, stride=PITCH), :] + skip * act
        gates[rows, :] = silu(gate)

    for run, gate_rows in ((CLEAN, clean_gate), (CORRUPT, corrupt_gate)):
        for tile in range(CUT_TILES):
            cols = pl.ds(pl.multiple_of(v * SPAN + tile * LANES, LANES), LANES)
            act = acts[run * ROWS : (run + 1) * ROWS, cols].astype(F32)
            prepare(cut_slot(run, tile), act, d_skip[:, cols], gate_rows[:, cols].astype(F32))

    def prepare_patched(tile, _):
        cols = pl.ds(pl.multiple_of(tile * LANES, LANES), LANES)
        gate = jnp.where(
            take_gate, clean_gate[:, cols].astype(F32), corrupt_gate[:, cols].astype(F32)
        )
        prepare(tile, acts[2 * ROWS :, cols].astype(F32), d_skip[:, cols], gate)
        return 0

    lax.fori_loop(0, TILES, prepare_patched, 0, unroll=2)
    def enter(k, _):
        end_a, total_a, _, _ = pair_of(k)
        before = landed[k]
        after = jnp.exp2(rates[rate_at(mine + k), :] * total_a) * before + end_a
        at = pl.ds(pl.multiple_of((mine + k) * STATE, 8), STATE)
        start[at, :] = jnp.where(leads, before, after)
        across[pl.ds(pl.multiple_of(k * STATE, 8), STATE), :] = jnp.where(leads, after, before)
        return 0

    swap_start = to_shard(
        mate, across, start.at[pl.ds(pl.multiple_of(mine * STATE, 8), HALF * STATE)],
        send_st, recv_st,
    )

    def enter_half(sources):
        wait_for(landed.at[pl.ds(0, sources)], recv_in)
        lax.fori_loop(0, HALF, enter, 0, unroll=8)
        swap_start.start()

    @pl.when(core == 1)
    def _():
        enter_half(BUSY)

    @pl.when(core == 0)
    def _():
        swap_start.wait_recv()

    def final_group(group, _):
        at = group * (STATE * 8)
        state = [start[pl.ds(at + n, 8, stride=STATE), :] for n in range(STATE)]

        def step(t, _):
            at = (group * ROWS + t) * (STATE * 8)
            total = None
            for n in range(STATE):
                term = weights[pl.ds(pl.multiple_of(at + n * 8, 8), 8), :] * state[n]
                total = term if total is None else total + term
            ys[pl.ds(pl.multiple_of(t * PITCH + group * 8, 8), 8), :] = total
            return 0

        lax.fori_loop(0, ROWS, step, 0, unroll=8)
        return 0

    def result(slot):
        rows = pl.ds(pl.multiple_of(slot * ROWS, 8), ROWS)
        y = ys[pl.ds(slot, ROWS, stride=PITCH), :]
        return ((y + base[rows, :]) * gates[rows, :]).astype(BF16)

    lax.fori_loop(6, GROUPS, final_group, 0)

    for tile in range(CUT_TILES):
        cut[:, tile * LANES : (tile + 1) * LANES] = result(cut_slot(CORRUPT, tile))
    directs = [
        to_variant(k, cut, whole.at[v], send_cut.at[k], recv_cut.at[k]) for k in (2, 1, VARS - 1)
    ]
    for direct in directs:
        direct.start()
    @pl.when(core == 0)
    def _():
        enter_half(CHIPS)

    @pl.when(core == 1)
    def _():
        swap_start.wait_recv()

    final_group(5, 0)
    squares[...] = jnp.zeros_like(squares)
    for tile in range(CUT_TILES):
        gap = result(cut_slot(CLEAN, tile)).astype(F32)
        gap = gap - cut[:, tile * LANES : (tile + 1) * LANES].astype(F32)
        squares[tile : tile + 1, :] = jnp.sum(gap * gap, axis=0, keepdims=True)

    def along_z(k):
        return 16 * row_x + 2 * lax.rem(line_z + k, 8) + 1

    def along_x(k):
        return 16 * lax.rem(row_x + k, 4) + 2 * line_z + 1

    def share(peer_of, count, slot, src, dst, send_sem, recv_sem):
        for k in sorted(range(1, count), key=lambda k: -min(k, count - k)):
            to_shard(peer_of(k), src, dst.at[slot], send_sem, recv_sem).start()
        dst[slot] = src[...]

    seven, three = pl.ds(0, 7), pl.ds(0, 3)
    squares_over = to_shard(mate, squares, pair_squares, send_qq, recv_qq)

    @pl.when(core == 0)
    def _():
        squares_over.start()

    whole[v] = cut[...]

    lax.fori_loop(0, 5, final_group, 0)
    def patched_tile(tile, _):
        cols = pl.ds(pl.multiple_of(tile * LANES, LANES), LANES)
        patched[:, cols] = result(tile)
        return 0

    lax.fori_loop(0, TILES, patched_tile, 0, unroll=4)


    @pl.when(core == 1)
    def _():
        squares_over.wait_recv()
        chip_squares[...] = squares[...] + pair_squares[...]
        share(along_z, 8, line_z, chip_squares, squares_z, send_sz, recv_sz)

    for direct in directs:
        direct.wait()

    for w in range(VARS):
        def peak_tile(i, _):
            here = pl.ds(pl.multiple_of(i * LANES, LANES), LANES)
            there = pl.ds(pl.multiple_of(w * SPAN + i * LANES, LANES), LANES)
            gap = jnp.abs(patched[:, there].astype(F32) - whole[w, :, here].astype(F32))
            peaks[pl.ds(w * CUT_TILES + i, 1), :] = jnp.max(gap, axis=0, keepdims=True)
            return 0

        lax.fori_loop(0, CUT_TILES, peak_tile, 0, unroll=2)

    sent_peaks[...] = peaks[...].astype(BF16)
    peaks_over = to_shard(mate, sent_peaks, pair_peaks, send_pp, recv_pp)
    answer_over = to_shard(mate, answer, answer, send_an, recv_an)

    @pl.when(core == 0)
    def _():
        peaks_over.start()

    @pl.when(core == 1)
    def _():
        wait_for(squares_z.at[seven], recv_sz)
        line_squares[...] = jnp.sum(squares_z[...], axis=0)
        share(along_x, 4, row_x, line_squares, squares_x, send_sx, recv_sx)
        peaks_over.wait_recv()
        both = jnp.maximum(sent_peaks[...].astype(F32), pair_peaks[...].astype(F32))
        chip_peaks[...] = both.astype(BF16)
        share(along_z, 8, line_z, chip_peaks, peaks_z, send_pz, recv_pz)
        wait_for(squares_x.at[three], recv_sx)
        spreads[v] = jnp.sqrt(jnp.sum(squares_x[...], axis=0) / (SHARDS * ROWS) + TINY)
        for k in range(1, VARS):
            to_variant(k, spreads.at[v], spreads.at[v], send_sp.at[k], recv_sp.at[k]).start()
        wait_for(peaks_z.at[seven], recv_pz)
        line_peaks[...] = jnp.max(peaks_z[...].astype(F32), axis=0).astype(BF16)
        share(along_x, 4, row_x, line_peaks, peaks_x, send_px, recv_px)
        wait_for(peaks_x.at[three], recv_px)
        for k in range(1, VARS):
            there = spreads.at[lax.rem(v + VARS - k, VARS)]
            to_variant(k, there, there, send_sp.at[k], recv_sp.at[k]).wait()
        peak = jnp.max(peaks_x[...].astype(F32), axis=0)
        for w in range(VARS):
            rows = slice(w * CUT_TILES, (w + 1) * CUT_TILES)
            answer[rows, :] = peak[rows, :] / spreads[w, :CUT_TILES, :]
        answer_over.start()
        wait_for(squares_z.at[seven], send_sz)
        wait_for(squares_x.at[three], send_sx)
        wait_for(peaks_z.at[seven], send_pz)
        wait_for(peaks_x.at[three], send_px)
        answer_over.wait_send()

    @pl.when(core == 0)
    def _():
        squares_over.wait_send()
        peaks_over.wait_send()
        answer_over.wait_recv()

    effect[...] = answer[...]
    @pl.when(core == 0)
    def _():
        wait_for(chip_ends.at[others], send_ce)

    @pl.when((core == 1) & (chip < BUSY))
    def _():
        wait_for(chip_ends.at[pl.ds(0, BUSY - 1)], send_ce)

    @pl.when((core == 1) & (chip >= BUSY))
    def _():
        wait_for(chip_ends.at[pl.ds(0, BUSY)], send_ce)

    @pl.when(owns)
    def _():
        wait_for(leaving.at[others], send_in)

    swap_start.wait_send()


SMEM = pl.BlockSpec(memory_space=pltpu.SMEM)
HBM = pl.BlockSpec(memory_space=pltpu.HBM)
VMEM = pl.BlockSpec(memory_space=pltpu.VMEM)
DMA = pltpu.SemaphoreType.DMA


def shards(
    clean_proj, corrupt_proj, patch_pos, patch_mode, a_log, dt_bias,
    conv_weight, conv_bias, x_weight, dt_weight, d_skip,
):
    hold = functools.partial(pltpu.with_memory_space_constraint, memory_space=pltpu.HBM)
    keep = functools.partial(pltpu.with_memory_space_constraint, memory_space=pltpu.VMEM)
    front = pl.pallas_call(
        front_kernel,
        out_shape=(
            pltpu.VMEM((3 * ROWS, INNER), BF16),
            pltpu.VMEM((RANK + 2 * STATE, INNER), BF16),
            pltpu.VMEM((RANK, INNER), BF16),
            pltpu.VMEM((1, INNER), F32),
            pltpu.VMEM((CHUNKS * STATE, LANES), F32),
        ),
        in_specs=[SMEM, SMEM] + [HBM] * 8,
        out_specs=(VMEM,) * 5,
        scratch_shapes=[
            pltpu.VMEM((8, INNER), BF16),
            pltpu.VMEM((STATE, INNER), F32),
            pltpu.VMEM((2, 8, INNER), BF16),
            pltpu.VMEM((8, INNER), F32),
            pltpu.VMEM((8, INNER), BF16),
            pltpu.VMEM((ROWS, INNER), BF16),
            pltpu.VMEM((ROWS, INNER), BF16),
            pltpu.VMEM((TAPS, INNER), F32),
            pltpu.VMEM((1, INNER), F32),
            pltpu.VMEM((3 * TILES * (8 + ROWS), LANES), F32),
            DMA((10,)),
            DMA,
            DMA,
        ],
        compiler_params=pltpu.CompilerParams(
            collective_id=1, has_side_effects=True, vmem_limit_bytes=40_000_000
        ),
        name="front",
    )(
        hold(patch_pos), patch_mode,
        *map(
            hold,
            (
                clean_proj, corrupt_proj, conv_weight, conv_bias[None], x_weight.T, dt_weight,
                dt_bias[None], a_log,
            ),
        ),
    )
    row = (1, LANES)
    tile = (STATE, LANES)
    patched, effect = pl.pallas_call(
        kernel,
        out_shape=(pltpu.VMEM((ROWS, INNER), BF16), pltpu.VMEM((TILES, LANES), F32)),
        in_specs=[SMEM, SMEM] + [VMEM] * 5 + [HBM] * 3,
        out_specs=(VMEM, VMEM),
        scratch_shapes=[
            pltpu.VMEM((ROWS, INNER), BF16),
            pltpu.VMEM((ROWS, INNER), BF16),
            pltpu.VMEM((1, INNER), F32),
            pltpu.VMEM((3 * ROWS, RANK), BF16),
            pltpu.VMEM((3 * ROWS, STATE), F32),
            pltpu.VMEM((GROUPS * ROWS * STATE * 8, LANES), F32),
            pltpu.VMEM((CHUNKS * ROWS, LANES), F32),
            pltpu.VMEM((CHUNKS * ROWS, LANES), F32),
            pltpu.VMEM((ROWS * PITCH, LANES), F32),
            pltpu.VMEM((ROWS * PITCH, LANES), F32),
            pltpu.VMEM((3 * ROWS * SPLAT + 8, LANES), F32),
            pltpu.VMEM((3 * ROWS * SPLAT + 8, LANES), F32),
            pltpu.VMEM((CHUNKS * STATE, LANES), F32),
            pltpu.VMEM((CHUNKS, *row), F32),
            pltpu.VMEM((HALF * STATE, LANES), F32),
            pltpu.VMEM((HALF, *row), F32),
            pltpu.VMEM((HALF, STATE + 1, LANES), F32),
            pltpu.VMEM((CHIPS, STATE + 1, LANES), F32),
            pltpu.VMEM((CHIPS, *tile), F32),
            pltpu.VMEM((HALF, *tile), F32),
            pltpu.VMEM((HALF * STATE, LANES), F32),
            pltpu.VMEM((CHUNKS * STATE, LANES), F32),
            pltpu.VMEM((ROWS * PITCH, LANES), F32),
            pltpu.VMEM((ROWS, SPAN), BF16),
            pltpu.VMEM((STATE, LANES), F32),
            pltpu.VMEM((VARS, ROWS, SPAN), BF16),
            pltpu.VMEM((TILES, LANES), F32),
            pltpu.VMEM((8, STATE, LANES), F32),
            pltpu.VMEM((STATE, LANES), F32),
            pltpu.VMEM((4, STATE, LANES), F32),
            pltpu.VMEM((VARS, STATE, LANES), F32),
            pltpu.VMEM((8, TILES, LANES), BF16),
            pltpu.VMEM((TILES, LANES), BF16),
            pltpu.VMEM((4, TILES, LANES), BF16),
            pltpu.VMEM((STATE, LANES), F32),
            pltpu.VMEM((STATE, LANES), F32),
            pltpu.VMEM((TILES, LANES), BF16),
            pltpu.VMEM((TILES, LANES), BF16),
            pltpu.VMEM((TILES, LANES), BF16),
            pltpu.VMEM((TILES, LANES), F32),
            DMA((3,)),
        ]
        + [DMA] * 10
        + [DMA((VARS,)), DMA((VARS,))]
        + [DMA] * 4
        + [DMA((VARS,)), DMA((VARS,))]
        + [DMA] * 10,
        compiler_params=pltpu.CompilerParams(
            collective_id=0, has_side_effects=True, vmem_limit_bytes=54_000_000
        ),
        name="mixer",
    )(
        hold(patch_pos), patch_mode, *map(keep, front),
        *map(hold, (clean_proj, corrupt_proj, d_skip[None])),
    )
    patched, effect = pl.pallas_call(
        emit_kernel,
        out_shape=(
            jax.ShapeDtypeStruct((ROWS, INNER), BF16),
            jax.ShapeDtypeStruct((TILES, LANES), F32),
        ),
        in_specs=[VMEM, VMEM],
        out_specs=(HBM, HBM),
        scratch_shapes=[DMA((2,))],
        compiler_params=pltpu.CompilerParams(vmem_limit_bytes=16_000_000),
        name="emit",
    )(
        keep(patched), keep(effect),
    )
    return (patched[None], effect.reshape(1, INNER))


def solution(mesh):
    return jax.shard_map(
        shards,
        mesh=mesh,
        in_specs=(
            P("seq", None), P("seq", None), P("var", None), P("var"),
            P(), P(), P(), P(), P(), P(), P(),
        ),
        out_specs=(P("var", "seq", None), P("var", None)),
        check_vma=False,
    )
```

```python
import functools

import jax
import jax.numpy as jnp
from jax import lax
from jax.experimental import pallas as pl
from jax.experimental.pallas import tpu as pltpu
from jax.sharding import PartitionSpec as P

STATE = 16
RANK = 160
ROWS = 32
INNER = 5120
SPAN = 1280
TAPS = 4
LANES = 128
CHUNKS = 64
SHARDS = 64
VARS = 4
TILES = INNER // LANES
CUT_TILES = SPAN // LANES
GROUPS = CHUNKS // 8
BUSY = 28
HALF = CHUNKS // 2
CHIPS = SHARDS // 2
PITCH = 72
SPLAT = 17
MESH = pl.DeviceIdType.MESH
LOG2E = 1.4426950408889634
TINY = 1e-06
F32 = jnp.float32
BF16 = jnp.bfloat16
UNROLL = 8
CLEAN, CORRUPT, PATCHED = 0, 1, 2
STEPS = sorted(
    ((dx, dz) for dx in range(4) for dz in range(8) if dx or dz),
    key=lambda step: -(min(step[0], 4 - step[0]) + min(step[1], 8 - step[1])),
)


def cut_slot(run, tile):
    if tile < 8:
        return TILES + 8 * run + tile
    return 56 + 2 * run + (tile - 8)


def rate_at(slot):
    return pl.ds(lax.div(slot, 8) * (STATE * 8) + lax.rem(slot, 8), STATE, stride=8)


def hit_rows(pos_ref, first, count):
    rows = first + lax.broadcasted_iota(jnp.int32, (count, LANES), 0)
    hits = rows == pos_ref[0, 0]
    for k in range(1, pos_ref.shape[1]):
        hits = hits | (rows == pos_ref[0, k])
    return hits


def silu(value):
    return value / (1.0 + jnp.exp(-value))


def softplus(value):
    return jnp.maximum(value, 0.0) + jnp.log1p(jnp.exp(-jnp.abs(value)))


def row_of(ref, row):
    return jnp.broadcast_to(ref[pl.ds(row, 1), :], (8, LANES))


def scan_group(dts, us, rate, group, state, drive, readout, out):
    def step(t, carry):
        row = pl.multiple_of(t * PITCH + group * 8, 8)
        steps = dts[pl.ds(row, 8), :]
        flow = us[pl.ds(row, 8), :]
        entries = []
        total = None
        for n in range(STATE):
            decay = jnp.exp2(steps * rate[n])
            entry = decay * carry[n] + flow * drive(t, n)
            entries.append(entry)
            if readout is not None:
                term = readout(t, n) * entry
                total = term if total is None else total + term
        if readout is not None:
            out[pl.ds(row, 8), :] = total
        return tuple(entries)

    return lax.fori_loop(0, ROWS, step, state, unroll=UNROLL)


def splat_reader(ref, base):
    return lambda t, n: row_of(ref, base + t * SPLAT + n)


def mixed_reader(ref):
    first = lax.broadcasted_iota(jnp.int32, (8, LANES), 0) < 2

    def read(t, n):
        return jnp.where(
            first,
            row_of(ref, CLEAN * ROWS * SPLAT + t * SPLAT + n),
            row_of(ref, CORRUPT * ROWS * SPLAT + t * SPLAT + n),
        )

    return read


def wait_for(ref, sem):
    pltpu.make_async_copy(ref, ref, sem).wait()


def front_kernel(
    pos, mode, clean_in, corrupt_in, conv_w_in, conv_b_in, x_w_in, dt_w_in, dt_b_in, a_log_in,
    acts, x_w, dt_w, dt_b, rates,
    rims, a_log, ends, wide, packed, clean, corrupt, conv_w, conv_b, pad, load_sem, send_sem, recv_sem,
):
    me = lax.axis_index("seq")
    v = lax.axis_index("var")
    after = lax.min(me + 1, SHARDS - 1)
    has_next, has_last = me < SHARDS - 1, me > 0
    barrier = pltpu.get_barrier_semaphore()
    loads = [
        pltpu.make_async_copy(src, dst, load_sem.at[i])
        for i, (src, dst) in enumerate(
            (
                (clean_in.at[ROWS - 8 :, :INNER], ends.at[0]),
                (corrupt_in.at[ROWS - 8 :, :INNER], ends.at[1]),
                (clean_in.at[:, :INNER], clean), (corrupt_in.at[:, :INNER], corrupt),
                (conv_w_in, conv_w), (conv_b_in, conv_b), (x_w_in, x_w), (dt_w_in, dt_w),
                (dt_b_in, dt_b), (a_log_in, a_log),
            )
        )
    ]
    for load in loads:
        load.start()

    def signal(peer):
        pl.semaphore_signal(barrier, inc=1, device_id=(peer, v), device_id_type=MESH)

    @pl.when(has_next)
    def _():
        signal(me + 1)

    @pl.when(has_last)
    def _():
        signal(me - 1)

    for load in loads[:2]:
        load.wait()
    margin = TAPS - 1
    wide[...] = jnp.zeros_like(wide)
    for i in range(2):
        wide[i * margin : (i + 1) * margin, :] = ends[i].astype(F32)[8 - margin :, :]
    packed[...] = wide[...].astype(BF16)
    first = me * ROWS
    take = hit_rows(pos, first, ROWS)[:, :1] & (mode[0] != 1)
    take_rim = hit_rows(pos, first - margin, margin)[:, :1] & (mode[0] != 1)
    pl.semaphore_wait(barrier, lax.min(me, 1) + lax.min(SHARDS - 1 - me, 1))
    copy = pltpu.make_async_remote_copy(
        src_ref=packed, dst_ref=rims, send_sem=send_sem, recv_sem=recv_sem,
        device_id=(after, v), device_id_type=MESH,
    )

    @pl.when(has_next)
    def _():
        copy.start()

    for load in loads[2:6]:
        load.wait()
    width = 512
    span = 8 + ROWS
    per = width // LANES

    def columns(i):
        return pl.ds(pl.multiple_of(i * width, width), width)

    def fill(i, _):
        sig_clean = clean[:, columns(i)].astype(F32)
        sig_corrupt = corrupt[:, columns(i)].astype(F32)
        pieces = (sig_clean, sig_corrupt, jnp.where(take, sig_clean, sig_corrupt))
        for run, sig in enumerate(pieces):
            for k in range(per):
                at = pl.multiple_of((run * TILES + i * per + k) * span, 8)
                pad[pl.ds(at, 8), :] = jnp.zeros((8, LANES), F32)
                pad[pl.ds(at + 8, ROWS), :] = sig[:, k * LANES : (k + 1) * LANES]
        return 0

    def convolve(rows):
        def body(tile, _):
            cols = pl.ds(pl.multiple_of(tile * LANES, LANES), LANES)
            bias = conv_b[:, cols]
            for run in range(3):
                at = (run * TILES + tile) * span + 8 - margin
                total = bias + conv_w[0:1, cols] * pad[pl.ds(at, rows), :]
                for k in range(1, TAPS):
                    total = total + conv_w[k : k + 1, cols] * pad[pl.ds(at + k, rows), :]
                acts[run * ROWS : run * ROWS + rows, cols] = silu(total).astype(BF16)
            return 0

        lax.fori_loop(0, TILES, body, 0, unroll=4 if rows == ROWS else 10)

    def fill_rim(i, _):
        rim = rims[:, columns(i)].astype(F32)
        rim_clean, rim_corrupt = rim[:margin], rim[margin : 2 * margin]
        pieces = (rim_clean, rim_corrupt, jnp.where(take_rim, rim_clean, rim_corrupt))
        for run, part in enumerate(pieces):
            for k in range(per):
                at = (run * TILES + i * per + k) * span + 8 - margin
                pad[pl.ds(at, margin), :] = part[:, k * LANES : (k + 1) * LANES]
        return 0

    lax.fori_loop(0, INNER // width, fill, 0)
    convolve(ROWS)
    for load in loads[6:]:
        load.wait()

    def rate_of(slot, cols):
        rates[rate_at(slot), :] = jnp.exp(a_log[:, cols]) * (-LOG2E)

    def patched_rate(tile, _):
        rate_of(tile, pl.ds(pl.multiple_of(tile * LANES, LANES), LANES))
        return 0

    lax.fori_loop(0, TILES, patched_rate, 0, unroll=4)
    for tile in range(CUT_TILES):
        for run in (CLEAN, CORRUPT):
            cols = pl.ds(pl.multiple_of(v * SPAN + tile * LANES, LANES), LANES)
            rate_of(cut_slot(run, tile), cols)
    for slot in range(60, CHUNKS):
        rates[rate_at(slot), :] = jnp.zeros((STATE, LANES), F32)

    @pl.when(has_last)
    def _():
        copy.wait_recv()
        lax.fori_loop(0, INNER // width, fill_rim, 0, unroll=5)
        convolve(8)

    @pl.when(has_next)
    def _():
        copy.wait_send()


def emit_kernel(patched, effect, patched_out, effect_out, sems):
    copies = [
        pltpu.make_async_copy(patched, patched_out, sems.at[0]),
        pltpu.make_async_copy(effect, effect_out, sems.at[1]),
    ]
    for copy in copies:
        copy.start()
    for copy in copies:
        copy.wait()


def kernel(
    pos, mode, acts, x_w, dt_w, dt_b, rates, clean_in, corrupt_in, d_skip_in,
    patched, effect,
    clean_gate, corrupt_gate, d_skip, low, maps, weights, base, gates, dts, us, bs, cs, ends, totals,
    pair_ends, pair_totals, chip_ends, got_ends,
    leaving, landed, across, start, ys,
    cut, squares, whole, peaks, squares_z, line_squares, squares_x, spreads,
    peaks_z, line_peaks, peaks_x, pair_squares, chip_squares, pair_peaks, chip_peaks, sent_peaks, answer,
    load_sem, send_pt, recv_pt, send_pe, recv_pe, send_ce, recv_ce,
    send_in, recv_in, send_st, recv_st,
    send_cut, recv_cut, send_sz, recv_sz, send_sx, recv_sx, send_sp, recv_sp,
    send_pz, recv_pz, send_px, recv_px, send_qq, recv_qq, send_pp, recv_pp, send_an, recv_an,
):
    me = lax.axis_index("seq")
    v = lax.axis_index("var")
    chip = lax.div(me, 2)
    core = lax.rem(me, 2)
    mate = me + 1 - 2 * core
    mine = core * HALF
    theirs = HALF - mine
    barrier = pltpu.get_barrier_semaphore()

    loads = [
        pltpu.make_async_copy(src, dst, load_sem.at[i])
        for i, (src, dst) in enumerate(
            (
                (d_skip_in, d_skip), (clean_in.at[:, INNER:], clean_gate),
                (corrupt_in.at[:, INNER:], corrupt_gate),
            )
        )
    ]
    for load in loads:
        load.start()

    def signal(peer, variant):
        pl.semaphore_signal(barrier, inc=1, device_id=(peer, variant), device_id_type=MESH)

    row_x, line_z = lax.div(chip, 8), lax.rem(chip, 8)
    peers = [8 * lax.rem(row_x + dx, 4) + lax.rem(line_z + dz, 8) for dx, dz in STEPS]
    for peer in peers:
        signal(2 * peer + core, v)
    signal(mate, v)
    for k in range(1, VARS):
        signal(me, lax.rem(v + k, VARS))

    def to_variant(k, src, dst, send_sem, recv_sem):
        return pltpu.make_async_remote_copy(
            src_ref=src, dst_ref=dst, send_sem=send_sem, recv_sem=recv_sem,
            device_id=(me, lax.rem(v + k, VARS)), device_id_type=MESH,
        )

    def to_shard(peer, src, dst, send_sem, recv_sem):
        return pltpu.make_async_remote_copy(
            src_ref=src, dst_ref=dst, send_sem=send_sem, recv_sem=recv_sem,
            device_id=(peer, v), device_id_type=MESH,
        )

    take_gate = hit_rows(pos, me * ROWS, ROWS)[:, :1] & (mode[0] != 0)

    projected = lax.dot_general(
        acts[...], x_w[...], (((1,), (1,)), ((), ())), preferred_element_type=F32
    )
    low[...] = projected[:, :RANK].astype(BF16)
    maps[...] = projected[:, RANK + STATE :]
    for run in range(3):
        part = projected[run * ROWS : (run + 1) * ROWS]
        for n in range(STATE):
            at = run * ROWS * SPLAT + n
            bs[pl.ds(at, ROWS, stride=SPLAT), :] = jnp.broadcast_to(
                part[:, RANK + n : RANK + n + 1], (ROWS, LANES)
            )


    def place(slot, steps, act):
        dts[pl.ds(slot, ROWS, stride=PITCH), :] = steps
        us[pl.ds(slot, ROWS, stride=PITCH), :] = steps * act
        totals[slot] = jnp.sum(steps, axis=0, keepdims=True)

    wide = 5120

    def patched_steps(i, _):
        cols = pl.ds(pl.multiple_of(i * wide, wide), wide)
        raw = jnp.dot(low[2 * ROWS :, :], dt_w[:, cols], preferred_element_type=F32)
        steps = softplus(raw + dt_b[:, cols])
        act = acts[2 * ROWS :, cols].astype(F32)
        for k in range(wide // LANES):
            part = slice(k * LANES, (k + 1) * LANES)
            place(i * (wide // LANES) + k, steps[:, part], act[:, part])
        return 0

    lax.fori_loop(0, INNER // wide, patched_steps, 0)

    cols = pl.ds(pl.multiple_of(v * SPAN, LANES), SPAN)
    raw = jnp.dot(low[: 2 * ROWS, :], dt_w[:, cols], preferred_element_type=F32)
    steps = softplus(raw + dt_b[:, cols])
    act = acts[: 2 * ROWS, cols].astype(F32)
    for run in (CLEAN, CORRUPT):
        rows = slice(run * ROWS, (run + 1) * ROWS)
        for tile in range(CUT_TILES):
            part = slice(tile * LANES, (tile + 1) * LANES)
            place(cut_slot(run, tile), steps[rows, part], act[rows, part])
    blank = jnp.zeros((ROWS, LANES), F32)
    for slot in range(60, CHUNKS):
        place(slot, blank, blank)

    zero = jnp.zeros((8, LANES), F32)

    def rates_of(group):
        base = group * (STATE * 8)
        return [rates[pl.ds(pl.multiple_of(base + n * 8, 8), 8), :] for n in range(STATE)]

    def run_base(group):
        return jnp.where(group < 5, PATCHED, group - 5) * (ROWS * SPLAT)

    def local_group(group, drive):
        found = scan_group(
            dts, us, rates_of(group), group, (zero,) * STATE, drive, None, None
        )
        for n in range(STATE):
            ends[pl.ds(group * (STATE * 8) + n, 8, stride=STATE), :] = found[n]

    def local_pass(offset):
        def body(i, _):
            group = offset + i

            @pl.when(group < GROUPS - 1)
            def _():
                local_group(group, splat_reader(bs, run_base(group)))

            @pl.when(group == GROUPS - 1)
            def _():
                local_group(group, mixed_reader(bs))

            return 0

        lax.fori_loop(0, GROUPS // 2, body, 0)

    local_pass(lax.div(theirs, 8))
    pl.semaphore_wait(barrier, CHIPS - 1 + 1 + VARS - 1)
    theirs_3 = pl.ds(theirs, HALF)
    swap_totals = to_shard(mate, totals.at[theirs_3], pair_totals, send_pt, recv_pt)
    swap_totals.start()

    theirs_2 = pl.ds(pl.multiple_of(theirs * STATE, 8), HALF * STATE)
    swap_ends = to_shard(mate, ends.at[theirs_2], pair_ends, send_pe, recv_pe)
    swap_ends.start()
    local_pass(lax.div(mine, 8))
    swap_totals.wait_recv()

    leads = core == 0

    def my_summary(k):
        own = ends[pl.ds(pl.multiple_of((mine + k) * STATE, 8), STATE), :]
        return own, totals[mine + k]

    def pair_of(k):
        own_end, own_total = my_summary(k)
        other_end = pair_ends[pl.ds(pl.multiple_of(k * STATE, 8), STATE), :]
        other_total = pair_totals[k]
        return (
            jnp.where(leads, own_end, other_end), jnp.where(leads, own_total, other_total),
            jnp.where(leads, other_end, own_end), jnp.where(leads, other_total, own_total),
        )

    swap_ends.wait_recv()

    def chip_end(k, _):
        end_a, total_a, end_b, total_b = pair_of(k)
        chip_ends[k, :STATE] = jnp.exp2(rates[rate_at(mine + k), :] * total_b) * end_a + end_b
        chip_ends[k, STATE:] = total_a + total_b
        return 0

    lax.fori_loop(0, HALF, chip_end, 0, unroll=8)
    owns = (core == 0) | (chip < BUSY)
    others = pl.ds(0, CHIPS - 1)

    @pl.when(owns)
    def _():
        pltpu.make_async_copy(chip_ends.at[chip], got_ends.at[chip], recv_ce).start()

    for peer in peers:
        @pl.when((core == 0) | (peer < BUSY))
        def _():
            target = 2 * peer + core
            to_shard(target, chip_ends.at[peer], got_ends.at[chip], send_ce, recv_ce).start()

    my_rate = rates[rate_at(mine + chip), :]
    for run in range(3):
        for n in range(STATE):
            cs[pl.ds(run * ROWS * SPLAT + n, ROWS, stride=SPLAT), :] = jnp.broadcast_to(
                maps[run * ROWS : (run + 1) * ROWS, n : n + 1], (ROWS, LANES)
            )

    def local_readout(group, drive, read):
        scan_group(dts, us, rates_of(group), group, (zero,) * STATE, drive, read, ys)

    def plain_readout(group, _):
        at = run_base(group)
        local_readout(group, splat_reader(bs, at), splat_reader(cs, at))
        return 0

    lax.fori_loop(0, GROUPS - 1, plain_readout, 0)
    local_readout(GROUPS - 1, mixed_reader(bs), mixed_reader(cs))
    def chain(s, state):
        leaving[s] = state
        return jnp.exp2(my_rate * got_ends[s, STATE:]) * state + got_ends[s, :STATE]

    @pl.when(owns)
    def _():
        wait_for(got_ends, recv_ce)
        lax.fori_loop(0, CHIPS, chain, jnp.zeros((STATE, LANES), F32), unroll=4)
        pltpu.make_async_copy(leaving.at[chip], landed.at[chip], recv_in).start()
        for peer in peers:
            to_shard(2 * peer + core, leaving.at[peer], landed.at[chip], send_in, recv_in).start()

    def entry_weights(group, read):
        rate = rates_of(group)

        def step(t, run_total):
            row = pl.multiple_of(t * PITCH + group * 8, 8)
            run_total = run_total + dts[pl.ds(row, 8), :]
            at = (group * ROWS + t) * (STATE * 8)
            for n in range(STATE):
                weights[pl.ds(pl.multiple_of(at + n * 8, 8), 8), :] = read(t, n) * jnp.exp2(
                    run_total * rate[n]
                )
            return run_total

        lax.fori_loop(0, ROWS, step, zero, unroll=4)

    def plain_weights(group, _):
        entry_weights(group, splat_reader(cs, run_base(group)))
        return 0

    lax.fori_loop(0, GROUPS - 1, plain_weights, 0)
    entry_weights(GROUPS - 1, mixed_reader(cs))
    for load in loads:
        load.wait()

    def prepare(slot, act, skip, gate):
        rows = pl.ds(pl.multiple_of(slot * ROWS, 8), ROWS)
        base[rows, :] = ys[pl.ds(slot, ROWS, stride=PITCH), :] + skip * act
        gates[rows, :] = silu(gate)

    for run, gate_rows in ((CLEAN, clean_gate), (CORRUPT, corrupt_gate)):
        for tile in range(CUT_TILES):
            cols = pl.ds(pl.multiple_of(v * SPAN + tile * LANES, LANES), LANES)
            act = acts[run * ROWS : (run + 1) * ROWS, cols].astype(F32)
            prepare(cut_slot(run, tile), act, d_skip[:, cols], gate_rows[:, cols].astype(F32))

    def prepare_patched(tile, _):
        cols = pl.ds(pl.multiple_of(tile * LANES, LANES), LANES)
        gate = jnp.where(
            take_gate, clean_gate[:, cols].astype(F32), corrupt_gate[:, cols].astype(F32)
        )
        prepare(tile, acts[2 * ROWS :, cols].astype(F32), d_skip[:, cols], gate)
        return 0

    lax.fori_loop(0, TILES, prepare_patched, 0, unroll=2)
    def enter(k, _):
        end_a, total_a, _, _ = pair_of(k)
        before = landed[k]
        after = jnp.exp2(rates[rate_at(mine + k), :] * total_a) * before + end_a
        at = pl.ds(pl.multiple_of((mine + k) * STATE, 8), STATE)
        start[at, :] = jnp.where(leads, before, after)
        across[pl.ds(pl.multiple_of(k * STATE, 8), STATE), :] = jnp.where(leads, after, before)
        return 0

    swap_start = to_shard(
        mate, across, start.at[pl.ds(pl.multiple_of(mine * STATE, 8), HALF * STATE)],
        send_st, recv_st,
    )

    def enter_half(sources):
        wait_for(landed.at[pl.ds(0, sources)], recv_in)
        lax.fori_loop(0, HALF, enter, 0, unroll=8)
        swap_start.start()

    @pl.when(core == 1)
    def _():
        enter_half(BUSY)

    @pl.when(core == 0)
    def _():
        swap_start.wait_recv()

    def final_group(group, _):
        at = group * (STATE * 8)
        state = [start[pl.ds(at + n, 8, stride=STATE), :] for n in range(STATE)]

        def step(t, _):
            at = (group * ROWS + t) * (STATE * 8)
            total = None
            for n in range(STATE):
                term = weights[pl.ds(pl.multiple_of(at + n * 8, 8), 8), :] * state[n]
                total = term if total is None else total + term
            ys[pl.ds(pl.multiple_of(t * PITCH + group * 8, 8), 8), :] = total
            return 0

        lax.fori_loop(0, ROWS, step, 0, unroll=8)
        return 0

    def result(slot):
        rows = pl.ds(pl.multiple_of(slot * ROWS, 8), ROWS)
        y = ys[pl.ds(slot, ROWS, stride=PITCH), :]
        return ((y + base[rows, :]) * gates[rows, :]).astype(BF16)

    lax.fori_loop(6, GROUPS, final_group, 0)

    for tile in range(CUT_TILES):
        cut[:, tile * LANES : (tile + 1) * LANES] = result(cut_slot(CORRUPT, tile))
    directs = [
        to_variant(k, cut, whole.at[v], send_cut.at[k], recv_cut.at[k]) for k in (2, 1, VARS - 1)
    ]
    for direct in directs:
        direct.start()
    @pl.when(core == 0)
    def _():
        enter_half(CHIPS)

    @pl.when(core == 1)
    def _():
        swap_start.wait_recv()

    final_group(5, 0)
    squares[...] = jnp.zeros_like(squares)
    for tile in range(CUT_TILES):
        gap = result(cut_slot(CLEAN, tile)).astype(F32)
        gap = gap - cut[:, tile * LANES : (tile + 1) * LANES].astype(F32)
        squares[tile : tile + 1, :] = jnp.sum(gap * gap, axis=0, keepdims=True)

    def along_z(k):
        return 16 * row_x + 2 * lax.rem(line_z + k, 8) + 1

    def along_x(k):
        return 16 * lax.rem(row_x + k, 4) + 2 * line_z + 1

    def share(peer_of, count, slot, src, dst, send_sem, recv_sem):
        for k in sorted(range(1, count), key=lambda k: -min(k, count - k)):
            to_shard(peer_of(k), src, dst.at[slot], send_sem, recv_sem).start()
        dst[slot] = src[...]

    seven, three = pl.ds(0, 7), pl.ds(0, 3)
    squares_over = to_shard(mate, squares, pair_squares, send_qq, recv_qq)

    @pl.when(core == 0)
    def _():
        squares_over.start()

    whole[v] = cut[...]

    lax.fori_loop(0, 5, final_group, 0)
    def patched_tile(tile, _):
        cols = pl.ds(pl.multiple_of(tile * LANES, LANES), LANES)
        patched[:, cols] = result(tile)
        return 0

    lax.fori_loop(0, TILES, patched_tile, 0, unroll=4)


    @pl.when(core == 1)
    def _():
        squares_over.wait_recv()
        chip_squares[...] = squares[...] + pair_squares[...]
        share(along_z, 8, line_z, chip_squares, squares_z, send_sz, recv_sz)

    for direct in directs:
        direct.wait_recv()

    for w in range(VARS):
        def peak_tile(i, _):
            here = pl.ds(pl.multiple_of(i * LANES, LANES), LANES)
            there = pl.ds(pl.multiple_of(w * SPAN + i * LANES, LANES), LANES)
            gap = jnp.abs(patched[:, there].astype(F32) - whole[w, :, here].astype(F32))
            peaks[pl.ds(w * CUT_TILES + i, 1), :] = jnp.max(gap, axis=0, keepdims=True)
            return 0

        lax.fori_loop(0, CUT_TILES, peak_tile, 0, unroll=2)

    sent_peaks[...] = peaks[...].astype(BF16)
    peaks_over = to_shard(mate, sent_peaks, pair_peaks, send_pp, recv_pp)
    answer_over = to_shard(mate, answer, answer, send_an, recv_an)

    @pl.when(core == 0)
    def _():
        peaks_over.start()

    @pl.when(core == 1)
    def _():
        wait_for(squares_z.at[seven], recv_sz)
        line_squares[...] = jnp.sum(squares_z[...], axis=0)
        share(along_x, 4, row_x, line_squares, squares_x, send_sx, recv_sx)
        peaks_over.wait_recv()
        both = jnp.maximum(sent_peaks[...].astype(F32), pair_peaks[...].astype(F32))
        chip_peaks[...] = both.astype(BF16)
        share(along_z, 8, line_z, chip_peaks, peaks_z, send_pz, recv_pz)
        wait_for(squares_x.at[three], recv_sx)
        spreads[v] = jnp.sqrt(jnp.sum(squares_x[...], axis=0) / (SHARDS * ROWS) + TINY)
        for k in range(1, VARS):
            to_variant(k, spreads.at[v], spreads.at[v], send_sp.at[k], recv_sp.at[k]).start()
        wait_for(peaks_z.at[seven], recv_pz)
        line_peaks[...] = jnp.max(peaks_z[...].astype(F32), axis=0).astype(BF16)
        share(along_x, 4, row_x, line_peaks, peaks_x, send_px, recv_px)
        wait_for(peaks_x.at[three], recv_px)
        for k in range(1, VARS):
            there = spreads.at[lax.rem(v + VARS - k, VARS)]
            to_variant(k, there, there, send_sp.at[k], recv_sp.at[k]).wait()
        peak = jnp.max(peaks_x[...].astype(F32), axis=0)
        for w in range(VARS):
            rows = slice(w * CUT_TILES, (w + 1) * CUT_TILES)
            answer[rows, :] = peak[rows, :] / spreads[w, :CUT_TILES, :]
        answer_over.start()
        wait_for(squares_z.at[seven], send_sz)
        wait_for(squares_x.at[three], send_sx)
        wait_for(peaks_z.at[seven], send_pz)
        wait_for(peaks_x.at[three], send_px)
        answer_over.wait_send()

    @pl.when(core == 0)
    def _():
        squares_over.wait_send()
        peaks_over.wait_send()
        answer_over.wait_recv()

    effect[...] = answer[...]
    @pl.when(core == 0)
    def _():
        wait_for(chip_ends.at[others], send_ce)

    @pl.when((core == 1) & (chip < BUSY))
    def _():
        wait_for(chip_ends.at[pl.ds(0, BUSY - 1)], send_ce)

    @pl.when((core == 1) & (chip >= BUSY))
    def _():
        wait_for(chip_ends.at[pl.ds(0, BUSY)], send_ce)

    @pl.when(owns)
    def _():
        wait_for(leaving.at[others], send_in)

    swap_start.wait_send()
    for sent in (swap_ends, swap_totals, *directs):
        sent.wait_send()


SMEM = pl.BlockSpec(memory_space=pltpu.SMEM)
HBM = pl.BlockSpec(memory_space=pltpu.HBM)
VMEM = pl.BlockSpec(memory_space=pltpu.VMEM)
DMA = pltpu.SemaphoreType.DMA


def shards(
    clean_proj, corrupt_proj, patch_pos, patch_mode, a_log, dt_bias,
    conv_weight, conv_bias, x_weight, dt_weight, d_skip,
):
    hold = functools.partial(pltpu.with_memory_space_constraint, memory_space=pltpu.HBM)
    keep = functools.partial(pltpu.with_memory_space_constraint, memory_space=pltpu.VMEM)
    front = pl.pallas_call(
        front_kernel,
        out_shape=(
            pltpu.VMEM((3 * ROWS, INNER), BF16),
            pltpu.VMEM((RANK + 2 * STATE, INNER), BF16),
            pltpu.VMEM((RANK, INNER), BF16),
            pltpu.VMEM((1, INNER), F32),
            pltpu.VMEM((CHUNKS * STATE, LANES), F32),
        ),
        in_specs=[SMEM, SMEM] + [HBM] * 8,
        out_specs=(VMEM,) * 5,
        scratch_shapes=[
            pltpu.VMEM((8, INNER), BF16),
            pltpu.VMEM((STATE, INNER), F32),
            pltpu.VMEM((2, 8, INNER), BF16),
            pltpu.VMEM((8, INNER), F32),
            pltpu.VMEM((8, INNER), BF16),
            pltpu.VMEM((ROWS, INNER), BF16),
            pltpu.VMEM((ROWS, INNER), BF16),
            pltpu.VMEM((TAPS, INNER), F32),
            pltpu.VMEM((1, INNER), F32),
            pltpu.VMEM((3 * TILES * (8 + ROWS), LANES), F32),
            DMA((10,)),
            DMA,
            DMA,
        ],
        compiler_params=pltpu.CompilerParams(
            collective_id=1, has_side_effects=True, vmem_limit_bytes=40_000_000
        ),
        name="front",
    )(
        hold(patch_pos), patch_mode,
        *map(
            hold,
            (
                clean_proj, corrupt_proj, conv_weight, conv_bias[None], x_weight.T, dt_weight,
                dt_bias[None], a_log,
            ),
        ),
    )
    row = (1, LANES)
    tile = (STATE, LANES)
    patched, effect = pl.pallas_call(
        kernel,
        out_shape=(pltpu.VMEM((ROWS, INNER), BF16), pltpu.VMEM((TILES, LANES), F32)),
        in_specs=[SMEM, SMEM] + [VMEM] * 5 + [HBM] * 3,
        out_specs=(VMEM, VMEM),
        scratch_shapes=[
            pltpu.VMEM((ROWS, INNER), BF16),
            pltpu.VMEM((ROWS, INNER), BF16),
            pltpu.VMEM((1, INNER), F32),
            pltpu.VMEM((3 * ROWS, RANK), BF16),
            pltpu.VMEM((3 * ROWS, STATE), F32),
            pltpu.VMEM((GROUPS * ROWS * STATE * 8, LANES), F32),
            pltpu.VMEM((CHUNKS * ROWS, LANES), F32),
            pltpu.VMEM((CHUNKS * ROWS, LANES), F32),
            pltpu.VMEM((ROWS * PITCH, LANES), F32),
            pltpu.VMEM((ROWS * PITCH, LANES), F32),
            pltpu.VMEM((3 * ROWS * SPLAT + 8, LANES), F32),
            pltpu.VMEM((3 * ROWS * SPLAT + 8, LANES), F32),
            pltpu.VMEM((CHUNKS * STATE, LANES), F32),
            pltpu.VMEM((CHUNKS, *row), F32),
            pltpu.VMEM((HALF * STATE, LANES), F32),
            pltpu.VMEM((HALF, *row), F32),
            pltpu.VMEM((HALF, STATE + 1, LANES), F32),
            pltpu.VMEM((CHIPS, STATE + 1, LANES), F32),
            pltpu.VMEM((CHIPS, *tile), F32),
            pltpu.VMEM((HALF, *tile), F32),
            pltpu.VMEM((HALF * STATE, LANES), F32),
            pltpu.VMEM((CHUNKS * STATE, LANES), F32),
            pltpu.VMEM((ROWS * PITCH, LANES), F32),
            pltpu.VMEM((ROWS, SPAN), BF16),
            pltpu.VMEM((STATE, LANES), F32),
            pltpu.VMEM((VARS, ROWS, SPAN), BF16),
            pltpu.VMEM((TILES, LANES), F32),
            pltpu.VMEM((8, STATE, LANES), F32),
            pltpu.VMEM((STATE, LANES), F32),
            pltpu.VMEM((4, STATE, LANES), F32),
            pltpu.VMEM((VARS, STATE, LANES), F32),
            pltpu.VMEM((8, TILES, LANES), BF16),
            pltpu.VMEM((TILES, LANES), BF16),
            pltpu.VMEM((4, TILES, LANES), BF16),
            pltpu.VMEM((STATE, LANES), F32),
            pltpu.VMEM((STATE, LANES), F32),
            pltpu.VMEM((TILES, LANES), BF16),
            pltpu.VMEM((TILES, LANES), BF16),
            pltpu.VMEM((TILES, LANES), BF16),
            pltpu.VMEM((TILES, LANES), F32),
            DMA((3,)),
        ]
        + [DMA] * 10
        + [DMA((VARS,)), DMA((VARS,))]
        + [DMA] * 4
        + [DMA((VARS,)), DMA((VARS,))]
        + [DMA] * 10,
        compiler_params=pltpu.CompilerParams(
            collective_id=0, has_side_effects=True, vmem_limit_bytes=54_000_000
        ),
        name="mixer",
    )(
        hold(patch_pos), patch_mode, *map(keep, front),
        *map(hold, (clean_proj, corrupt_proj, d_skip[None])),
    )
    patched, effect = pl.pallas_call(
        emit_kernel,
        out_shape=(
            jax.ShapeDtypeStruct((ROWS, INNER), BF16),
            jax.ShapeDtypeStruct((TILES, LANES), F32),
        ),
        in_specs=[VMEM, VMEM],
        out_specs=(HBM, HBM),
        scratch_shapes=[DMA((2,))],
        compiler_params=pltpu.CompilerParams(vmem_limit_bytes=16_000_000),
        name="emit",
    )(
        keep(patched), keep(effect),
    )
    return (patched[None], effect.reshape(1, INNER))


def solution(mesh):
    return jax.shard_map(
        shards,
        mesh=mesh,
        in_specs=(
            P("seq", None), P("seq", None), P("var", None), P("var"),
            P(), P(), P(), P(), P(), P(), P(),
        ),
        out_specs=(P("var", "seq", None), P("var", None)),
        check_vma=False,
    )
```

```python
import functools

import jax
import jax.numpy as jnp
from jax import lax
from jax.experimental import pallas as pl
from jax.experimental.pallas import tpu as pltpu
from jax.sharding import PartitionSpec as P

STATE = 16
RANK = 160
ROWS = 32
INNER = 5120
SPAN = 1280
TAPS = 4
LANES = 128
CHUNKS = 64
SHARDS = 64
VARS = 4
TILES = INNER // LANES
CUT_TILES = SPAN // LANES
GROUPS = CHUNKS // 8
BUSY = 28
HALF = CHUNKS // 2
CHIPS = SHARDS // 2
PITCH = 72
SPLAT = 17
MESH = pl.DeviceIdType.MESH
LOG2E = 1.4426950408889634
TINY = 1e-06
F32 = jnp.float32
BF16 = jnp.bfloat16
UNROLL = 16
CLEAN, CORRUPT, PATCHED = 0, 1, 2
STEPS = sorted(
    ((dx, dz) for dx in range(4) for dz in range(8) if dx or dz),
    key=lambda step: -(min(step[0], 4 - step[0]) + min(step[1], 8 - step[1])),
)


def cut_slot(run, tile):
    if tile < 8:
        return TILES + 8 * run + tile
    return 56 + 2 * run + (tile - 8)


def rate_at(slot):
    return pl.ds(lax.div(slot, 8) * (STATE * 8) + lax.rem(slot, 8), STATE, stride=8)


def hit_rows(pos_ref, first, count):
    rows = first + lax.broadcasted_iota(jnp.int32, (count, LANES), 0)
    hits = rows == pos_ref[0, 0]
    for k in range(1, pos_ref.shape[1]):
        hits = hits | (rows == pos_ref[0, k])
    return hits


def silu(value):
    return value / (1.0 + jnp.exp(-value))


def softplus(value):
    return jnp.maximum(value, 0.0) + jnp.log1p(jnp.exp(-jnp.abs(value)))


def row_of(ref, row):
    return jnp.broadcast_to(ref[pl.ds(row, 1), :], (8, LANES))


def scan_group(dts, us, rate, group, state, drive, readout, out):
    def step(t, carry):
        row = pl.multiple_of(t * PITCH + group * 8, 8)
        steps = dts[pl.ds(row, 8), :]
        flow = us[pl.ds(row, 8), :]
        entries = []
        total = None
        for n in range(STATE):
            decay = jnp.exp2(steps * rate[n])
            entry = decay * carry[n] + flow * drive(t, n)
            entries.append(entry)
            if readout is not None:
                term = readout(t, n) * entry
                total = term if total is None else total + term
        if readout is not None:
            out[pl.ds(row, 8), :] = total
        return tuple(entries)

    return lax.fori_loop(0, ROWS, step, state, unroll=UNROLL)


def splat_reader(ref, base):
    return lambda t, n: row_of(ref, base + t * SPLAT + n)


def mixed_reader(ref):
    first = lax.broadcasted_iota(jnp.int32, (8, LANES), 0) < 2

    def read(t, n):
        return jnp.where(
            first,
            row_of(ref, CLEAN * ROWS * SPLAT + t * SPLAT + n),
            row_of(ref, CORRUPT * ROWS * SPLAT + t * SPLAT + n),
        )

    return read


def wait_for(ref, sem):
    pltpu.make_async_copy(ref, ref, sem).wait()


def front_kernel(
    pos, mode, clean_in, corrupt_in, conv_w_in, conv_b_in, x_w_in, dt_w_in, dt_b_in, a_log_in,
    acts, x_w, dt_w, dt_b, rates,
    rims, a_log, ends, wide, packed, clean, corrupt, conv_w, conv_b, pad, load_sem, send_sem, recv_sem,
):
    me = lax.axis_index("seq")
    v = lax.axis_index("var")
    after = lax.min(me + 1, SHARDS - 1)
    has_next, has_last = me < SHARDS - 1, me > 0
    barrier = pltpu.get_barrier_semaphore()
    loads = [
        pltpu.make_async_copy(src, dst, load_sem.at[i])
        for i, (src, dst) in enumerate(
            (
                (clean_in.at[ROWS - 8 :, :INNER], ends.at[0]),
                (corrupt_in.at[ROWS - 8 :, :INNER], ends.at[1]),
                (clean_in.at[:, :INNER], clean), (corrupt_in.at[:, :INNER], corrupt),
                (conv_w_in, conv_w), (conv_b_in, conv_b), (x_w_in, x_w), (dt_w_in, dt_w),
                (dt_b_in, dt_b), (a_log_in, a_log),
            )
        )
    ]
    for load in loads:
        load.start()

    def signal(peer):
        pl.semaphore_signal(barrier, inc=1, device_id=(peer, v), device_id_type=MESH)

    @pl.when(has_next)
    def _():
        signal(me + 1)

    @pl.when(has_last)
    def _():
        signal(me - 1)

    for load in loads[:2]:
        load.wait()
    margin = TAPS - 1
    wide[...] = jnp.zeros_like(wide)
    for i in range(2):
        wide[i * margin : (i + 1) * margin, :] = ends[i].astype(F32)[8 - margin :, :]
    packed[...] = wide[...].astype(BF16)
    first = me * ROWS
    take = hit_rows(pos, first, ROWS)[:, :1] & (mode[0] != 1)
    take_rim = hit_rows(pos, first - margin, margin)[:, :1] & (mode[0] != 1)
    pl.semaphore_wait(barrier, lax.min(me, 1) + lax.min(SHARDS - 1 - me, 1))
    copy = pltpu.make_async_remote_copy(
        src_ref=packed, dst_ref=rims, send_sem=send_sem, recv_sem=recv_sem,
        device_id=(after, v), device_id_type=MESH,
    )

    @pl.when(has_next)
    def _():
        copy.start()

    for load in loads[2:6]:
        load.wait()
    width = 512
    span = 8 + ROWS
    per = width // LANES

    def columns(i):
        return pl.ds(pl.multiple_of(i * width, width), width)

    def fill(i, _):
        sig_clean = clean[:, columns(i)].astype(F32)
        sig_corrupt = corrupt[:, columns(i)].astype(F32)
        pieces = (sig_clean, sig_corrupt, jnp.where(take, sig_clean, sig_corrupt))
        for run, sig in enumerate(pieces):
            for k in range(per):
                at = pl.multiple_of((run * TILES + i * per + k) * span, 8)
                pad[pl.ds(at, 8), :] = jnp.zeros((8, LANES), F32)
                pad[pl.ds(at + 8, ROWS), :] = sig[:, k * LANES : (k + 1) * LANES]
        return 0

    def convolve(rows):
        def body(tile, _):
            cols = pl.ds(pl.multiple_of(tile * LANES, LANES), LANES)
            bias = conv_b[:, cols]
            for run in range(3):
                at = (run * TILES + tile) * span + 8 - margin
                total = bias + conv_w[0:1, cols] * pad[pl.ds(at, rows), :]
                for k in range(1, TAPS):
                    total = total + conv_w[k : k + 1, cols] * pad[pl.ds(at + k, rows), :]
                acts[run * ROWS : run * ROWS + rows, cols] = silu(total).astype(BF16)
            return 0

        lax.fori_loop(0, TILES, body, 0, unroll=4 if rows == ROWS else 10)

    def fill_rim(i, _):
        rim = rims[:, columns(i)].astype(F32)
        rim_clean, rim_corrupt = rim[:margin], rim[margin : 2 * margin]
        pieces = (rim_clean, rim_corrupt, jnp.where(take_rim, rim_clean, rim_corrupt))
        for run, part in enumerate(pieces):
            for k in range(per):
                at = (run * TILES + i * per + k) * span + 8 - margin
                pad[pl.ds(at, margin), :] = part[:, k * LANES : (k + 1) * LANES]
        return 0

    lax.fori_loop(0, INNER // width, fill, 0)
    convolve(ROWS)
    for load in loads[6:]:
        load.wait()

    def rate_of(slot, cols):
        rates[rate_at(slot), :] = jnp.exp(a_log[:, cols]) * (-LOG2E)

    def patched_rate(tile, _):
        rate_of(tile, pl.ds(pl.multiple_of(tile * LANES, LANES), LANES))
        return 0

    lax.fori_loop(0, TILES, patched_rate, 0, unroll=4)
    for tile in range(CUT_TILES):
        for run in (CLEAN, CORRUPT):
            cols = pl.ds(pl.multiple_of(v * SPAN + tile * LANES, LANES), LANES)
            rate_of(cut_slot(run, tile), cols)
    for slot in range(60, CHUNKS):
        rates[rate_at(slot), :] = jnp.zeros((STATE, LANES), F32)

    @pl.when(has_last)
    def _():
        copy.wait_recv()
        lax.fori_loop(0, INNER // width, fill_rim, 0, unroll=5)
        convolve(8)

    @pl.when(has_next)
    def _():
        copy.wait_send()


def emit_kernel(patched, effect, patched_out, effect_out, sems):
    copies = [
        pltpu.make_async_copy(patched, patched_out, sems.at[0]),
        pltpu.make_async_copy(effect, effect_out, sems.at[1]),
    ]
    for copy in copies:
        copy.start()
    for copy in copies:
        copy.wait()


def kernel(
    pos, mode, acts, x_w, dt_w, dt_b, rates, clean_in, corrupt_in, d_skip_in,
    patched, effect,
    clean_gate, corrupt_gate, d_skip, low, maps, weights, base, gates, dts, us, bs, cs, ends, totals,
    pair_ends, pair_totals, chip_ends, got_ends,
    leaving, landed, across, start, ys,
    cut, squares, whole, peaks, squares_z, line_squares, squares_x, spreads,
    peaks_z, line_peaks, peaks_x, pair_squares, chip_squares, pair_peaks, chip_peaks, sent_peaks, answer,
    load_sem, send_pt, recv_pt, send_pe, recv_pe, send_ce, recv_ce,
    send_in, recv_in, send_st, recv_st,
    send_cut, recv_cut, send_sz, recv_sz, send_sx, recv_sx, send_sp, recv_sp,
    send_pz, recv_pz, send_px, recv_px, send_qq, recv_qq, send_pp, recv_pp, send_an, recv_an,
):
    me = lax.axis_index("seq")
    v = lax.axis_index("var")
    chip = lax.div(me, 2)
    core = lax.rem(me, 2)
    mate = me + 1 - 2 * core
    mine = core * HALF
    theirs = HALF - mine
    barrier = pltpu.get_barrier_semaphore()

    loads = [
        pltpu.make_async_copy(src, dst, load_sem.at[i])
        for i, (src, dst) in enumerate(
            (
                (d_skip_in, d_skip), (clean_in.at[:, INNER:], clean_gate),
                (corrupt_in.at[:, INNER:], corrupt_gate),
            )
        )
    ]
    for load in loads:
        load.start()

    def signal(peer, variant):
        pl.semaphore_signal(barrier, inc=1, device_id=(peer, variant), device_id_type=MESH)

    row_x, line_z = lax.div(chip, 8), lax.rem(chip, 8)
    peers = [8 * lax.rem(row_x + dx, 4) + lax.rem(line_z + dz, 8) for dx, dz in STEPS]
    for peer in peers:
        signal(2 * peer + core, v)
    signal(mate, v)
    for k in range(1, VARS):
        signal(me, lax.rem(v + k, VARS))

    def to_variant(k, src, dst, send_sem, recv_sem):
        return pltpu.make_async_remote_copy(
            src_ref=src, dst_ref=dst, send_sem=send_sem, recv_sem=recv_sem,
            device_id=(me, lax.rem(v + k, VARS)), device_id_type=MESH,
        )

    def to_shard(peer, src, dst, send_sem, recv_sem):
        return pltpu.make_async_remote_copy(
            src_ref=src, dst_ref=dst, send_sem=send_sem, recv_sem=recv_sem,
            device_id=(peer, v), device_id_type=MESH,
        )

    take_gate = hit_rows(pos, me * ROWS, ROWS)[:, :1] & (mode[0] != 0)

    projected = lax.dot_general(
        acts[...], x_w[...], (((1,), (1,)), ((), ())), preferred_element_type=F32
    )
    low[...] = projected[:, :RANK].astype(BF16)
    maps[...] = projected[:, RANK + STATE :]
    for run in range(3):
        part = projected[run * ROWS : (run + 1) * ROWS]
        for n in range(STATE):
            at = run * ROWS * SPLAT + n
            bs[pl.ds(at, ROWS, stride=SPLAT), :] = jnp.broadcast_to(
                part[:, RANK + n : RANK + n + 1], (ROWS, LANES)
            )


    def place(slot, steps, act):
        dts[pl.ds(slot, ROWS, stride=PITCH), :] = steps
        us[pl.ds(slot, ROWS, stride=PITCH), :] = steps * act
        totals[slot] = jnp.sum(steps, axis=0, keepdims=True)

    wide = 5120

    def patched_steps(i, _):
        cols = pl.ds(pl.multiple_of(i * wide, wide), wide)
        raw = jnp.dot(low[2 * ROWS :, :], dt_w[:, cols], preferred_element_type=F32)
        steps = softplus(raw + dt_b[:, cols])
        act = acts[2 * ROWS :, cols].astype(F32)
        for k in range(wide // LANES):
            part = slice(k * LANES, (k + 1) * LANES)
            place(i * (wide // LANES) + k, steps[:, part], act[:, part])
        return 0

    lax.fori_loop(0, INNER // wide, patched_steps, 0)

    cols = pl.ds(pl.multiple_of(v * SPAN, LANES), SPAN)
    raw = jnp.dot(low[: 2 * ROWS, :], dt_w[:, cols], preferred_element_type=F32)
    steps = softplus(raw + dt_b[:, cols])
    act = acts[: 2 * ROWS, cols].astype(F32)
    for run in (CLEAN, CORRUPT):
        rows = slice(run * ROWS, (run + 1) * ROWS)
        for tile in range(CUT_TILES):
            part = slice(tile * LANES, (tile + 1) * LANES)
            place(cut_slot(run, tile), steps[rows, part], act[rows, part])
    blank = jnp.zeros((ROWS, LANES), F32)
    for slot in range(60, CHUNKS):
        place(slot, blank, blank)

    zero = jnp.zeros((8, LANES), F32)

    def rates_of(group):
        base = group * (STATE * 8)
        return [rates[pl.ds(pl.multiple_of(base + n * 8, 8), 8), :] for n in range(STATE)]

    def run_base(group):
        return jnp.where(group < 5, PATCHED, group - 5) * (ROWS * SPLAT)

    def local_group(group, drive):
        found = scan_group(
            dts, us, rates_of(group), group, (zero,) * STATE, drive, None, None
        )
        for n in range(STATE):
            ends[pl.ds(group * (STATE * 8) + n, 8, stride=STATE), :] = found[n]

    def local_pass(offset):
        def body(i, _):
            group = offset + i

            @pl.when(group < GROUPS - 1)
            def _():
                local_group(group, splat_reader(bs, run_base(group)))

            @pl.when(group == GROUPS - 1)
            def _():
                local_group(group, mixed_reader(bs))

            return 0

        lax.fori_loop(0, GROUPS // 2, body, 0)

    local_pass(lax.div(theirs, 8))
    pl.semaphore_wait(barrier, CHIPS - 1 + 1 + VARS - 1)
    theirs_3 = pl.ds(theirs, HALF)
    swap_totals = to_shard(mate, totals.at[theirs_3], pair_totals, send_pt, recv_pt)
    swap_totals.start()

    theirs_2 = pl.ds(pl.multiple_of(theirs * STATE, 8), HALF * STATE)
    swap_ends = to_shard(mate, ends.at[theirs_2], pair_ends, send_pe, recv_pe)
    swap_ends.start()
    local_pass(lax.div(mine, 8))
    swap_totals.wait()

    leads = core == 0

    def my_summary(k):
        own = ends[pl.ds(pl.multiple_of((mine + k) * STATE, 8), STATE), :]
        return own, totals[mine + k]

    def pair_of(k):
        own_end, own_total = my_summary(k)
        other_end = pair_ends[pl.ds(pl.multiple_of(k * STATE, 8), STATE), :]
        other_total = pair_totals[k]
        return (
            jnp.where(leads, own_end, other_end), jnp.where(leads, own_total, other_total),
            jnp.where(leads, other_end, own_end), jnp.where(leads, other_total, own_total),
        )

    swap_ends.wait()

    def chip_end(k, _):
        end_a, total_a, end_b, total_b = pair_of(k)
        chip_ends[k, :STATE] = jnp.exp2(rates[rate_at(mine + k), :] * total_b) * end_a + end_b
        chip_ends[k, STATE:] = total_a + total_b
        return 0

    lax.fori_loop(0, HALF, chip_end, 0, unroll=8)
    owns = (core == 0) | (chip < BUSY)
    others = pl.ds(0, CHIPS - 1)

    @pl.when(owns)
    def _():
        pltpu.make_async_copy(chip_ends.at[chip], got_ends.at[chip], recv_ce).start()

    for peer in peers:
        @pl.when((core == 0) | (peer < BUSY))
        def _():
            target = 2 * peer + core
            to_shard(target, chip_ends.at[peer], got_ends.at[chip], send_ce, recv_ce).start()

    my_rate = rates[rate_at(mine + chip), :]
    for run in range(3):
        for n in range(STATE):
            cs[pl.ds(run * ROWS * SPLAT + n, ROWS, stride=SPLAT), :] = jnp.broadcast_to(
                maps[run * ROWS : (run + 1) * ROWS, n : n + 1], (ROWS, LANES)
            )

    def local_readout(group, drive, read):
        scan_group(dts, us, rates_of(group), group, (zero,) * STATE, drive, read, ys)

    def plain_readout(group, _):
        at = run_base(group)
        local_readout(group, splat_reader(bs, at), splat_reader(cs, at))
        return 0

    lax.fori_loop(0, GROUPS - 1, plain_readout, 0)
    local_readout(GROUPS - 1, mixed_reader(bs), mixed_reader(cs))
    def chain(s, state):
        leaving[s] = state
        return jnp.exp2(my_rate * got_ends[s, STATE:]) * state + got_ends[s, :STATE]

    @pl.when(owns)
    def _():
        wait_for(got_ends, recv_ce)
        lax.fori_loop(0, CHIPS, chain, jnp.zeros((STATE, LANES), F32), unroll=4)
        pltpu.make_async_copy(leaving.at[chip], landed.at[chip], recv_in).start()
        for peer in peers:
            to_shard(2 * peer + core, leaving.at[peer], landed.at[chip], send_in, recv_in).start()

    def entry_weights(group, read):
        rate = rates_of(group)

        def step(t, run_total):
            row = pl.multiple_of(t * PITCH + group * 8, 8)
            run_total = run_total + dts[pl.ds(row, 8), :]
            at = (group * ROWS + t) * (STATE * 8)
            for n in range(STATE):
                weights[pl.ds(pl.multiple_of(at + n * 8, 8), 8), :] = read(t, n) * jnp.exp2(
                    run_total * rate[n]
                )
            return run_total

        lax.fori_loop(0, ROWS, step, zero, unroll=4)

    def plain_weights(group, _):
        entry_weights(group, splat_reader(cs, run_base(group)))
        return 0

    lax.fori_loop(0, GROUPS - 1, plain_weights, 0)
    entry_weights(GROUPS - 1, mixed_reader(cs))
    for load in loads:
        load.wait()

    def prepare(slot, act, skip, gate):
        rows = pl.ds(pl.multiple_of(slot * ROWS, 8), ROWS)
        base[rows, :] = ys[pl.ds(slot, ROWS, stride=PITCH), :] + skip * act
        gates[rows, :] = silu(gate)

    for run, gate_rows in ((CLEAN, clean_gate), (CORRUPT, corrupt_gate)):
        for tile in range(CUT_TILES):
            cols = pl.ds(pl.multiple_of(v * SPAN + tile * LANES, LANES), LANES)
            act = acts[run * ROWS : (run + 1) * ROWS, cols].astype(F32)
            prepare(cut_slot(run, tile), act, d_skip[:, cols], gate_rows[:, cols].astype(F32))

    def prepare_patched(tile, _):
        cols = pl.ds(pl.multiple_of(tile * LANES, LANES), LANES)
        gate = jnp.where(
            take_gate, clean_gate[:, cols].astype(F32), corrupt_gate[:, cols].astype(F32)
        )
        prepare(tile, acts[2 * ROWS :, cols].astype(F32), d_skip[:, cols], gate)
        return 0

    lax.fori_loop(0, TILES, prepare_patched, 0, unroll=2)
    def enter(k, _):
        end_a, total_a, _, _ = pair_of(k)
        before = landed[k]
        after = jnp.exp2(rates[rate_at(mine + k), :] * total_a) * before + end_a
        at = pl.ds(pl.multiple_of((mine + k) * STATE, 8), STATE)
        start[at, :] = jnp.where(leads, before, after)
        across[pl.ds(pl.multiple_of(k * STATE, 8), STATE), :] = jnp.where(leads, after, before)
        return 0

    swap_start = to_shard(
        mate, across, start.at[pl.ds(pl.multiple_of(mine * STATE, 8), HALF * STATE)],
        send_st, recv_st,
    )

    def enter_half(sources):
        wait_for(landed.at[pl.ds(0, sources)], recv_in)
        lax.fori_loop(0, HALF, enter, 0, unroll=8)
        swap_start.start()

    @pl.when(core == 1)
    def _():
        enter_half(BUSY)

    @pl.when(core == 0)
    def _():
        swap_start.wait_recv()

    def final_group(group, _):
        at = group * (STATE * 8)
        state = [start[pl.ds(at + n, 8, stride=STATE), :] for n in range(STATE)]

        def step(t, _):
            at = (group * ROWS + t) * (STATE * 8)
            total = None
            for n in range(STATE):
                term = weights[pl.ds(pl.multiple_of(at + n * 8, 8), 8), :] * state[n]
                total = term if total is None else total + term
            ys[pl.ds(pl.multiple_of(t * PITCH + group * 8, 8), 8), :] = total
            return 0

        lax.fori_loop(0, ROWS, step, 0, unroll=8)
        return 0

    def result(slot):
        rows = pl.ds(pl.multiple_of(slot * ROWS, 8), ROWS)
        y = ys[pl.ds(slot, ROWS, stride=PITCH), :]
        return ((y + base[rows, :]) * gates[rows, :]).astype(BF16)

    lax.fori_loop(6, GROUPS, final_group, 0)

    for tile in range(CUT_TILES):
        cut[:, tile * LANES : (tile + 1) * LANES] = result(cut_slot(CORRUPT, tile))
    directs = [
        to_variant(k, cut, whole.at[v], send_cut.at[k], recv_cut.at[k]) for k in (2, 1, VARS - 1)
    ]
    for direct in directs:
        direct.start()
    @pl.when(core == 0)
    def _():
        enter_half(CHIPS)

    @pl.when(core == 1)
    def _():
        swap_start.wait_recv()

    final_group(5, 0)
    squares[...] = jnp.zeros_like(squares)
    for tile in range(CUT_TILES):
        gap = result(cut_slot(CLEAN, tile)).astype(F32)
        gap = gap - cut[:, tile * LANES : (tile + 1) * LANES].astype(F32)
        squares[tile : tile + 1, :] = jnp.sum(gap * gap, axis=0, keepdims=True)

    def along_z(k):
        return 16 * row_x + 2 * lax.rem(line_z + k, 8) + 1

    def along_x(k):
        return 16 * lax.rem(row_x + k, 4) + 2 * line_z + 1

    def share(peer_of, count, slot, src, dst, send_sem, recv_sem):
        for k in sorted(range(1, count), key=lambda k: -min(k, count - k)):
            to_shard(peer_of(k), src, dst.at[slot], send_sem, recv_sem).start()
        dst[slot] = src[...]

    seven, three = pl.ds(0, 7), pl.ds(0, 3)
    squares_over = to_shard(mate, squares, pair_squares, send_qq, recv_qq)

    @pl.when(core == 0)
    def _():
        squares_over.start()

    whole[v] = cut[...]

    lax.fori_loop(0, 5, final_group, 0)
    def patched_tile(tile, _):
        cols = pl.ds(pl.multiple_of(tile * LANES, LANES), LANES)
        patched[:, cols] = result(tile)
        return 0

    lax.fori_loop(0, TILES, patched_tile, 0, unroll=4)


    @pl.when(core == 1)
    def _():
        squares_over.wait_recv()
        chip_squares[...] = squares[...] + pair_squares[...]
        share(along_z, 8, line_z, chip_squares, squares_z, send_sz, recv_sz)

    for direct in directs:
        direct.wait()

    for w in range(VARS):
        def peak_tile(i, _):
            here = pl.ds(pl.multiple_of(i * LANES, LANES), LANES)
            there = pl.ds(pl.multiple_of(w * SPAN + i * LANES, LANES), LANES)
            gap = jnp.abs(patched[:, there].astype(F32) - whole[w, :, here].astype(F32))
            peaks[pl.ds(w * CUT_TILES + i, 1), :] = jnp.max(gap, axis=0, keepdims=True)
            return 0

        lax.fori_loop(0, CUT_TILES, peak_tile, 0, unroll=2)

    sent_peaks[...] = peaks[...].astype(BF16)
    peaks_over = to_shard(mate, sent_peaks, pair_peaks, send_pp, recv_pp)
    answer_over = to_shard(mate, answer, answer, send_an, recv_an)

    @pl.when(core == 0)
    def _():
        peaks_over.start()

    @pl.when(core == 1)
    def _():
        wait_for(squares_z.at[seven], recv_sz)
        line_squares[...] = jnp.sum(squares_z[...], axis=0)
        share(along_x, 4, row_x, line_squares, squares_x, send_sx, recv_sx)
        peaks_over.wait_recv()
        both = jnp.maximum(sent_peaks[...].astype(F32), pair_peaks[...].astype(F32))
        chip_peaks[...] = both.astype(BF16)
        share(along_z, 8, line_z, chip_peaks, peaks_z, send_pz, recv_pz)
        wait_for(squares_x.at[three], recv_sx)
        spreads[v] = jnp.sqrt(jnp.sum(squares_x[...], axis=0) / (SHARDS * ROWS) + TINY)
        for k in range(1, VARS):
            to_variant(k, spreads.at[v], spreads.at[v], send_sp.at[k], recv_sp.at[k]).start()
        wait_for(peaks_z.at[seven], recv_pz)
        line_peaks[...] = jnp.max(peaks_z[...].astype(F32), axis=0).astype(BF16)
        share(along_x, 4, row_x, line_peaks, peaks_x, send_px, recv_px)
        wait_for(peaks_x.at[three], recv_px)
        for k in range(1, VARS):
            there = spreads.at[lax.rem(v + VARS - k, VARS)]
            to_variant(k, there, there, send_sp.at[k], recv_sp.at[k]).wait()
        peak = jnp.max(peaks_x[...].astype(F32), axis=0)
        for w in range(VARS):
            rows = slice(w * CUT_TILES, (w + 1) * CUT_TILES)
            answer[rows, :] = peak[rows, :] / spreads[w, :CUT_TILES, :]
        answer_over.start()
        wait_for(squares_z.at[seven], send_sz)
        wait_for(squares_x.at[three], send_sx)
        wait_for(peaks_z.at[seven], send_pz)
        wait_for(peaks_x.at[three], send_px)
        answer_over.wait_send()

    @pl.when(core == 0)
    def _():
        squares_over.wait_send()
        peaks_over.wait_send()
        answer_over.wait_recv()

    effect[...] = answer[...]
    @pl.when(core == 0)
    def _():
        wait_for(chip_ends.at[others], send_ce)

    @pl.when((core == 1) & (chip < BUSY))
    def _():
        wait_for(chip_ends.at[pl.ds(0, BUSY - 1)], send_ce)

    @pl.when((core == 1) & (chip >= BUSY))
    def _():
        wait_for(chip_ends.at[pl.ds(0, BUSY)], send_ce)

    @pl.when(owns)
    def _():
        wait_for(leaving.at[others], send_in)

    swap_start.wait_send()


SMEM = pl.BlockSpec(memory_space=pltpu.SMEM)
HBM = pl.BlockSpec(memory_space=pltpu.HBM)
VMEM = pl.BlockSpec(memory_space=pltpu.VMEM)
DMA = pltpu.SemaphoreType.DMA


def shards(
    clean_proj, corrupt_proj, patch_pos, patch_mode, a_log, dt_bias,
    conv_weight, conv_bias, x_weight, dt_weight, d_skip,
):
    hold = functools.partial(pltpu.with_memory_space_constraint, memory_space=pltpu.HBM)
    keep = functools.partial(pltpu.with_memory_space_constraint, memory_space=pltpu.VMEM)
    front = pl.pallas_call(
        front_kernel,
        out_shape=(
            pltpu.VMEM((3 * ROWS, INNER), BF16),
            pltpu.VMEM((RANK + 2 * STATE, INNER), BF16),
            pltpu.VMEM((RANK, INNER), BF16),
            pltpu.VMEM((1, INNER), F32),
            pltpu.VMEM((CHUNKS * STATE, LANES), F32),
        ),
        in_specs=[SMEM, SMEM] + [HBM] * 8,
        out_specs=(VMEM,) * 5,
        scratch_shapes=[
            pltpu.VMEM((8, INNER), BF16),
            pltpu.VMEM((STATE, INNER), F32),
            pltpu.VMEM((2, 8, INNER), BF16),
            pltpu.VMEM((8, INNER), F32),
            pltpu.VMEM((8, INNER), BF16),
            pltpu.VMEM((ROWS, INNER), BF16),
            pltpu.VMEM((ROWS, INNER), BF16),
            pltpu.VMEM((TAPS, INNER), F32),
            pltpu.VMEM((1, INNER), F32),
            pltpu.VMEM((3 * TILES * (8 + ROWS), LANES), F32),
            DMA((10,)),
            DMA,
            DMA,
        ],
        compiler_params=pltpu.CompilerParams(
            collective_id=1, has_side_effects=True, vmem_limit_bytes=40_000_000
        ),
        name="front",
    )(
        hold(patch_pos), patch_mode,
        *map(
            hold,
            (
                clean_proj, corrupt_proj, conv_weight, conv_bias[None], x_weight.T, dt_weight,
                dt_bias[None], a_log,
            ),
        ),
    )
    row = (1, LANES)
    tile = (STATE, LANES)
    patched, effect = pl.pallas_call(
        kernel,
        out_shape=(pltpu.VMEM((ROWS, INNER), BF16), pltpu.VMEM((TILES, LANES), F32)),
        in_specs=[SMEM, SMEM] + [VMEM] * 5 + [HBM] * 3,
        out_specs=(VMEM, VMEM),
        scratch_shapes=[
            pltpu.VMEM((ROWS, INNER), BF16),
            pltpu.VMEM((ROWS, INNER), BF16),
            pltpu.VMEM((1, INNER), F32),
            pltpu.VMEM((3 * ROWS, RANK), BF16),
            pltpu.VMEM((3 * ROWS, STATE), F32),
            pltpu.VMEM((GROUPS * ROWS * STATE * 8, LANES), F32),
            pltpu.VMEM((CHUNKS * ROWS, LANES), F32),
            pltpu.VMEM((CHUNKS * ROWS, LANES), F32),
            pltpu.VMEM((ROWS * PITCH, LANES), F32),
            pltpu.VMEM((ROWS * PITCH, LANES), F32),
            pltpu.VMEM((3 * ROWS * SPLAT + 8, LANES), F32),
            pltpu.VMEM((3 * ROWS * SPLAT + 8, LANES), F32),
            pltpu.VMEM((CHUNKS * STATE, LANES), F32),
            pltpu.VMEM((CHUNKS, *row), F32),
            pltpu.VMEM((HALF * STATE, LANES), F32),
            pltpu.VMEM((HALF, *row), F32),
            pltpu.VMEM((HALF, STATE + 1, LANES), F32),
            pltpu.VMEM((CHIPS, STATE + 1, LANES), F32),
            pltpu.VMEM((CHIPS, *tile), F32),
            pltpu.VMEM((HALF, *tile), F32),
            pltpu.VMEM((HALF * STATE, LANES), F32),
            pltpu.VMEM((CHUNKS * STATE, LANES), F32),
            pltpu.VMEM((ROWS * PITCH, LANES), F32),
            pltpu.VMEM((ROWS, SPAN), BF16),
            pltpu.VMEM((STATE, LANES), F32),
            pltpu.VMEM((VARS, ROWS, SPAN), BF16),
            pltpu.VMEM((TILES, LANES), F32),
            pltpu.VMEM((8, STATE, LANES), F32),
            pltpu.VMEM((STATE, LANES), F32),
            pltpu.VMEM((4, STATE, LANES), F32),
            pltpu.VMEM((VARS, STATE, LANES), F32),
            pltpu.VMEM((8, TILES, LANES), BF16),
            pltpu.VMEM((TILES, LANES), BF16),
            pltpu.VMEM((4, TILES, LANES), BF16),
            pltpu.VMEM((STATE, LANES), F32),
            pltpu.VMEM((STATE, LANES), F32),
            pltpu.VMEM((TILES, LANES), BF16),
            pltpu.VMEM((TILES, LANES), BF16),
            pltpu.VMEM((TILES, LANES), BF16),
            pltpu.VMEM((TILES, LANES), F32),
            DMA((3,)),
        ]
        + [DMA] * 10
        + [DMA((VARS,)), DMA((VARS,))]
        + [DMA] * 4
        + [DMA((VARS,)), DMA((VARS,))]
        + [DMA] * 10,
        compiler_params=pltpu.CompilerParams(
            collective_id=0, has_side_effects=True, vmem_limit_bytes=54_000_000
        ),
        name="mixer",
    )(
        hold(patch_pos), patch_mode, *map(keep, front),
        *map(hold, (clean_proj, corrupt_proj, d_skip[None])),
    )
    patched, effect = pl.pallas_call(
        emit_kernel,
        out_shape=(
            jax.ShapeDtypeStruct((ROWS, INNER), BF16),
            jax.ShapeDtypeStruct((TILES, LANES), F32),
        ),
        in_specs=[VMEM, VMEM],
        out_specs=(HBM, HBM),
        scratch_shapes=[DMA((2,))],
        compiler_params=pltpu.CompilerParams(vmem_limit_bytes=16_000_000),
        name="emit",
    )(
        keep(patched), keep(effect),
    )
    return (patched[None], effect.reshape(1, INNER))


def solution(mesh):
    return jax.shard_map(
        shards,
        mesh=mesh,
        in_specs=(
            P("seq", None), P("seq", None), P("var", None), P("var"),
            P(), P(), P(), P(), P(), P(), P(),
        ),
        out_specs=(P("var", "seq", None), P("var", None)),
        check_vma=False,
    )
```
